8 devices in a mesh: dp: 2 (over z, y), pp: 4 (over x, core).
Axes of the slice: x: 2, y: 2, z: 1, core: 2. Of those that a mesh axis runs over, the one named last changes fastest.
Arguments:
- patches: bfloat16 [8, 2, 256, 588], P('dp'), parts along dimension 0
- labels: int32 [8, 2], P('dp'), parts along dimension 0
- w_patch: bfloat16 [588, 1408], replicated
- b_patch: bfloat16 [1408], replicated
- cls_token: bfloat16 [1408], replicated
- pos_embed: bfloat16 [257, 1408], replicated
- ln1_gain: bfloat16 [4, 1408], P('pp')
- ln1_bias: bfloat16 [4, 1408], P('pp')
- w_qkv: bfloat16 [4, 1408, 3, 16, 88], P('pp')
- b_qkv: bfloat16 [4, 3, 16, 88], P('pp')
- w_proj: bfloat16 [4, 16, 88, 1408], P('pp')
- b_proj: bfloat16 [4, 1408], P('pp')
- ln2_gain: bfloat16 [4, 1408], P('pp')
- ln2_bias: bfloat16 [4, 1408], P('pp')
- w_fc1: bfloat16 [4, 1408, 6144], P('pp')
- b_fc1: bfloat16 [4, 6144], P('pp')
- w_fc2: bfloat16 [4, 6144, 1408], P('pp')
- b_fc2: bfloat16 [4, 1408], P('pp')
- lnf_gain: bfloat16 [1408], replicated
- lnf_bias: bfloat16 [1408], replicated
- w_head: bfloat16 [1408, 1000], replicated
- b_head: bfloat16 [1000], replicated
Outputs:
- output 1: float32 [2], P('dp'), parts along dimension 0
- output 2: float32 [1176, 1408], P('dp'), parts along dimension 0
- output 3: float32 [2816], P('dp'), parts along dimension 0
- output 4: float32 [2816], P('dp'), parts along dimension 0
- output 5: float32 [514, 1408], P('dp'), parts along dimension 0
- output 6: float32 [8, 1408], P(('dp', 'pp')), parts along dimension 0
- output 7: float32 [8, 1408], P(('dp', 'pp')), parts along dimension 0
- output 8: float32 [8, 1408, 3, 16, 88], P(('dp', 'pp')), parts along dimension 0
- output 9: float32 [8, 3, 16, 88], P(('dp', 'pp')), parts along dimension 0
- output 10: float32 [8, 16, 88, 1408], P(('dp', 'pp')), parts along dimension 0
- output 11: float32 [8, 1408], P(('dp', 'pp')), parts along dimension 0
- output 12: float32 [8, 1408], P(('dp', 'pp')), parts along dimension 0
- output 13: float32 [8, 1408], P(('dp', 'pp')), parts along dimension 0
- output 14: float32 [8, 1408, 6144], P(('dp', 'pp')), parts along dimension 0
- output 15: float32 [8, 6144], P(('dp', 'pp')), parts along dimension 0
- output 16: float32 [8, 6144, 1408], P(('dp', 'pp')), parts along dimension 0
- output 17: float32 [8, 1408], P(('dp', 'pp')), parts along dimension 0
- output 18: float32 [2816], P('dp'), parts along dimension 0
- output 19: float32 [2816], P('dp'), parts along dimension 0
- output 20: float32 [2816, 1000], P('dp'), parts along dimension 0
- output 21: float32 [2000], P('dp'), parts along dimension 0
There are 2 independent parts. The reference program is written for one: setup_inputs(seed, part) draws one part's arguments, and reference() takes and returns one part's arrays. A program takes and returns all parts, laid end to end along the dimension named above; an argument that names none is the same for every part.
All inputs are finite; a program needn't handle non-finite values.
Results may differ from the reference program's by a relative error of at most 0.02.
Values are sent between devices in bfloat16 or wider.
A program may use at most 1 GiB of HBM per device.

```python
import jax
import jax.numpy as jnp
from jax import lax

M = 4
MB = 2
NP = 256
PD = 588
D = 1408
HEADS = 16
HEAD = 88
FF = 6144
CLASSES = 1000
LAYERS = 4
TOKENS = NP + 1
EPS = 1e-6
SMOOTH = 0.1


def normal_draw(key, shape, scale):
    return (jax.random.normal(key, shape, jnp.float32) * scale).astype(jnp.bfloat16)


def gain_draw(key, shape):
    return (1.0 + 0.25 * jax.random.normal(key, shape, jnp.float32)).astype(jnp.bfloat16)


def setup_inputs(seed: int = 0, part: int = 0) -> dict:
    part_keys = jax.random.split(jax.random.fold_in(jax.random.key(seed), part), 2)
    shared_keys = jax.random.split(jax.random.key(seed + 1), 20)
    return {
        "patches": normal_draw(part_keys[0], (M, MB, NP, PD), 1.0),
        "labels": jax.random.randint(part_keys[1], (M, MB), 0, CLASSES, jnp.int32),
        "w_patch": normal_draw(shared_keys[0], (PD, D), PD ** -0.5),
        "b_patch": normal_draw(shared_keys[1], (D,), 0.3),
        "cls_token": normal_draw(shared_keys[2], (D,), 1.0),
        "pos_embed": normal_draw(shared_keys[3], (TOKENS, D), 0.5),
        "ln1_gain": gain_draw(shared_keys[4], (LAYERS, D)),
        "ln1_bias": normal_draw(shared_keys[5], (LAYERS, D), 0.2),
        "w_qkv": normal_draw(shared_keys[6], (LAYERS, D, 3, HEADS, HEAD), D ** -0.5),
        "b_qkv": normal_draw(shared_keys[7], (LAYERS, 3, HEADS, HEAD), 0.3),
        "w_proj": normal_draw(shared_keys[8], (LAYERS, HEADS, HEAD, D), D ** -0.5),
        "b_proj": normal_draw(shared_keys[9], (LAYERS, D), 0.3),
        "ln2_gain": gain_draw(shared_keys[10], (LAYERS, D)),
        "ln2_bias": normal_draw(shared_keys[11], (LAYERS, D), 0.2),
        "w_fc1": normal_draw(shared_keys[12], (LAYERS, D, FF), D ** -0.5),
        "b_fc1": normal_draw(shared_keys[13], (LAYERS, FF), 0.3),
        "w_fc2": normal_draw(shared_keys[14], (LAYERS, FF, D), FF ** -0.5),
        "b_fc2": normal_draw(shared_keys[15], (LAYERS, D), 0.3),
        "lnf_gain": gain_draw(shared_keys[16], (D,)),
        "lnf_bias": normal_draw(shared_keys[17], (D,), 0.2),
        "w_head": normal_draw(shared_keys[18], (D, CLASSES), D ** -0.5),
        "b_head": normal_draw(shared_keys[19], (CLASSES,), 0.5),
    }


def wide(values):
    return values.astype(jnp.float32)


def layer_norm(hidden, gain, bias):
    values = wide(hidden)
    centered = values - jnp.mean(values, axis=-1, keepdims=True)
    variance = jnp.mean(jnp.square(centered), axis=-1, keepdims=True)
    normed = centered * lax.rsqrt(variance + EPS)
    return (normed * wide(gain) + wide(bias)).astype(jnp.bfloat16)


def block(hidden, weights):
    ln1_gain, ln1_bias, w_qkv, b_qkv, w_proj, b_proj, ln2_gain, ln2_bias, w_fc1, b_fc1, w_fc2, b_fc2 = weights
    normed = layer_norm(hidden, ln1_gain, ln1_bias)
    qkv_rows = (jnp.einsum("btd,dkhe->btkhe", wide(normed), wide(w_qkv)) + wide(b_qkv)).astype(jnp.bfloat16)
    scores = jnp.einsum("bqhe,bkhe->bhqk", wide(qkv_rows[:, :, 0]), wide(qkv_rows[:, :, 1])) * (HEAD ** -0.5)
    probs = jax.nn.softmax(scores, axis=-1).astype(jnp.bfloat16)
    context = jnp.einsum("bhqk,bkhe->bqhe", wide(probs), wide(qkv_rows[:, :, 2])).astype(jnp.bfloat16)
    mid = (wide(hidden) + jnp.einsum("bthe,hed->btd", wide(context), wide(w_proj)) + wide(b_proj)).astype(jnp.bfloat16)
    normed_mlp = layer_norm(mid, ln2_gain, ln2_bias)
    pre_act = jnp.einsum("btd,df->btf", wide(normed_mlp), wide(w_fc1)) + wide(b_fc1)
    activ = jax.nn.gelu(pre_act, approximate=False).astype(jnp.bfloat16)
    return (wide(mid) + jnp.einsum("btf,fd->btd", wide(activ), wide(w_fc2)) + wide(b_fc2)).astype(jnp.bfloat16)


def microbatch_loss(params, patch_rows, label_rows):
    w_patch, b_patch, cls_token, pos_embed = params[:4]
    layer_params = tuple(params[4:16])
    lnf_gain, lnf_bias, w_head, b_head = params[16:]
    batch_size = patch_rows.shape[0]
    projected = jnp.einsum("bnp,pd->bnd", wide(patch_rows), wide(w_patch)) + wide(b_patch)
    cls_rows = jnp.broadcast_to(wide(cls_token), (batch_size, 1, D))
    hidden = (jnp.concatenate([cls_rows, projected], axis=1) + wide(pos_embed)).astype(jnp.bfloat16)

    def layer_step(carry, weights):
        return jax.checkpoint(block)(carry, weights), None

    hidden, _ = lax.scan(layer_step, hidden, layer_params)
    pooled = layer_norm(hidden[:, 0], lnf_gain, lnf_bias)
    logits = jnp.dot(wide(pooled), wide(w_head)) + wide(b_head)
    log_probs = jax.nn.log_softmax(logits, axis=-1)
    target = (1.0 - SMOOTH) * jax.nn.one_hot(label_rows, CLASSES, dtype=jnp.float32) + SMOOTH / CLASSES
    return -jnp.sum(target * log_probs) / (M * MB)


def reference(patches, labels, w_patch, b_patch, cls_token, pos_embed, ln1_gain, ln1_bias, w_qkv, b_qkv, w_proj, b_proj, ln2_gain, ln2_bias, w_fc1, b_fc1, w_fc2, b_fc2, lnf_gain, lnf_bias, w_head, b_head):
    params = tuple(wide(tensor) for tensor in (w_patch, b_patch, cls_token, pos_embed, ln1_gain, ln1_bias, w_qkv, b_qkv, w_proj, b_proj, ln2_gain, ln2_bias, w_fc1, b_fc1, w_fc2, b_fc2, lnf_gain, lnf_bias, w_head, b_head))
    loss_grad = jax.value_and_grad(microbatch_loss)

    def micro_step(carry, inputs):
        loss_acc, grad_acc = carry
        value, grads = loss_grad(params, inputs[0], inputs[1])
        return (loss_acc + value, tuple(total + piece for total, piece in zip(grad_acc, grads))), None

    init = (jnp.zeros((), jnp.float32), tuple(jnp.zeros_like(tensor) for tensor in params))
    (loss_total, grads), _ = lax.scan(micro_step, init, (patches, labels))
    g_w_patch, g_b_patch, g_cls_token, g_pos_embed, g_ln1_gain, g_ln1_bias, g_w_qkv, g_b_qkv, g_w_proj, g_b_proj, g_ln2_gain, g_ln2_bias, g_w_fc1, g_b_fc1, g_w_fc2, g_b_fc2, g_lnf_gain, g_lnf_bias, g_w_head, g_b_head = grads
    return (loss_total.reshape(1), g_w_patch, g_b_patch, g_cls_token, g_pos_embed, g_ln1_gain, g_ln1_bias, g_w_qkv, g_b_qkv, g_w_proj, g_b_proj, g_ln2_gain, g_ln2_bias, g_w_fc1, g_b_fc1, g_w_fc2, g_b_fc2, g_lnf_gain, g_lnf_bias, g_w_head, g_b_head)
```

```python
import functools
import jax
import jax.numpy as jnp
from jax import lax
from jax.sharding import PartitionSpec as P

EPS = 1e-6
SMOOTH = 0.1
F32 = jnp.float32
BF16 = jnp.bfloat16
exact_gelu = functools.partial(jax.nn.gelu, approximate=False)


def layer_norm(hidden, gain, bias):
    values = hidden.astype(F32)
    centered = values - jnp.mean(values, axis=-1, keepdims=True)
    variance = jnp.mean(jnp.square(centered), axis=-1, keepdims=True)
    return (centered * lax.rsqrt(variance + EPS) * gain + bias).astype(BF16)


def norm_backward(grad, hidden, gain):
    values = hidden.astype(F32)
    centered = values - jnp.mean(values, axis=-1, keepdims=True)
    inv = lax.rsqrt(jnp.mean(jnp.square(centered), axis=-1, keepdims=True) + EPS)
    unit = centered * inv
    grad = grad.astype(F32)
    scaled = grad * gain
    grad_in = inv * (scaled - jnp.mean(scaled, axis=-1, keepdims=True) - unit * jnp.mean(scaled * unit, axis=-1, keepdims=True))
    return grad_in, jnp.sum(grad * unit, axis=(0, 1)), jnp.sum(grad, axis=(0, 1))


def dot(spec, left, right):
    return jnp.einsum(spec, left, right, preferred_element_type=F32)


def layer_forward(hidden, weights):
    ln1_gain, ln1_bias, w_qkv, b_qkv, w_proj, b_proj, ln2_gain, ln2_bias, w_fc1, b_fc1, w_fc2, b_fc2 = weights
    scale = w_qkv.shape[-1] ** -0.5
    normed = layer_norm(hidden, ln1_gain, ln1_bias)
    qkv = (dot("btd,dkhe->btkhe", normed, w_qkv) + b_qkv).astype(BF16)
    scores = dot("bqhe,bkhe->bhqk", qkv[:, :, 0], qkv[:, :, 1]) * scale
    probs = jax.nn.softmax(scores, axis=-1)
    context = dot("bhqk,bkhe->bqhe", probs.astype(BF16), qkv[:, :, 2]).astype(BF16)
    mid = (hidden.astype(F32) + dot("bthe,hed->btd", context, w_proj) + b_proj).astype(BF16)
    normed_mlp = layer_norm(mid, ln2_gain, ln2_bias)
    pre_act = dot("btd,df->btf", normed_mlp, w_fc1) + b_fc1
    activ = exact_gelu(pre_act).astype(BF16)
    out = (mid.astype(F32) + dot("btf,fd->btd", activ, w_fc2) + b_fc2).astype(BF16)
    return out, (hidden, normed, qkv, probs, context, mid, normed_mlp, pre_act, activ)


def layer_backward(grad_out, weights, saved):
    ln1_gain, ln1_bias, w_qkv, b_qkv, w_proj, b_proj, ln2_gain, ln2_bias, w_fc1, b_fc1, w_fc2, b_fc2 = weights
    hidden, normed, qkv, probs, context, mid, normed_mlp, pre_act, activ = saved
    scale = w_qkv.shape[-1] ** -0.5
    grad_activ = dot("btd,fd->btf", grad_out, w_fc2).astype(BF16)
    grad_pre = jax.vjp(exact_gelu, pre_act)[1](grad_activ.astype(F32))[0]
    g_b_fc1 = jnp.sum(grad_pre, axis=(0, 1))
    grad_pre = grad_pre.astype(BF16)
    grad_normed_mlp = dot("btf,df->btd", grad_pre, w_fc1).astype(BF16)
    grad_mid, g_ln2_gain, g_ln2_bias = norm_backward(grad_normed_mlp, mid, ln2_gain)
    grad_mid = (grad_out.astype(F32) + grad_mid).astype(BF16)
    grad_context = dot("btd,hed->bthe", grad_mid, w_proj).astype(BF16)
    grad_probs = dot("bqhe,bkhe->bhqk", grad_context, qkv[:, :, 2])
    grad_value = dot("bhqk,bqhe->bkhe", probs.astype(BF16), grad_context).astype(BF16)
    grad_scores = probs * (grad_probs - jnp.sum(grad_probs * probs, axis=-1, keepdims=True))
    grad_scores = (grad_scores * scale).astype(BF16)
    grad_query = dot("bhqk,bkhe->bqhe", grad_scores, qkv[:, :, 1]).astype(BF16)
    grad_key = dot("bhqk,bqhe->bkhe", grad_scores, qkv[:, :, 0]).astype(BF16)
    grad_qkv = jnp.stack([grad_query, grad_key, grad_value], axis=2)
    grad_normed = dot("btkhe,dkhe->btd", grad_qkv, w_qkv).astype(BF16)
    grad_hidden, g_ln1_gain, g_ln1_bias = norm_backward(grad_normed, hidden, ln1_gain)
    grad_hidden = (grad_mid.astype(F32) + grad_hidden).astype(BF16)
    return grad_hidden, (grad_out, grad_pre, grad_mid, grad_qkv), (g_ln1_gain, g_ln1_bias, g_ln2_gain, g_ln2_bias, g_b_fc1)


def solution(mesh):
    stages = mesh.shape["pp"]
    forward_perm = [(index, index + 1) for index in range(stages - 1)]
    backward_perm = [(index + 1, index) for index in range(stages - 1)]
    in_specs = (P("dp"), P("dp"), P(), P(), P(), P()) + (P("pp"),) * 12 + (P(),) * 4
    out_specs = (P("dp"),) * 5 + (P(("dp", "pp")),) * 12 + (P("dp"),) * 4

    def body(patches, labels, w_patch, b_patch, cls_token, pos_embed, *rest):
        weights = [tensor[0] for tensor in rest[:12]]
        for index in (0, 1, 3, 5, 6, 7, 9, 11):
            weights[index] = weights[index].astype(F32)
        weights = tuple(weights)
        lnf_gain, lnf_bias, w_head, b_head = rest[12:]
        stage = lax.axis_index("pp")
        is_first = stage == 0
        is_last = stage == stages - 1
        micros, batch = labels.shape
        tokens, width = pos_embed.shape
        inv_count = 1.0 / (micros * batch)
        steps = micros + stages - 1

        projected = dot("mbnp,pd->mbnd", patches, w_patch) + b_patch.astype(F32)
        first = jnp.broadcast_to(cls_token.astype(F32), (micros, batch, 1, width))
        embedded = (jnp.concatenate([first, projected], axis=2) + pos_embed.astype(F32)).astype(BF16)

        received = embedded[0]
        saves, outs = [], []
        for step in range(steps):
            stage_in = jnp.where(is_first, embedded[min(step, micros - 1)], received)
            out, saved = layer_forward(stage_in, weights)
            saves.append(saved)
            outs.append(out)
            if step < steps - 1:
                received = lax.ppermute(out, "pp", forward_perm)
        tops = jnp.stack([out[:, 0] for out in outs[stages - 1:]])
        tops = lax.all_gather(tops, "pp")[stages - 1].reshape(micros * batch, width)

        pooled, lnf_vjp = jax.vjp(layer_norm, tops, lnf_gain.astype(F32), lnf_bias.astype(F32))
        logits = jnp.dot(pooled, w_head, preferred_element_type=F32) + b_head.astype(F32)
        classes = logits.shape[-1]
        log_probs = jax.nn.log_softmax(logits, axis=-1)
        target = (1.0 - SMOOTH) * jax.nn.one_hot(labels.reshape(-1), classes, dtype=F32) + SMOOTH / classes
        loss = -jnp.sum(target * log_probs) * inv_count
        grad_logits = (jnp.exp(log_probs) - target) * inv_count
        grad_low = grad_logits.astype(BF16)
        g_w_head = dot("bd,bc->dc", pooled, grad_low)
        g_b_head = jnp.sum(grad_logits, axis=0)
        grad_pooled = dot("bc,dc->bd", grad_low, w_head).astype(BF16)
        grad_tops, g_lnf_gain, g_lnf_bias = lnf_vjp(grad_pooled)
        grad_tops = grad_tops.reshape(micros, batch, 1, width)
        grad_tops = jnp.concatenate([grad_tops, jnp.zeros((micros, batch, tokens - 1, width), BF16)], axis=2)

        stacks = [jnp.stack(group) for group in zip(*saves)]
        received = grad_tops[0]
        parts, smalls, grads_in = [], [], []
        for step in range(steps):
            grad_out = jnp.where(is_last, grad_tops[min(step, micros - 1)], received)
            slot = jnp.clip(step - (stages - 1) + 2 * stage, 0, steps - 1)
            saved = tuple(lax.dynamic_index_in_dim(stack, slot, 0, keepdims=False) for stack in stacks)
            grad_in, part, small = layer_backward(grad_out, weights, saved)
            micro = step - (stages - 1 - stage)
            valid = (micro >= 0) & (micro < micros)
            parts.append(part)
            smalls.append(tuple(jnp.where(valid, piece, 0.0) for piece in small))
            grads_in.append(grad_in)
            if step < steps - 1:
                received = lax.ppermute(grad_in, "pp", backward_perm)

        g_ln1_gain, g_ln1_bias, g_ln2_gain, g_ln2_bias, g_b_fc1 = (sum(group) for group in zip(*smalls))
        window = lambda stack, start: lax.dynamic_slice_in_dim(stack, start, micros, 0)
        grad_out, grad_pre, grad_mid, grad_qkv = (window(jnp.stack(group), stages - 1 - stage) for group in zip(*parts))
        normed, context, normed_mlp, activ = (window(stacks[index], stage) for index in (1, 4, 6, 8))
        total = lambda grad: jnp.sum(grad.astype(F32), axis=(0, 1, 2))
        grad_embedded = jnp.stack(grads_in[stages - 1:])
        mine = grad_embedded
        for other in range(1, stages):
            moved = lax.ppermute(mine, "pp", [(0, other)])
            grad_embedded = jnp.where(stage == other, moved, grad_embedded)
        layer_grads = (
            g_ln1_gain, g_ln1_bias,
            dot("mbtd,mbtkhe->dkhe", normed, grad_qkv), total(grad_qkv),
            dot("mbthe,mbtd->hed", context, grad_mid), total(grad_mid),
            g_ln2_gain, g_ln2_bias,
            dot("mbtd,mbtf->df", normed_mlp, grad_pre), g_b_fc1,
            dot("mbtf,mbtd->fd", activ, grad_out), total(grad_out),
        )
        g_pos_embed = jnp.sum(grad_embedded.astype(F32), axis=(0, 1))
        embed_grads = (
            dot("mbnp,mbnd->pd", patches, grad_embedded[:, :, 1:]),
            jnp.sum(g_pos_embed[1:], axis=0), g_pos_embed[0], g_pos_embed,
        )
        return (loss.reshape(1),) + embed_grads + tuple(grad[None] for grad in layer_grads) + (g_lnf_gain, g_lnf_bias, g_w_head, g_b_head)

    return jax.shard_map(body, mesh=mesh, in_specs=in_specs, out_specs=out_specs, check_vma=False)
```

```python
import functools
import math
import jax
import jax.numpy as jnp
from jax import lax
from jax.experimental import pallas as pl
from jax.experimental.pallas import tpu as pltpu
from jax.sharding import PartitionSpec as P

EPS = 1e-6
SMOOTH = 0.1
F32 = jnp.float32
BF16 = jnp.bfloat16
MESH = pl.DeviceIdType.MESH
CHUNK = 512
GROUP = 2
BLOCK = 64


def layer_norm(hidden, gain, bias):
    values = hidden.astype(F32)
    centered = values - jnp.mean(values, axis=-1, keepdims=True)
    variance = jnp.mean(jnp.square(centered), axis=-1, keepdims=True)
    return (centered * lax.rsqrt(variance + EPS) * gain + bias).astype(BF16)


def dot(left, right, left_axis=1, right_axis=0):
    return lax.dot_general(left, right, (((left_axis,), (right_axis,)), ((), ())), preferred_element_type=F32)


def by_rows(rows, visit):
    def step(index, carry):
        visit(pl.ds(pl.multiple_of(index * BLOCK, BLOCK), BLOCK))
        return carry

    lax.fori_loop(0, rows // BLOCK, step, 0)
    if rows % BLOCK:
        visit(pl.ds(rows - rows % BLOCK, rows % BLOCK))


def fold(values):
    rows, columns = values.shape
    return jnp.sum(values.reshape(rows // 8, 8, columns), axis=0)


def everyone(stage, stages):
    barrier = pltpu.get_barrier_semaphore()
    for hop in range(1, stages):
        pl.semaphore_signal(barrier, inc=1, device_id={"pp": lax.rem(stage + hop, stages)}, device_id_type=MESH)
    pl.semaphore_wait(barrier, stages - 1)


def forward_kernel(dims, *refs):
    (emb, wqkv, wproj, wfc1, wfc2, g1, b1, bqkv, bproj, g2, b2, bfc1, bfc2,
     x_s, a_s, qkv_s, c_s, h_s, n_s, d_s, g_s, p_s, tops_out,
     vqkv, vproj, vfc1, vfc2, xin, act, qkv, ctx, mid, yacc, ubuf, gbuf, pbuf, yout, tops,
     wsem, qsem, recv_sem, send_sem, top_sem, save_sem, usem, gsem, psem, free_sem) = refs
    stages, images, tokens, heads, head = dims
    rows, width = mid.shape
    chunks = vfc1.shape[1] // CHUNK
    stage = lax.axis_index("pp")
    is_first = stage == 0
    is_last = stage == stages - 1
    scale2 = head ** -0.5 / math.log(2.0)

    def qkv_copy(index, slot):
        part = lax.rem(index, 3)
        return pltpu.make_async_copy(wqkv.at[pl.ds(part * width, width)], vqkv.at[slot], qsem.at[slot])

    def emb_copy(image, slot):
        return pltpu.make_async_copy(emb.at[image], xin.at[slot], recv_sem.at[slot])

    qkv_copy(0, 0).start()

    @pl.when(is_first)
    def _():
        emb_copy(0, 0).start()
        emb_copy(1, 1).start()

    qkv_copy(1, 1).start()
    proj_copy = pltpu.make_async_copy(wproj, vproj, wsem.at[0])
    fc1_copy = pltpu.make_async_copy(wfc1, vfc1, wsem.at[1])
    fc2_copy = pltpu.make_async_copy(wfc2, vfc2, wsem.at[2])
    proj_copy.start()
    fc1_copy.start()
    fc2_copy.start()
    everyone(stage, stages)

    def saves(image, slot):
        pairs = ((xin.at[slot], x_s), (act, a_s), (qkv, qkv_s), (ctx, c_s), (mid, h_s), (act, n_s))
        return [pltpu.make_async_copy(src, dst.at[image], save_sem.at[at]) for at, (src, dst) in enumerate(pairs)]

    def u_save(image, chunk):
        slot = lax.rem(chunk, 3)
        return pltpu.make_async_copy(ubuf.at[slot], d_s.at[image, :, pl.ds(pl.multiple_of(chunk * CHUNK, CHUNK), CHUNK)], usem.at[slot])

    def g_save(image, chunk):
        slot = lax.rem(chunk, 2)
        return pltpu.make_async_copy(gbuf.at[slot], g_s.at[image, :, pl.ds(pl.multiple_of(chunk * CHUNK, CHUNK), CHUNK)], gsem.at[slot])

    def p_save(image, group):
        slot = group % 2
        return pltpu.make_async_copy(pbuf.at[slot], p_s.at[image, pl.ds(group * GROUP, GROUP)], psem.at[slot])

    def top_copy(image, other):
        return pltpu.make_async_remote_copy(
            src_ref=yout.at[pl.ds(0, 16)], dst_ref=tops.at[image], send_sem=send_sem.at[1 + other], recv_sem=top_sem,
            device_id={"pp": other}, device_id_type=MESH)

    def next_copy(image, slot):
        return pltpu.make_async_remote_copy(
            src_ref=yout, dst_ref=xin.at[slot], send_sem=send_sem.at[0], recv_sem=recv_sem.at[slot],
            device_id={"pp": lax.rem(stage + 1, stages)}, device_id_type=MESH)

    def wait_sent(image):
        @pl.when(jnp.logical_not(is_last))
        def _():
            next_copy(image, 0).wait_send()

        @pl.when(is_last)
        def _():
            for other in range(stages - 1):
                top_copy(image, other).wait_send()

    def one_image(image, carry):
        slot = lax.rem(image, 2)
        save_x, save_a, save_qkv, save_c, save_h, save_n = saves(image, slot)
        emb_copy(image, slot).wait()
        save_x.start()

        @pl.when(image > 0)
        def _():
            save_n.wait()
            save_qkv.wait()

        def norm1(lines):
            act[lines, :] = layer_norm(xin[slot, lines, :], g1[...], b1[...])

        by_rows(rows, norm1)
        save_a.start()

        def qkv_part(part, carry):
            index = image * 3 + part
            where = lax.rem(index, 2)
            qkv_copy(index, where).wait()
            columns = pl.ds(pl.multiple_of(part * width, 128), width)
            qkv[:, columns] = (dot(act[...], vqkv[where], 1, 1) + bqkv[:, columns]).astype(BF16)

            @pl.when(index + 2 < images * 3)
            def _():
                qkv_copy(index + 2, where).start()

            return carry

        lax.fori_loop(0, 3, qkv_part, 0)
        save_qkv.start()

        @pl.when(image > 0)
        def _():
            save_c.wait()
            save_h.wait()
            p_save(image, 0).wait()
            p_save(image, 1).wait()

        for group in range(heads // GROUP):
            if group >= 2:
                p_save(image, group).wait()
            for inner in range(GROUP):
                at = (group * GROUP + inner) * head
                q = qkv[:, at:at + head]
                k = qkv[:, width + at:width + at + head]
                v = qkv[:, 2 * width + at:2 * width + at + head]
                scores = dot(k, q, 1, 1)
                top, tail = scores[:tokens - 1], scores[tokens - 1:]
                most = jnp.maximum(jnp.max(top, axis=0, keepdims=True), tail[:1])
                top = jnp.exp2((top - most) * scale2)
                real = lax.broadcasted_iota(jnp.int32, tail.shape, 0) < 1
                tail = jnp.where(real, jnp.exp2(jnp.minimum(tail - most, 0.0) * scale2), 0.0)
                inv = 1.0 / (jnp.sum(top, axis=0, keepdims=True) + jnp.sum(tail, axis=0, keepdims=True))
                probs = jnp.concatenate([top, tail], axis=0) * inv
                pbuf[group % 2, inner] = probs
                ctx[:, at:at + head] = dot(probs.astype(BF16), v, 0, 0).astype(BF16)
            p_save(image, group).start()
        save_c.start()

        @pl.when(image == 0)
        def _():
            proj_copy.wait()

        mid[...] = (dot(ctx[...], vproj[...]) + bproj[...] + xin[slot].astype(F32)).astype(BF16)
        save_h.start()
        save_x.wait()

        @pl.when(jnp.logical_and(is_first, image + 2 < images))
        def _():
            emb_copy(image + 2, slot).start()

        @pl.when(jnp.logical_and(stage > 0, image + 2 < images))
        def _():
            pl.semaphore_signal(free_sem, inc=1, device_id={"pp": lax.rem(stage + stages - 1, stages)}, device_id_type=MESH)

        save_a.wait()

        def norm2(lines):
            hidden = mid[lines, :]
            act[lines, :] = layer_norm(hidden, g2[...], b2[...])
            yacc[lines, :] = hidden.astype(F32) + bfc2[...]

        by_rows(rows, norm2)
        save_n.start()

        @pl.when(image == 0)
        def _():
            fc1_copy.wait()
            fc2_copy.wait()

        @pl.when(image > 0)
        def _():
            for chunk in range(3):
                u_save(image, chunk).wait()
            for chunk in range(2):
                g_save(image, chunk).wait()

        def fc1(chunk):
            columns = pl.ds(pl.multiple_of(chunk * CHUNK, CHUNK), CHUNK)
            ubuf[lax.rem(chunk, 3)] = dot(act[...], vfc1[:, columns]) + bfc1[:, columns]

        def fc2(chunk):
            slot3, slot2 = lax.rem(chunk, 3), lax.rem(chunk, 2)
            pre = ubuf[slot3]
            cdf = 0.5 + 0.5 * lax.erf(pre * (0.5 ** 0.5))
            pdf = jnp.exp2(pre * pre * (-0.5 / math.log(2.0))) * ((2.0 * math.pi) ** -0.5)
            activ = (pre * cdf).astype(BF16)
            gbuf[slot2] = activ
            ubuf[slot3] = cdf + pre * pdf
            yacc[...] += dot(activ, vfc2[pl.ds(pl.multiple_of(chunk * CHUNK, CHUNK), CHUNK), :])

        fc1(0)

        def mlp_step(chunk, carry):
            @pl.when(chunk >= 3)
            def _():
                u_save(image, chunk).wait()
                g_save(image, chunk - 1).wait()

            fc1(chunk)
            fc2(chunk - 1)
            u_save(image, chunk - 1).start()
            g_save(image, chunk - 1).start()
            return carry

        lax.fori_loop(1, chunks, mlp_step, 0)
        g_save(image, chunks - 1).wait()
        fc2(chunks - 1)
        u_save(image, chunks - 1).start()
        g_save(image, chunks - 1).start()

        @pl.when(image > 0)
        def _():
            wait_sent(image)

        yout[...] = yacc[...].astype(BF16)

        @pl.when(jnp.logical_and(jnp.logical_not(is_last), image >= 2))
        def _():
            pl.semaphore_wait(free_sem, 1)

        @pl.when(jnp.logical_not(is_last))
        def _():
            next_copy(image, slot).start()

        @pl.when(is_last)
        def _():
            for other in range(stages - 1):
                top_copy(image, other).start()
            tops[image] = yout[pl.ds(0, 16), :]

        return carry

    lax.fori_loop(0, images, one_image, 0)
    wait_sent(images - 1)
    _, _, save_qkv, save_c, save_h, save_n = saves(images - 1, 0)
    for copy in (save_qkv, save_c, save_h, save_n):
        copy.wait()
    for chunk in range(3):
        u_save(images - 1, chunk).wait()
    for chunk in range(2):
        g_save(images - 1, chunk).wait()
        p_save(images - 1, chunk).wait()

    @pl.when(jnp.logical_not(is_last))
    def _():
        pltpu.make_async_copy(tops_out, tops, top_sem).wait()

    out = pltpu.make_async_copy(tops, tops_out, wsem.at[0])
    out.start()
    out.wait()


def norm_backward(grad, hidden, gain):
    values = hidden.astype(F32)
    centered = values - jnp.mean(values, axis=-1, keepdims=True)
    inv = lax.rsqrt(jnp.mean(jnp.square(centered), axis=-1, keepdims=True) + EPS)
    unit = centered * inv
    scaled = grad * gain
    grad_in = inv * (scaled - jnp.mean(scaled, axis=-1, keepdims=True) - unit * jnp.mean(scaled * unit, axis=-1, keepdims=True))
    return grad_in, grad * unit


def backward_kernel(dims, *refs):
    (gtop, wqkv, wproj, wfc1, wfc2, g1, g2, x_s, qkv_s, h_s, d_s, p_s,
     gy_s, gpre_s, gmid_s, gqkv_s, gemb, sum1g, sum1b, sum2g, sum2b, sumproj, sumfc2, sumqkv, sumfc1,
     vqkv, vproj, vfc1, vfc2, gin, acc, dbuf, abuf, gbuf, hid, gmid, gctx, qkv, gqkv, pbuf, gout,
     wsem, qsem, recv_sem, send_sem, emb_sem, save_sem, load_sem, dsem, gsem, psem, free_sem) = refs
    stages, images, tokens, heads, head = dims
    rows, width = gmid.shape
    chunks = vfc1.shape[1] // CHUNK
    groups = heads // GROUP
    stage = lax.axis_index("pp")
    is_first = stage == 0
    is_last = stage == stages - 1
    scale = head ** -0.5

    def qkv_copy(index, slot):
        part = lax.rem(index, 3)
        return pltpu.make_async_copy(wqkv.at[pl.ds(part * width, width)], vqkv.at[slot], qsem.at[slot])

    def top_copy(image, slot):
        return pltpu.make_async_copy(gtop.at[image], gin.at[slot], recv_sem.at[slot])

    def d_load(image, chunk):
        slot = lax.rem(chunk, 3)
        return pltpu.make_async_copy(d_s.at[image, :, pl.ds(pl.multiple_of(chunk * CHUNK, CHUNK), CHUNK)], dbuf.at[slot], dsem.at[slot])

    def g_save(image, chunk):
        slot = lax.rem(chunk, 2)
        return pltpu.make_async_copy(gbuf.at[slot], gpre_s.at[image, :, pl.ds(pl.multiple_of(chunk * CHUNK, CHUNK), CHUNK)], gsem.at[slot])

    def p_load(image, group):
        slot = group % 2
        return pltpu.make_async_copy(p_s.at[image, pl.ds(group * GROUP, GROUP)], pbuf.at[slot], psem.at[slot])

    def saves(image, slot):
        pairs = ((gin.at[slot], gy_s), (gmid, gmid_s), (gqkv, gqkv_s))
        return [pltpu.make_async_copy(src, dst.at[image], save_sem.at[at]) for at, (src, dst) in enumerate(pairs)]

    def loads(image):
        pairs = ((h_s, hid), (x_s, hid), (qkv_s, qkv))
        return [pltpu.make_async_copy(src.at[image], dst, load_sem.at[at]) for at, (src, dst) in enumerate(pairs)]

    def next_copy(slot):
        return pltpu.make_async_remote_copy(
            src_ref=gout, dst_ref=gin.at[slot], send_sem=send_sem.at[0], recv_sem=recv_sem.at[slot],
            device_id={"pp": lax.rem(stage + stages - 1, stages)}, device_id_type=MESH)

    def emb_send(image, other):
        return pltpu.make_async_remote_copy(
            src_ref=gout, dst_ref=gemb.at[image], send_sem=send_sem.at[other], recv_sem=emb_sem,
            device_id={"pp": other}, device_id_type=MESH)

    def emb_local(image):
        return pltpu.make_async_copy(gout, gemb.at[image], save_sem.at[3])

    def wait_sent(image):
        @pl.when(jnp.logical_not(is_first))
        def _():
            next_copy(0).wait_send()

        @pl.when(is_first)
        def _():
            for other in range(1, stages):
                emb_send(image, other).wait_send()
            emb_local(image).wait()

    @pl.when(is_last)
    def _():
        top_copy(0, 0).start()
        top_copy(1, 1).start()

    fc2_copy = pltpu.make_async_copy(wfc2, vfc2, wsem.at[2])
    fc1_copy = pltpu.make_async_copy(wfc1, vfc1, wsem.at[1])
    proj_copy = pltpu.make_async_copy(wproj, vproj, wsem.at[0])
    fc2_copy.start()
    for chunk in range(3):
        d_load(0, chunk).start()
    fc1_copy.start()
    loads(0)[0].start()
    loads(0)[2].start()
    proj_copy.start()
    for group in range(2):
        p_load(0, group).start()
    qkv_copy(0, 0).start()
    qkv_copy(1, 1).start()
    for total in (sum1g, sum1b, sum2g, sum2b, sumproj, sumfc2, sumqkv, sumfc1):
        total[...] = jnp.zeros_like(total)
    everyone(stage, stages)

    def one_image(image, carry):
        slot = lax.rem(image, 2)
        more = image + 1 < images
        save_gy, save_mid, save_qkv = saves(image, slot)
        load_h, load_x, load_qkv = loads(image)
        top_copy(image, slot).wait()
        save_gy.start()

        @pl.when(image == 0)
        def _():
            fc2_copy.wait()
            fc1_copy.wait()

        @pl.when(image > 0)
        def _():
            for chunk in range(2):
                g_save(image, chunk).wait()

        acc[...] = jnp.zeros_like(acc)

        def fc2(chunk):
            lines = pl.ds(pl.multiple_of(chunk * CHUNK, CHUNK), CHUNK)
            abuf[lax.rem(chunk, 2)] = dot(gin[slot], vfc2[lines, :], 1, 1).astype(BF16)

        def fc1(chunk):
            columns = pl.ds(pl.multiple_of(chunk * CHUNK, CHUNK), CHUNK)
            slot2 = lax.rem(chunk, 2)
            pre = abuf[slot2].astype(F32) * dbuf[lax.rem(chunk, 3)]
            sumfc1[:, columns] += fold(pre)
            low = pre.astype(BF16)
            gbuf[slot2] = low
            acc[...] += dot(low, vfc1[:, columns], 1, 1)

        fc2(0)

        def mlp_step(chunk, carry):
            d_load(image, chunk - 1).wait()

            @pl.when(chunk >= 3)
            def _():
                g_save(image, chunk - 1).wait()

            fc2(chunk)
            fc1(chunk - 1)
            g_save(image, chunk - 1).start()

            @pl.when(chunk + 2 < chunks)
            def _():
                d_load(image, chunk + 2).start()

            return carry

        lax.fori_loop(1, chunks, mlp_step, 0)
        d_load(image, chunks - 1).wait()
        g_save(image, chunks - 1).wait()
        fc1(chunks - 1)
        g_save(image, chunks - 1).start()

        @pl.when(more)
        def _():
            for chunk in range(3):
                d_load(image + 1, chunk).start()

        load_h.wait()

        @pl.when(image > 0)
        def _():
            save_mid.wait()
            save_qkv.wait()

        def back2(lines):
            grad = acc[lines, :].astype(BF16).astype(F32)
            grad_in, by_unit = norm_backward(grad, hid[lines, :], g2[...])
            sum2g[...] += fold(by_unit)
            sum2b[...] += fold(grad)
            top = gin[slot, lines, :].astype(F32)
            sumfc2[...] += fold(top)
            low = (top + grad_in).astype(BF16)
            gmid[lines, :] = low
            sumproj[...] += fold(low.astype(F32))

        by_rows(rows, back2)
        save_mid.start()
        load_x.start()
        save_gy.wait()

        @pl.when(jnp.logical_and(is_last, image + 2 < images))
        def _():
            top_copy(image + 2, slot).start()

        @pl.when(jnp.logical_and(stage < stages - 1, image + 2 < images))
        def _():
            pl.semaphore_signal(free_sem, inc=1, device_id={"pp": lax.rem(stage + 1, stages)}, device_id_type=MESH)

        @pl.when(image == 0)
        def _():
            proj_copy.wait()

        gctx[...] = dot(gmid[...], vproj[...], 1, 1).astype(BF16)
        load_qkv.wait()
        for group in range(groups):
            p_load(image, group).wait()
            for inner in range(GROUP):
                at = (group * GROUP + inner) * head
                q = qkv[:, at:at + head]
                k = qkv[:, width + at:width + at + head]
                v = qkv[:, 2 * width + at:2 * width + at + head]
                grad = gctx[:, at:at + head]
                probs = pbuf[group % 2, inner]
                grad_probs = dot(v, grad, 1, 1)
                mean = jnp.sum(grad_probs * probs, axis=0, keepdims=True)
                low = (probs * (grad_probs - mean) * scale).astype(BF16)
                gqkv[:, at:at + head] = dot(low, k, 0, 0).astype(BF16)
                gqkv[:, width + at:width + at + head] = dot(low, q).astype(BF16)
                gqkv[:, 2 * width + at:2 * width + at + head] = dot(probs.astype(BF16), grad).astype(BF16)
            if group + 2 < groups:
                p_load(image, group + 2).start()
            else:
                @pl.when(more)
                def _():
                    p_load(image + 1, group + 2 - groups).start()
        save_qkv.start()

        @pl.when(more)
        def _():
            loads(image + 1)[2].start()

        def qkv_part(part, carry):
            index = image * 3 + part
            where = lax.rem(index, 2)
            qkv_copy(index, where).wait()
            columns = pl.ds(pl.multiple_of(part * width, 128), width)
            piece = gqkv[:, columns]
            sumqkv[:, columns] += fold(piece.astype(F32))
            acc[...] += dot(piece, vqkv[where])

            @pl.when(index + 2 < images * 3)
            def _():
                qkv_copy(index + 2, where).start()

            return carry

        acc[...] = jnp.zeros_like(acc)
        lax.fori_loop(0, 3, qkv_part, 0)
        load_x.wait()

        @pl.when(image > 0)
        def _():
            wait_sent(image)

        def back1(lines):
            grad = acc[lines, :].astype(BF16).astype(F32)
            grad_in, by_unit = norm_backward(grad, hid[lines, :], g1[...])
            sum1g[...] += fold(by_unit)
            sum1b[...] += fold(grad)
            gout[lines, :] = (gmid[lines, :].astype(F32) + grad_in).astype(BF16)

        by_rows(rows, back1)

        @pl.when(more)
        def _():
            loads(image + 1)[0].start()

        @pl.when(jnp.logical_and(jnp.logical_not(is_first), image >= 2))
        def _():
            pl.semaphore_wait(free_sem, 1)

        @pl.when(jnp.logical_not(is_first))
        def _():
            next_copy(slot).start()

        @pl.when(is_first)
        def _():
            for other in range(1, stages):
                emb_send(image, other).start()
            emb_local(image).start()

        return carry

    lax.fori_loop(0, images, one_image, 0)
    wait_sent(images - 1)
    _, save_mid, save_qkv = saves(images - 1, 0)
    save_mid.wait()
    save_qkv.wait()
    for chunk in range(2):
        g_save(images - 1, chunk).wait()

    @pl.when(jnp.logical_not(is_first))
    def _():
        pltpu.make_async_copy(gemb, gemb, emb_sem).wait()


ANY = pl.BlockSpec(memory_space=pl.ANY)
VMEM = pl.BlockSpec(memory_space=pltpu.VMEM)
LIMIT = 67_043_328
DMA = pltpu.SemaphoreType.DMA


def run_forward(dims, emb, wqkv, wproj, wfc1, wfc2, vectors):
    stages, images, tokens, heads, head = dims
    rows, width = emb.shape[1:]
    hidden = wfc1.shape[1]
    hbm = lambda *shape, dtype=BF16: jax.ShapeDtypeStruct((images, rows) + shape, dtype)
    return pl.pallas_call(
        functools.partial(forward_kernel, dims),
        out_shape=(
            hbm(width), hbm(width), hbm(3 * width), hbm(width), hbm(width), hbm(width), hbm(hidden, dtype=F32), hbm(hidden),
            jax.ShapeDtypeStruct((images, heads, rows, rows), F32), jax.ShapeDtypeStruct((images, 16, width), BF16)),
        in_specs=[ANY] * 5 + [VMEM] * 8,
        out_specs=(ANY,) * 10,
        scratch_shapes=[
            pltpu.VMEM((2, width, width), BF16), pltpu.VMEM(wproj.shape, BF16), pltpu.VMEM(wfc1.shape, BF16), pltpu.VMEM(wfc2.shape, BF16),
            pltpu.VMEM((2, rows, width), BF16), pltpu.VMEM((rows, width), BF16), pltpu.VMEM((rows, 3 * width), BF16),
            pltpu.VMEM((rows, width), BF16), pltpu.VMEM((rows, width), BF16), pltpu.VMEM((rows, width), F32),
            pltpu.VMEM((3, rows, CHUNK), F32), pltpu.VMEM((2, rows, CHUNK), BF16), pltpu.VMEM((2, GROUP, rows, rows), F32),
            pltpu.VMEM((rows, width), BF16), pltpu.VMEM((images, 16, width), BF16),
            DMA((3,)), DMA((2,)), DMA((2,)), DMA((stages,)), DMA(()), DMA((6,)), DMA((3,)), DMA((2,)), DMA((2,)),
            pltpu.SemaphoreType.REGULAR],
        compiler_params=pltpu.CompilerParams(collective_id=0, has_side_effects=True, vmem_limit_bytes=LIMIT),
        name="forward",
    )(emb, wqkv, wproj, wfc1, wfc2, *vectors)


def run_backward(dims, gtop, wqkv, wproj, wfc1, wfc2, g1, g2, x_s, qkv_s, h_s, d_s, p_s):
    stages, images, tokens, heads, head = dims
    rows, width = gtop.shape[1:]
    hidden = wfc1.shape[1]
    hbm = lambda *shape: jax.ShapeDtypeStruct((images, rows) + shape, BF16)
    total = lambda size: jax.ShapeDtypeStruct((8, size), F32)
    return pl.pallas_call(
        functools.partial(backward_kernel, dims),
        out_shape=(hbm(width), hbm(hidden), hbm(width), hbm(3 * width), hbm(width)) + (total(width),) * 6 + (total(3 * width), total(hidden)),
        in_specs=[ANY] * 5 + [VMEM] * 2 + [ANY] * 5,
        out_specs=(ANY,) * 5 + (VMEM,) * 8,
        scratch_shapes=[
            pltpu.VMEM((2, width, width), BF16), pltpu.VMEM(wproj.shape, BF16), pltpu.VMEM(wfc1.shape, BF16), pltpu.VMEM(wfc2.shape, BF16),
            pltpu.VMEM((2, rows, width), BF16), pltpu.VMEM((rows, width), F32), pltpu.VMEM((3, rows, CHUNK), F32),
            pltpu.VMEM((2, rows, CHUNK), BF16), pltpu.VMEM((2, rows, CHUNK), BF16),
            pltpu.VMEM((rows, width), BF16), pltpu.VMEM((rows, width), BF16), pltpu.VMEM((rows, width), BF16),
            pltpu.VMEM((rows, 3 * width), BF16), pltpu.VMEM((rows, 3 * width), BF16), pltpu.VMEM((2, GROUP, rows, rows), F32),
            pltpu.VMEM((rows, width), BF16),
            DMA((3,)), DMA((2,)), DMA((2,)), DMA((stages,)), DMA(()), DMA((4,)), DMA((3,)), DMA((3,)), DMA((2,)), DMA((2,)),
            pltpu.SemaphoreType.REGULAR],
        compiler_params=pltpu.CompilerParams(collective_id=1, has_side_effects=True, vmem_limit_bytes=LIMIT),
        name="backward",
    )(gtop, wqkv, wproj, wfc1, wfc2, g1, g2, x_s, qkv_s, h_s, d_s, p_s)


def matmul_rows(spec, left, right):
    return jnp.einsum(spec, left, right, preferred_element_type=F32)


def solution(mesh):
    stages = mesh.shape["pp"]
    in_specs = (P("dp"), P("dp"), P(), P(), P(), P()) + (P("pp"),) * 12 + (P(),) * 4
    out_specs = (P("dp"),) * 5 + (P(("dp", "pp")),) * 12 + (P("dp"),) * 4

    def body(patches, labels, w_patch, b_patch, cls_token, pos_embed, *rest):
        ln1_gain, ln1_bias, w_qkv, b_qkv, w_proj, b_proj, ln2_gain, ln2_bias, w_fc1, b_fc1, w_fc2, b_fc2 = (tensor[0] for tensor in rest[:12])
        lnf_gain, lnf_bias, w_head, b_head = rest[12:]
        tokens, width = pos_embed.shape
        heads, head = w_qkv.shape[2:]
        images = labels.size
        inv_count = 1.0 / images
        rows = -(-tokens // 16) * 16
        dims = (stages, images, tokens, heads, head)
        pad = ((0, 0), (0, rows - tokens), (0, 0))

        patch_rows = patches.reshape((images,) + patches.shape[2:])
        projected = matmul_rows("inp,pd->ind", patch_rows, w_patch) + b_patch.astype(F32)
        first = jnp.broadcast_to(cls_token.astype(F32), (images, 1, width))
        embedded = (jnp.concatenate([first, projected], axis=1) + pos_embed.astype(F32)).astype(BF16)
        embedded = jnp.pad(embedded, pad)

        line = lambda tensor: tensor.astype(F32).reshape(1, -1)
        wqkv_t = jnp.transpose(w_qkv, (1, 2, 3, 0)).reshape(3 * width, width)
        big = (wqkv_t, w_proj.reshape(width, width), w_fc1, w_fc2)
        vectors = tuple(map(line, (ln1_gain, ln1_bias, b_qkv, b_proj, ln2_gain, ln2_bias, b_fc1, b_fc2)))
        x_s, a_s, qkv_s, c_s, h_s, n_s, d_s, g_s, p_s, tops = run_forward(dims, embedded, *big, vectors)

        pooled, lnf_vjp = jax.vjp(layer_norm, tops[:, 0], lnf_gain.astype(F32), lnf_bias.astype(F32))
        logits = jnp.dot(pooled, w_head, preferred_element_type=F32) + b_head.astype(F32)
        classes = logits.shape[-1]
        log_probs = jax.nn.log_softmax(logits, axis=-1)
        target = (1.0 - SMOOTH) * jax.nn.one_hot(labels.reshape(-1), classes, dtype=F32) + SMOOTH / classes
        loss = -jnp.sum(target * log_probs) * inv_count
        grad_logits = (jnp.exp(log_probs) - target) * inv_count
        grad_low = grad_logits.astype(BF16)
        g_w_head = matmul_rows("bd,bc->dc", pooled, grad_low)
        g_b_head = jnp.sum(grad_logits, axis=0)
        grad_pooled = matmul_rows("bc,dc->bd", grad_low, w_head).astype(BF16)
        grad_tops, g_lnf_gain, g_lnf_bias = lnf_vjp(grad_pooled)
        gtop = jnp.pad(grad_tops[:, None], ((0, 0), (0, rows - 1), (0, 0)))

        gy_s, gpre_s, gmid_s, gqkv_s, gemb, *sums = run_backward(dims, gtop, *big, vectors[0], vectors[4], x_s, qkv_s, h_s, d_s, p_s)
        g_ln1_gain, g_ln1_bias, g_ln2_gain, g_ln2_bias, g_b_proj, g_b_fc2, g_b_qkv, g_b_fc1 = (jnp.sum(total, axis=0) for total in sums)

        flat = lambda array: array.reshape(images * rows, -1)
        g_w_qkv = matmul_rows("tn,td->nd", flat(gqkv_s), flat(a_s)).reshape(3, heads, head, width)
        layer_grads = (
            g_ln1_gain, g_ln1_bias, jnp.transpose(g_w_qkv, (3, 0, 1, 2)), g_b_qkv.reshape(3, heads, head),
            matmul_rows("tn,td->nd", flat(c_s), flat(gmid_s)).reshape(heads, head, width), g_b_proj,
            g_ln2_gain, g_ln2_bias,
            matmul_rows("tn,td->nd", flat(n_s), flat(gpre_s)), g_b_fc1,
            matmul_rows("tn,td->nd", flat(g_s), flat(gy_s)), g_b_fc2,
        )
        grad_embedded = gemb[:, :tokens]
        g_pos_embed = jnp.sum(grad_embedded.astype(F32), axis=0)
        embed_grads = (
            matmul_rows("inp,ind->pd", patch_rows, grad_embedded[:, 1:]),
            jnp.sum(g_pos_embed[1:], axis=0), g_pos_embed[0], g_pos_embed,
        )
        return (loss.reshape(1),) + embed_grads + tuple(grad[None] for grad in layer_grads) + (g_lnf_gain, g_lnf_bias, g_w_head, g_b_head)

    return jax.shard_map(body, mesh=mesh, in_specs=in_specs, out_specs=out_specs, check_vma=False)
```

```python
import functools
import math
import jax
import jax.numpy as jnp
from jax import lax
from jax.experimental import pallas as pl
from jax.experimental.pallas import tpu as pltpu
from jax.sharding import PartitionSpec as P

EPS = 1e-6
SMOOTH = 0.1
F32 = jnp.float32
BF16 = jnp.bfloat16
MESH = pl.DeviceIdType.MESH
LANES = 128
HALF = 384
CHUNK = 2 * HALF
GROUP = 4
BLOCK = 136


def layer_norm(hidden, gain, bias):
    values = hidden.astype(F32)
    centered = values - jnp.mean(values, axis=-1, keepdims=True)
    variance = jnp.mean(jnp.square(centered), axis=-1, keepdims=True)
    return (centered * lax.rsqrt(variance + EPS) * gain + bias).astype(BF16)


def dot(left, right, left_axis=1, right_axis=0):
    return lax.dot_general(left, right, (((left_axis,), (right_axis,)), ((), ())), preferred_element_type=F32)


def by_rows(rows, visit):
    def step(index, carry):
        visit(pl.ds(pl.multiple_of(index * BLOCK, BLOCK), BLOCK))
        return carry

    lax.fori_loop(0, rows // BLOCK, step, 0)
    if rows % BLOCK:
        visit(pl.ds(rows - rows % BLOCK, rows % BLOCK))


def fold(values):
    rows, columns = values.shape
    return jnp.sum(values.reshape(rows // 8, 8, columns), axis=0)


def everyone(stage, stages):
    barrier = pltpu.get_barrier_semaphore()
    for hop in range(1, stages):
        pl.semaphore_signal(barrier, inc=1, device_id={"pp": lax.rem(stage + hop, stages)}, device_id_type=MESH)
    pl.semaphore_wait(barrier, stages - 1)


def forward_kernel(dims, *refs):
    (emb, wqkv, wproj, wfc1, wfc2, *given,
     x_s, a_s, qkv_s, c_s, h_s, n_s, d_s, g_s, p_s, tops_out,
     vqkv, vproj, vfc1, vfc2, xin, act, qkv, mid, yacc, ubuf, gbuf, pbuf, tops,
     g1, b1, bqkv, bproj, g2, b2, bfc1, bfc2,
     wsem, qsem, recv_sem, send_sem, top_sem, save_sem, usem, gsem, psem, free_sem) = refs
    stages, images, tokens, heads, head = dims
    rows, width = mid.shape
    chunks = vfc1.shape[1] // CHUNK
    stage = lax.axis_index("pp")
    is_first = stage == 0
    is_last = stage == stages - 1
    scale2 = head ** -0.5 / math.log(2.0)


    def qkv_copy(index):
        slot = lax.rem(index, 2)
        lines = pl.ds(pl.multiple_of(lax.rem(index, 3) * width, 128), width)
        return pltpu.make_async_copy(wqkv.at[lines], vqkv.at[slot], qsem.at[slot])

    def emb_copy(image, slot):
        return pltpu.make_async_copy(emb.at[image], xin.at[slot], recv_sem.at[slot])

    qkv_copy(0).start()

    @pl.when(is_first)
    def _():
        emb_copy(0, 0).start()
        emb_copy(1, 1).start()

    qkv_copy(1).start()
    proj_copy = pltpu.make_async_copy(wproj, vproj, wsem.at[0])
    fc1_copy = pltpu.make_async_copy(wfc1, vfc1, wsem.at[1])
    fc2_copy = pltpu.make_async_copy(wfc2, vfc2, wsem.at[2])
    proj_copy.start()
    fc1_copy.start()
    fc2_copy.start()
    qkv[...] = jnp.zeros_like(qkv)
    for low, wide in zip(given, (g1, b1, bqkv, bproj, g2, b2, bfc1, bfc2)):
        wide[...] = low[...].astype(F32)
    everyone(stage, stages)

    def saves(image, slot):
        pairs = ((xin.at[slot], x_s), (act, a_s), (qkv, qkv_s), (act, c_s), (mid, h_s), (act, n_s))
        return [pltpu.make_async_copy(src, dst.at[image], save_sem.at[at]) for at, (src, dst) in enumerate(pairs)]

    class u_save:
        def __init__(self, image, chunk):
            slot = lax.rem(chunk, 3)
            self.copies = [
                pltpu.make_async_copy(ubuf.at[slot, :, pl.ds(side * HALF, HALF)], d_s.at[image, chunk * 2 + side], usem.at[slot, side])
                for side in range(2)]

        def start(self):
            for copy in self.copies:
                copy.start()

        def wait(self):
            for copy in self.copies:
                copy.wait()

    def g_save(image, chunk):
        slot = lax.rem(chunk, 2)
        return pltpu.make_async_copy(gbuf.at[slot], g_s.at[image, :, pl.ds(pl.multiple_of(chunk * CHUNK, CHUNK), CHUNK)], gsem.at[slot])

    def p_save(image, group):
        slot = group % 2
        return pltpu.make_async_copy(pbuf.at[slot], p_s.at[image, pl.ds(group * GROUP, GROUP)], psem.at[slot])

    def top_copy(image, other):
        return pltpu.make_async_remote_copy(
            src_ref=mid.at[pl.ds(0, 16)], dst_ref=tops.at[image], send_sem=send_sem.at[1 + other], recv_sem=top_sem,
            device_id={"pp": other}, device_id_type=MESH)

    def next_copy(image, slot):
        return pltpu.make_async_remote_copy(
            src_ref=mid, dst_ref=xin.at[slot], send_sem=send_sem.at[0], recv_sem=recv_sem.at[slot],
            device_id={"pp": lax.rem(stage + 1, stages)}, device_id_type=MESH)

    def wait_sent(image):
        @pl.when(jnp.logical_not(is_last))
        def _():
            next_copy(image, 0).wait_send()

        @pl.when(is_last)
        def _():
            for other in range(stages - 1):
                top_copy(image, other).wait_send()

    def one_image(image, carry):
        slot = lax.rem(image, 2)
        save_x, save_a, save_qkv, save_c, save_h, save_n = saves(image, slot)
        emb_copy(image, slot).wait()
        save_x.start()

        @pl.when(image > 0)
        def _():
            save_n.wait()
            save_qkv.wait()

        def norm1(lines):
            act[lines, :] = layer_norm(xin[slot, lines, :], g1[...], b1[...])

        by_rows(rows, norm1)
        save_a.start()

        def qkv_part(part, carry):
            index = image * 3 + part
            qkv_copy(index).wait()
            low = (dot(act[...], vqkv[lax.rem(index, 2)], 1, 1) + bqkv[part]).astype(BF16)
            for at in range(heads):
                lane = part * (heads * LANES) + at * LANES
                qkv[:, pl.ds(pl.multiple_of(lane, LANES), head)] = low[:, at * head:(at + 1) * head]

            @pl.when(index + 2 < images * 3)
            def _():
                qkv_copy(index + 2).start()

            return carry

        lax.fori_loop(0, 3, qkv_part, 0)
        save_qkv.start()

        save_a.wait()

        @pl.when(image > 0)
        def _():
            p_save(image, 0).wait()
            p_save(image, 1).wait()

        def scores_of(number):
            q, k = (qkv[:, lane:lane + LANES] for lane in (number * LANES, (heads + number) * LANES))
            return dot(k, q, 1, 1)

        def attend(number, scores):
            group, inner = number // GROUP, number % GROUP
            if group >= 2 and inner == 0:
                p_save(image, group).wait()
            v = qkv[:, (2 * heads + number) * LANES:(2 * heads + number + 1) * LANES]
            top, tail = scores[:tokens - 1], scores[tokens - 1:]
            most = jnp.maximum(jnp.max(top, axis=0, keepdims=True), tail[:1])
            top = jnp.exp2((top - most) * scale2)
            real = lax.broadcasted_iota(jnp.int32, tail.shape, 0) < 1
            tail = jnp.where(real, jnp.exp2(jnp.minimum(tail - most, 0.0) * scale2), 0.0)
            inv = 1.0 / (jnp.sum(top, axis=0, keepdims=True) + jnp.sum(tail, axis=0, keepdims=True))
            probs = jnp.concatenate([top, tail], axis=0) * inv
            pbuf[group % 2, inner, :, :rows] = probs
            act[:, number * head:(number + 1) * head] = dot(probs.astype(BF16), v, 0, 0).astype(BF16)[:, :head]
            if inner == GROUP - 1:
                p_save(image, group).start()

        scores = scores_of(0)
        for number in range(heads):
            later = scores_of(number + 1) if number + 1 < heads else None
            attend(number, scores)
            scores = later
        save_c.start()

        @pl.when(image == 0)
        def _():
            proj_copy.wait()

        @pl.when(image > 0)
        def _():
            wait_sent(image)

        mid[...] = (dot(act[...], vproj[...]) + bproj[...] + xin[slot].astype(F32)).astype(BF16)
        save_h.start()
        save_x.wait()

        @pl.when(jnp.logical_and(is_first, image + 2 < images))
        def _():
            emb_copy(image + 2, slot).start()

        @pl.when(jnp.logical_and(stage > 0, image + 2 < images))
        def _():
            pl.semaphore_signal(free_sem, inc=1, device_id={"pp": lax.rem(stage + stages - 1, stages)}, device_id_type=MESH)

        save_c.wait()

        def norm2(lines):
            hidden = mid[lines, :]
            act[lines, :] = layer_norm(hidden, g2[...], b2[...])
            yacc[lines, :] = hidden.astype(F32) + bfc2[...]

        by_rows(rows, norm2)
        save_n.start()

        @pl.when(image == 0)
        def _():
            fc1_copy.wait()
            fc2_copy.wait()

        @pl.when(image > 0)
        def _():
            for chunk in range(3):
                u_save(image, chunk).wait()
            for chunk in range(2):
                g_save(image, chunk).wait()

        def fc1(chunk):
            columns = pl.ds(pl.multiple_of(chunk * CHUNK, CHUNK), CHUNK)
            ubuf[lax.rem(chunk, 3)] = dot(act[...], vfc1[:, columns]) + bfc1[:, columns]

        def gelu(chunk):
            slot3, slot2 = lax.rem(chunk, 3), lax.rem(chunk, 2)
            pre = ubuf[slot3]
            cdf = 0.5 + 0.5 * lax.erf(pre * (0.5 ** 0.5))
            pdf = jnp.exp2(pre * pre * (-0.5 / math.log(2.0))) * ((2.0 * math.pi) ** -0.5)
            activ = (pre * cdf).astype(BF16)
            gbuf[slot2] = activ
            ubuf[slot3] = cdf + pre * pdf
            return activ

        def fc2(chunk, activ):
            yacc[...] += dot(activ, vfc2[pl.ds(pl.multiple_of(chunk * CHUNK, CHUNK), CHUNK), :])

        fc1(0)

        def mlp_step(chunk, carry):
            @pl.when(chunk >= 3)
            def _():
                u_save(image, chunk).wait()
                g_save(image, chunk - 1).wait()

            @pl.when(chunk >= 2)
            def _():
                u_save(image, chunk - 2).start()
                g_save(image, chunk - 2).start()

            activ = gelu(chunk - 1)
            fc1(chunk)
            fc2(chunk - 1, activ)
            return carry

        lax.fori_loop(1, chunks, mlp_step, 0)
        g_save(image, chunks - 1).wait()
        u_save(image, chunks - 2).start()
        g_save(image, chunks - 2).start()
        fc2(chunks - 1, gelu(chunks - 1))
        u_save(image, chunks - 1).start()
        g_save(image, chunks - 1).start()

        save_h.wait()
        mid[...] = yacc[...].astype(BF16)

        @pl.when(jnp.logical_and(jnp.logical_not(is_last), image >= 2))
        def _():
            pl.semaphore_wait(free_sem, 1)

        @pl.when(jnp.logical_not(is_last))
        def _():
            next_copy(image, slot).start()

        @pl.when(is_last)
        def _():
            for other in range(stages - 1):
                top_copy(image, other).start()
            tops[image] = mid[pl.ds(0, 16), :]

        return carry

    lax.fori_loop(0, images, one_image, 0)
    wait_sent(images - 1)
    _, _, save_qkv, _, _, save_n = saves(images - 1, 0)
    save_qkv.wait()
    save_n.wait()
    for chunk in range(3):
        u_save(images - 1, chunk).wait()
    for chunk in range(2):
        g_save(images - 1, chunk).wait()
        p_save(images - 1, chunk).wait()

    @pl.when(jnp.logical_not(is_last))
    def _():
        pltpu.make_async_copy(tops, tops, top_sem).wait()

    for image in range(images):
        tops_out[image:image + 1, :] = tops[image, 0:1, :]


def norm_backward(grad, hidden, gain):
    values = hidden.astype(F32)
    centered = values - jnp.mean(values, axis=-1, keepdims=True)
    inv = lax.rsqrt(jnp.mean(jnp.square(centered), axis=-1, keepdims=True) + EPS)
    unit = centered * inv
    scaled = grad * gain
    grad_in = inv * (scaled - jnp.mean(scaled, axis=-1, keepdims=True) - unit * jnp.mean(scaled * unit, axis=-1, keepdims=True))
    return grad_in, grad * unit


def backward_kernel(dims, *refs):
    (gtop, wqkv, wproj, wfc1, wfc2, low1, low2, x_s, qkv_s, h_s, d_s, p_s,
     gy_s, gpre_s, gmid_s, gqkv_s, gemb, *sums_out,
     vqkv, vproj, vfc1, vfc2, gin, acc, shared, abuf, gbuf, hid, gmid, gctx, qkv, gqkv, gout, g1, g2,
     sum1g, sum1b, sum2g, sum2b, sumproj, sumfc2, sumqkv, sumfc1,
     wsem, qsem, recv_sem, top_sem, send_sem, emb_sem, save_sem, load_sem, dsem, gsem, psem, free_sem) = refs
    stages, images, tokens, heads, head = dims
    rows, width = gmid.shape
    chunks = vfc1.shape[1] // CHUNK
    groups = heads // GROUP
    stage = lax.axis_index("pp")
    is_first = stage == 0
    is_last = stage == stages - 1
    scale = head ** -0.5

    pieces = ((0, vqkv.shape[1]), (vqkv.shape[1], width - vqkv.shape[1]))

    def qkv_copy(part, side):
        slot = lax.rem(part * 2 + side, 3)
        at, size = pieces[side]
        lines = pl.ds(pl.multiple_of(lax.rem(part, 3) * width + at, 128), size)
        return pltpu.make_async_copy(wqkv.at[lines], vqkv.at[slot, pl.ds(0, size)], qsem.at[slot])

    def top_copy(image, slot):
        return pltpu.make_async_copy(gtop.at[image], gin.at[slot, pl.ds(0, 16)], top_sem.at[slot])

    def d_load(image, chunk):
        slot = lax.rem(chunk, 4)
        return pltpu.make_async_copy(d_s.at[image, pl.ds(chunk * 2, 2)], shared.at[pl.ds(slot * 2, 2)], dsem.at[slot])

    def g_save(image, chunk):
        slot = lax.rem(chunk, 2)
        return pltpu.make_async_copy(gbuf.at[slot], gpre_s.at[image, :, pl.ds(pl.multiple_of(chunk * CHUNK, CHUNK), CHUNK)], gsem.at[slot])

    def p_load(image, group):
        slot = group % 2
        return pltpu.make_async_copy(p_s.at[image, pl.ds(group * GROUP, GROUP)], shared.at[pl.ds(slot * GROUP, GROUP)], psem.at[slot])

    def saves(image, slot):
        pairs = ((gin.at[slot], gy_s), (gmid, gmid_s), (gqkv, gqkv_s))
        return [pltpu.make_async_copy(src, dst.at[image], save_sem.at[at]) for at, (src, dst) in enumerate(pairs)]

    def loads(image):
        pairs = ((h_s, hid), (x_s, hid), (qkv_s, qkv))
        return [pltpu.make_async_copy(src.at[image], dst, load_sem.at[at]) for at, (src, dst) in enumerate(pairs)]

    def next_copy(slot):
        return pltpu.make_async_remote_copy(
            src_ref=gout, dst_ref=gin.at[slot], send_sem=send_sem.at[0], recv_sem=recv_sem.at[slot],
            device_id={"pp": lax.rem(stage + stages - 1, stages)}, device_id_type=MESH)

    def emb_send(image, other):
        return pltpu.make_async_remote_copy(
            src_ref=gout, dst_ref=gemb.at[image], send_sem=send_sem.at[other], recv_sem=emb_sem,
            device_id={"pp": other}, device_id_type=MESH)

    def emb_local(image):
        return pltpu.make_async_copy(gout, gemb.at[image], save_sem.at[3])

    def wait_sent(image):
        @pl.when(jnp.logical_not(is_first))
        def _():
            next_copy(0).wait_send()

        @pl.when(is_first)
        def _():
            for other in range(1, stages):
                emb_send(image, other).wait_send()
            emb_local(image).wait()

    @pl.when(is_last)
    def _():
        gin[...] = jnp.zeros_like(gin)
        top_copy(0, 0).start()
        top_copy(1, 1).start()

    fc2_copy = pltpu.make_async_copy(wfc2, vfc2, wsem.at[2])
    fc1_copy = pltpu.make_async_copy(wfc1, vfc1, wsem.at[1])
    proj_copy = pltpu.make_async_copy(wproj, vproj, wsem.at[0])
    fc2_copy.start()
    for chunk in range(4):
        d_load(0, chunk).start()
    fc1_copy.start()
    loads(0)[0].start()
    loads(0)[2].start()
    proj_copy.start()
    qkv_copy(0, 0).start()
    qkv_copy(0, 1).start()
    qkv_copy(1, 0).start()
    gctx[...] = jnp.zeros_like(gctx)
    sums_out, totals = sums_out[:8], (sum1g, sum1b, sum2g, sum2b, sumproj, sumfc2, sumqkv, sumfc1)
    for total in totals:
        total[...] = jnp.zeros_like(total)
    g1[...] = low1[...].astype(F32)
    g2[...] = low2[...].astype(F32)
    everyone(stage, stages)

    def one_image(image, carry):
        slot = lax.rem(image, 2)
        more = image + 1 < images
        save_gy, save_mid, save_qkv = saves(image, slot)
        load_h, load_x, load_qkv = loads(image)

        @pl.when(is_last)
        def _():
            top_copy(image, slot).wait()

        @pl.when(jnp.logical_not(is_last))
        def _():
            next_copy(slot).wait_recv()

        save_gy.start()

        @pl.when(image == 0)
        def _():
            fc2_copy.wait()
            fc1_copy.wait()

        @pl.when(image > 0)
        def _():
            for chunk in range(2):
                g_save(image, chunk).wait()

        acc[...] = jnp.zeros_like(acc)

        def fc2(chunk):
            lines = pl.ds(pl.multiple_of(chunk * CHUNK, CHUNK), CHUNK)
            abuf[lax.rem(chunk, 2)] = dot(gin[slot], vfc2[lines, :], 1, 1).astype(BF16)

        def gelu(chunk):
            columns = pl.ds(pl.multiple_of(chunk * CHUNK, CHUNK), CHUNK)
            slot2 = lax.rem(chunk, 2)
            slot4 = lax.rem(chunk, 4)
            pre = abuf[slot2].astype(F32) * jnp.concatenate([shared[slot4 * 2], shared[slot4 * 2 + 1]], axis=1)
            sumfc1[:, columns] += fold(pre)
            low = pre.astype(BF16)
            gbuf[slot2] = low
            return low

        def fc1(chunk, low):
            columns = pl.ds(pl.multiple_of(chunk * CHUNK, CHUNK), CHUNK)
            acc[...] += dot(low, vfc1[:, columns], 1, 1)

        fc2(0)

        def mlp_step(chunk, carry):
            d_load(image, chunk - 1).wait()

            @pl.when(chunk >= 3)
            def _():
                g_save(image, chunk - 1).wait()

            @pl.when(chunk >= 2)
            def _():
                g_save(image, chunk - 2).start()

                @pl.when(chunk + 2 < chunks)
                def _():
                    d_load(image, chunk + 2).start()

            low = gelu(chunk - 1)
            fc2(chunk)
            fc1(chunk - 1, low)
            return carry

        lax.fori_loop(1, chunks, mlp_step, 0)
        d_load(image, chunks - 1).wait()
        g_save(image, chunks - 1).wait()
        g_save(image, chunks - 2).start()
        fc1(chunks - 1, gelu(chunks - 1))
        g_save(image, chunks - 1).start()

        for group in range(2):
            p_load(image, group).start()
        load_h.wait()

        @pl.when(image > 0)
        def _():
            save_mid.wait()
            save_qkv.wait()

        def back2(lines):
            grad = acc[lines, :].astype(BF16).astype(F32)
            grad_in, by_unit = norm_backward(grad, hid[lines, :], g2[...])
            sum2g[...] += fold(by_unit)
            sum2b[...] += fold(grad)
            top = gin[slot, lines, :].astype(F32)
            sumfc2[...] += fold(top)
            low = (top + grad_in).astype(BF16)
            gmid[lines, :] = low
            sumproj[...] += fold(low.astype(F32))

        by_rows(rows, back2)
        save_mid.start()
        load_x.start()
        save_gy.wait()

        @pl.when(jnp.logical_and(is_last, image + 2 < images))
        def _():
            top_copy(image + 2, slot).start()

        @pl.when(jnp.logical_and(stage < stages - 1, image + 2 < images))
        def _():
            pl.semaphore_signal(free_sem, inc=1, device_id={"pp": lax.rem(stage + 1, stages)}, device_id_type=MESH)

        @pl.when(image == 0)
        def _():
            proj_copy.wait()

        low = dot(gmid[...], vproj[...], 1, 1).astype(BF16)
        for number in range(heads):
            gctx[:, number * LANES:number * LANES + head] = low[:, number * head:(number + 1) * head]
        load_qkv.wait()
        def lanes_of(number):
            return slice(number * LANES, (number + 1) * LANES)

        def grad_probs_of(number):
            return dot(qkv[:, lanes_of(2 * heads + number)], gctx[:, lanes_of(number)], 1, 1)

        def attend(number, grad_probs):
            group, inner = number // GROUP, number % GROUP
            if inner == 0:
                p_load(image, group).wait()
            probs = shared[group % 2 * GROUP + inner, :, :rows]
            at = number * head
            mean = jnp.sum(grad_probs * probs, axis=0, keepdims=True)
            low = (probs * (grad_probs - mean) * scale).astype(BF16)
            value = dot(probs.astype(BF16), gctx[:, lanes_of(number)]).astype(BF16)
            gqkv[:, 2 * width + at:2 * width + at + head] = value[:, :head]
            key = dot(low, qkv[:, lanes_of(number)]).astype(BF16)
            gqkv[:, width + at:width + at + head] = key[:, :head]
            query = dot(low, qkv[:, lanes_of(heads + number)], 0, 0).astype(BF16)
            gqkv[:, at:at + head] = query[:, :head]

        def refill(group):
            if group + 2 < groups:
                p_load(image, group + 2).start()
            else:
                @pl.when(more)
                def _():
                    for chunk in range((group + 2 - groups) * 2, (group + 2 - groups) * 2 + 2):
                        d_load(image + 1, chunk).start()

        grad_probs = grad_probs_of(0)
        for number in range(heads):
            later = grad_probs_of(number + 1) if number + 1 < heads else None
            attend(number, grad_probs)
            grad_probs = later
            if number % GROUP == GROUP - 1:
                refill(number // GROUP)
        save_qkv.start()

        @pl.when(more)
        def _():
            loads(image + 1)[2].start()

        def qkv_part(part, carry):
            for side in range(2):
                at, size = pieces[side]
                index = image * 3 + part
                qkv_copy(index, side).wait()
                columns = pl.ds(pl.multiple_of(part * width + at, 128), size)
                piece = gqkv[:, columns]
                sumqkv[:, columns] += fold(piece.astype(F32))
                acc[...] += dot(piece, vqkv[lax.rem(index * 2 + side, 3), :size])

                @pl.when(index + 1 + side < images * 3)
                def _():
                    qkv_copy(index + 1 + side, 1 - side).start()

            return carry

        acc[...] = jnp.zeros_like(acc)
        lax.fori_loop(0, 3, qkv_part, 0)
        load_x.wait()

        @pl.when(image > 0)
        def _():
            wait_sent(image)

        def back1(lines):
            grad = acc[lines, :].astype(BF16).astype(F32)
            grad_in, by_unit = norm_backward(grad, hid[lines, :], g1[...])
            sum1g[...] += fold(by_unit)
            sum1b[...] += fold(grad)
            gout[lines, :] = (gmid[lines, :].astype(F32) + grad_in).astype(BF16)

        by_rows(rows, back1)

        @pl.when(more)
        def _():
            loads(image + 1)[0].start()

        @pl.when(jnp.logical_and(jnp.logical_not(is_first), image >= 2))
        def _():
            pl.semaphore_wait(free_sem, 1)

        @pl.when(jnp.logical_not(is_first))
        def _():
            next_copy(slot).start()

        @pl.when(is_first)
        def _():
            for other in range(1, stages):
                emb_send(image, other).start()
            emb_local(image).start()

        return carry

    lax.fori_loop(0, images, one_image, 0)
    wait_sent(images - 1)
    _, save_mid, save_qkv = saves(images - 1, 0)
    save_mid.wait()
    save_qkv.wait()
    for chunk in range(2):
        g_save(images - 1, chunk).wait()

    for out, total in zip(sums_out, totals):
        out[...] = jnp.sum(total[...], axis=0, keepdims=True)

    @pl.when(jnp.logical_not(is_first))
    def _():
        pltpu.make_async_copy(gemb, gemb, emb_sem).wait()


ANY = pl.BlockSpec(memory_space=pl.ANY)
VMEM = pl.BlockSpec(memory_space=pltpu.VMEM)
LIMIT = 67_043_328
DMA = pltpu.SemaphoreType.DMA


def run_forward(dims, emb, wqkv, wproj, wfc1, wfc2, vectors):
    stages, images, tokens, heads, head = dims
    rows, width = emb.shape[1:]
    hidden = wfc1.shape[1]
    hbm = lambda *shape, dtype=BF16: jax.ShapeDtypeStruct((images, rows) + shape, dtype)
    return pl.pallas_call(
        functools.partial(forward_kernel, dims),
        out_shape=(
            hbm(width), hbm(width), hbm(3 * heads * LANES), hbm(width), hbm(width), hbm(width),
            jax.ShapeDtypeStruct((images, hidden // HALF, rows, HALF), F32), hbm(hidden),
            jax.ShapeDtypeStruct((images, heads, rows, HALF), F32), jax.ShapeDtypeStruct((images, width), BF16)),
        in_specs=[ANY] * 5 + [VMEM] * 8,
        out_specs=(ANY,) * 9 + (VMEM,),
        scratch_shapes=[
            pltpu.VMEM((2, width, width), BF16), pltpu.VMEM(wproj.shape, BF16), pltpu.VMEM(wfc1.shape, BF16), pltpu.VMEM(wfc2.shape, BF16),
            pltpu.VMEM((2, rows, width), BF16), pltpu.VMEM((rows, width), BF16), pltpu.VMEM((rows, 3 * heads * LANES), BF16),
            pltpu.VMEM((rows, width), BF16), pltpu.VMEM((rows, width), F32),
            pltpu.VMEM((3, rows, CHUNK), F32), pltpu.VMEM((2, rows, CHUNK), BF16), pltpu.VMEM((2, GROUP, rows, HALF), F32),
            pltpu.VMEM((images, 16, width), BF16),
            *(pltpu.VMEM(vector.shape, F32) for vector in vectors),
            DMA((3,)), DMA((2,)), DMA((2,)), DMA((stages,)), DMA(()), DMA((6,)), DMA((3, 2)), DMA((2,)), DMA((2,)),
            pltpu.SemaphoreType.REGULAR],
        compiler_params=pltpu.CompilerParams(collective_id=0, has_side_effects=True, vmem_limit_bytes=LIMIT),
        name="forward",
    )(emb, wqkv, wproj, wfc1, wfc2, *vectors)


def run_backward(dims, gtop, wqkv, wproj, wfc1, wfc2, g1, g2, x_s, qkv_s, h_s, d_s, p_s):
    stages, images, tokens, heads, head = dims
    rows, width = x_s.shape[1:]
    hidden = wfc1.shape[1]
    hbm = lambda *shape: jax.ShapeDtypeStruct((images, rows) + shape, BF16)
    sizes = (width,) * 6 + (3 * width, hidden)
    return pl.pallas_call(
        functools.partial(backward_kernel, dims),
        out_shape=(hbm(width), hbm(hidden), hbm(width), hbm(3 * width), hbm(width)) + tuple(jax.ShapeDtypeStruct((1, size), F32) for size in sizes),
        in_specs=[ANY] * 5 + [VMEM] * 2 + [ANY] * 5,
        out_specs=(ANY,) * 5 + (VMEM,) * 8,
        scratch_shapes=[
            pltpu.VMEM((3, -(-width // 256) * LANES, width), BF16), pltpu.VMEM(wproj.shape, BF16), pltpu.VMEM(wfc1.shape, BF16), pltpu.VMEM(wfc2.shape, BF16),
            pltpu.VMEM((2, rows, width), BF16), pltpu.VMEM((rows, width), F32), pltpu.VMEM((2 * GROUP, rows, HALF), F32),
            pltpu.VMEM((2, rows, CHUNK), BF16), pltpu.VMEM((2, rows, CHUNK), BF16),
            pltpu.VMEM((rows, width), BF16), pltpu.VMEM((rows, width), BF16), pltpu.VMEM((rows, heads * LANES), BF16),
            pltpu.VMEM((rows, 3 * heads * LANES), BF16), pltpu.VMEM((rows, 3 * width), BF16),
            pltpu.VMEM((rows, width), BF16), pltpu.VMEM((1, width), F32), pltpu.VMEM((1, width), F32),
            *(pltpu.VMEM((8, size), F32) for size in sizes),
            DMA((3,)), DMA((3,)), DMA((2,)), DMA((2,)), DMA((stages,)), DMA(()), DMA((4,)), DMA((3,)), DMA((4,)), DMA((2,)), DMA((2,)),
            pltpu.SemaphoreType.REGULAR],
        compiler_params=pltpu.CompilerParams(collective_id=1, has_side_effects=True, vmem_limit_bytes=LIMIT),
        name="backward",
    )(gtop, wqkv, wproj, wfc1, wfc2, g1, g2, x_s, qkv_s, h_s, d_s, p_s)


def head_kernel(inv_count, tops, labels, gain, bias, w_head, b_head, loss, gtop, g_gain, g_bias, g_w_head, g_b_head):
    images, width = tops.shape
    wide_gain = gain[...].astype(F32)
    pooled = layer_norm(tops[...], wide_gain, bias[...].astype(F32))
    logits = dot(pooled, w_head[...], 1, 1) + b_head[...].astype(F32)
    shifted = logits - jnp.max(logits, axis=-1, keepdims=True)
    log_probs = shifted - jnp.log(jnp.sum(jnp.exp(shifted), axis=-1, keepdims=True))
    classes = logits.shape[-1]
    line = lax.broadcasted_iota(jnp.int32, (images, 1), 0)
    label = jnp.zeros((images, 1), jnp.int32)
    for image in range(images):
        label = jnp.where(line == image, labels[image // labels.shape[1], image % labels.shape[1]], label)
    chosen = (lax.broadcasted_iota(jnp.int32, logits.shape, 1) == label).astype(F32)
    target = (1.0 - SMOOTH) * chosen + SMOOTH / classes
    parts = jnp.sum(target * log_probs, axis=-1, keepdims=True)
    loss[...] = -jnp.sum(parts, axis=0, keepdims=True) * inv_count
    grad_logits = (jnp.exp(log_probs) - target) * inv_count
    low = grad_logits.astype(BF16)
    g_w_head[...] = dot(low, pooled, 0, 0)
    g_b_head[...] = jnp.sum(grad_logits, axis=0, keepdims=True)
    grad = dot(low, w_head[...]).astype(BF16).astype(F32)
    grad_in, by_unit = norm_backward(grad, tops[...], wide_gain)
    g_gain[...] = jnp.sum(by_unit, axis=0, keepdims=True)
    g_bias[...] = jnp.sum(grad, axis=0, keepdims=True)
    gtop[...] = jnp.zeros_like(gtop)
    for image in range(images):
        gtop[image, 0:1, :] = grad_in[image:image + 1].astype(BF16)


def run_head(inv_count, tops, labels, gain, bias, w_head, b_head):
    images, width = tops.shape
    classes = w_head.shape[0]
    shape = lambda *dims, dtype=F32: jax.ShapeDtypeStruct(dims, dtype)
    return pl.pallas_call(
        functools.partial(head_kernel, inv_count),
        out_shape=(shape(1, 1), shape(images, 16, width, dtype=BF16), shape(1, width), shape(1, width), shape(classes, width), shape(1, classes)),
        in_specs=[VMEM, pl.BlockSpec(memory_space=pltpu.SMEM)] + [VMEM] * 4,
        out_specs=(VMEM,) * 6,
        compiler_params=pltpu.CompilerParams(vmem_limit_bytes=LIMIT),
        name="head",
    )(tops, labels, gain, bias, w_head, b_head)


def outer_kernel(left, right, out):
    out[...] = dot(left[...], right[...], 0, 0)


def outer_by_left(left, right, block):
    rows, size = left.shape
    width = right.shape[1]
    return pl.pallas_call(
        outer_kernel,
        out_shape=jax.ShapeDtypeStruct((size, width), F32),
        grid=(size // block,),
        in_specs=[pl.BlockSpec((rows, block), lambda at: (0, at)), pl.BlockSpec((rows, width), lambda at: (0, 0))],
        out_specs=pl.BlockSpec((block, width), lambda at: (at, 0)),
        compiler_params=pltpu.CompilerParams(vmem_limit_bytes=LIMIT),
        cost_estimate=pl.CostEstimate(flops=2 * rows * size * width, bytes_accessed=2 * rows * (size + width) + 4 * size * width, transcendentals=0),
        name="outer_left",
    )(left, right)


def outer_right_kernel(left, right, *refs):
    count = len(refs) // 2 - 1
    sums, out, sums_out, turned = refs[:count], refs[count], refs[count + 1:-1], refs[-1]

    @pl.when(pl.program_id(0) == 0)
    def _():
        turned[...] = left[...].T
        for given, passed in zip(sums, sums_out):
            passed[...] = given[...]

    out[...] = dot(turned[...], right[...])


def outer_by_right(left, right, block, sums):
    rows, size = left.shape
    width = right.shape[1]
    return pl.pallas_call(
        outer_right_kernel,
        out_shape=(jax.ShapeDtypeStruct((size, width), F32),) + tuple(jax.ShapeDtypeStruct(total.shape, F32) for total in sums),
        grid=(width // block,),
        in_specs=[pl.BlockSpec((rows, size), lambda at: (0, 0)), pl.BlockSpec((rows, block), lambda at: (0, at))] + [VMEM] * len(sums),
        out_specs=(pl.BlockSpec((size, block), lambda at: (0, at)),) + (VMEM,) * len(sums),
        scratch_shapes=[pltpu.VMEM((size, rows), BF16)],
        compiler_params=pltpu.CompilerParams(vmem_limit_bytes=LIMIT),
        cost_estimate=pl.CostEstimate(flops=2 * rows * size * width, bytes_accessed=2 * rows * (size + width) + 4 * size * width, transcendentals=0),
        name="outer_right",
    )(left, right, *sums)


def matmul_rows(spec, left, right):
    return jnp.einsum(spec, left, right, preferred_element_type=F32)


def solution(mesh):
    stages = mesh.shape["pp"]
    in_specs = (P("dp"), P("dp"), P(), P(), P(), P()) + (P("pp"),) * 12 + (P(),) * 4
    out_specs = (P("dp"),) * 5 + (P(("dp", "pp")),) * 12 + (P("dp"),) * 4

    def body(patches, labels, w_patch, b_patch, cls_token, pos_embed, *rest):
        ln1_gain, ln1_bias, w_qkv, b_qkv, w_proj, b_proj, ln2_gain, ln2_bias, w_fc1, b_fc1, w_fc2, b_fc2 = (tensor[0] for tensor in rest[:12])
        lnf_gain, lnf_bias, w_head, b_head = rest[12:]
        tokens, width = pos_embed.shape
        heads, head = w_qkv.shape[2:]
        images = labels.size
        inv_count = 1.0 / images
        rows = -(-tokens // 16) * 16
        dims = (stages, images, tokens, heads, head)

        patch_rows = jnp.pad(patches.reshape((images,) + patches.shape[2:]), ((0, 0), (1, rows - tokens), (0, 0)))
        is_patch = lax.broadcasted_iota(jnp.int32, (rows, 1), 0) > 0
        base = jnp.pad(pos_embed, ((0, rows - tokens), (0, 0))).astype(F32) + jnp.where(is_patch, b_patch.astype(F32), cls_token.astype(F32))
        embedded = (matmul_rows("inp,pd->ind", patch_rows, w_patch) + base).astype(BF16)

        line = lambda tensor: tensor.reshape(1, -1)
        wqkv_t = jnp.transpose(w_qkv, (1, 2, 3, 0)).reshape(3 * width, width)
        big = (wqkv_t, w_proj.reshape(width, width), w_fc1, w_fc2)
        vectors = tuple(map(line, (ln1_gain, ln1_bias, b_qkv, b_proj, ln2_gain, ln2_bias, b_fc1, b_fc2)))
        vectors = vectors[:2] + (vectors[2].reshape(3, 1, width),) + vectors[3:]
        x_s, a_s, qkv_s, c_s, h_s, n_s, d_s, g_s, p_s, tops = run_forward(dims, embedded, *big, vectors)

        row = lambda tensor: tensor.reshape(1, -1)
        loss, gtop, g_lnf_gain, g_lnf_bias, g_w_head, g_b_head = run_head(
            inv_count, tops, labels, row(lnf_gain), row(lnf_bias), jnp.transpose(w_head), row(b_head))

        gy_s, gpre_s, gmid_s, gqkv_s, gemb, *sums = run_backward(dims, gtop, *big, vectors[0], vectors[4], x_s, qkv_s, h_s, d_s, p_s)
        flat = lambda array: array.reshape(images * rows, -1)
        g_w_fc1, *sums = outer_by_right(flat(n_s), flat(gpre_s), 4 * LANES, sums)
        g_ln1_gain, g_ln1_bias, g_ln2_gain, g_ln2_bias, g_b_proj, g_b_fc2, g_b_qkv, g_b_fc1 = sums
        g_w_qkv = outer_by_left(flat(gqkv_s), flat(a_s), 3 * LANES).reshape(3, heads, head, width)
        layer_grads = (
            g_ln1_gain, g_ln1_bias, jnp.transpose(g_w_qkv, (3, 0, 1, 2))[None], g_b_qkv.reshape(1, 3, heads, head),
            outer_by_left(flat(c_s), flat(gmid_s), LANES).reshape(1, heads, head, width), g_b_proj,
            g_ln2_gain, g_ln2_bias,
            g_w_fc1[None], g_b_fc1,
            outer_by_left(flat(g_s), flat(gy_s), 4 * LANES)[None], g_b_fc2,
        )
        g_pos_embed = jnp.sum(gemb[:, :tokens].astype(F32), axis=0)
        embed_grads = (
            matmul_rows("tp,td->pd", flat(patch_rows), flat(gemb)),
            jnp.sum(g_pos_embed[1:], axis=0), g_pos_embed[0], g_pos_embed,
        )
        return (loss.reshape(1),) + embed_grads + layer_grads + (g_lnf_gain[0], g_lnf_bias[0], jnp.transpose(g_w_head), g_b_head[0])

    return jax.shard_map(body, mesh=mesh, in_specs=in_specs, out_specs=out_specs, check_vma=False)
```

```python
import functools
import math
import jax
import jax.numpy as jnp
from jax import lax
from jax.experimental import pallas as pl
from jax.experimental.pallas import tpu as pltpu
from jax.sharding import PartitionSpec as P

EPS = 1e-6
SMOOTH = 0.1
F32 = jnp.float32
BF16 = jnp.bfloat16
MESH = pl.DeviceIdType.MESH
LANES = 128
HALF = 384
CHUNK = 2 * HALF
GROUP = 4
BLOCK = 136


def layer_norm(hidden, gain, bias):
    values = hidden.astype(F32)
    centered = values - jnp.mean(values, axis=-1, keepdims=True)
    variance = jnp.mean(jnp.square(centered), axis=-1, keepdims=True)
    return (centered * lax.rsqrt(variance + EPS) * gain + bias).astype(BF16)


def dot(left, right, left_axis=1, right_axis=0):
    return lax.dot_general(left, right, (((left_axis,), (right_axis,)), ((), ())), preferred_element_type=F32)


def by_rows(rows, visit):
    def step(index, carry):
        visit(pl.ds(pl.multiple_of(index * BLOCK, BLOCK), BLOCK))
        return carry

    lax.fori_loop(0, rows // BLOCK, step, 0)
    if rows % BLOCK:
        visit(pl.ds(rows - rows % BLOCK, rows % BLOCK))


def fold(values):
    rows, columns = values.shape
    return jnp.sum(values.reshape(rows // 8, 8, columns), axis=0)


def everyone(stage, stages):
    barrier = pltpu.get_barrier_semaphore()
    for hop in range(1, stages):
        pl.semaphore_signal(barrier, inc=1, device_id={"pp": lax.rem(stage + hop, stages)}, device_id_type=MESH)
    pl.semaphore_wait(barrier, stages - 1)


def forward_kernel(dims, *refs):
    (emb, wqkv, wproj, wfc1, wfc2, *given,
     x_s, a_s, qkv_s, c_s, h_s, n_s, d_s, g_s, p_s, tops_out,
     vqkv, vproj, vfc1, vfc2, xin, act, qkv, mid, yacc, ubuf, gbuf, pbuf, tops,
     g1, b1, bqkv, bproj, g2, b2, bfc1, bfc2,
     wsem, qsem, recv_sem, send_sem, top_sem, save_sem, usem, gsem, psem, free_sem) = refs
    stages, images, tokens, heads, head = dims
    rows, width = mid.shape
    chunks = vfc1.shape[1] // CHUNK
    stage = lax.axis_index("pp")
    is_first = stage == 0
    is_last = stage == stages - 1
    scale2 = head ** -0.5 / math.log(2.0)


    def qkv_copy(index):
        slot = lax.rem(index, 2)
        lines = pl.ds(pl.multiple_of(lax.rem(index, 3) * width, 128), width)
        return pltpu.make_async_copy(wqkv.at[lines], vqkv.at[slot], qsem.at[slot])

    def emb_copy(image, slot):
        return pltpu.make_async_copy(emb.at[image], xin.at[slot], recv_sem.at[slot])

    @pl.when(is_first)
    def _():
        emb_copy(0, 0).start()

    qkv_copy(0).start()

    @pl.when(is_first)
    def _():
        emb_copy(1, 1).start()

    qkv_copy(1).start()
    proj_copy = pltpu.make_async_copy(wproj, vproj, wsem.at[0])
    fc1_copy = pltpu.make_async_copy(wfc1, vfc1, wsem.at[1])
    fc2_copy = pltpu.make_async_copy(wfc2, vfc2, wsem.at[2])
    qkv[...] = jnp.zeros_like(qkv)
    for low, wide in zip(given, (g1, b1, bqkv, bproj, g2, b2, bfc1, bfc2)):
        wide[...] = low[...].astype(F32)
    everyone(stage, stages)

    def saves(image, slot):
        pairs = ((xin.at[slot], x_s), (act, a_s), (qkv, qkv_s), (act, c_s), (mid, h_s), (act, n_s))
        return [pltpu.make_async_copy(src, dst.at[image], save_sem.at[at]) for at, (src, dst) in enumerate(pairs)]

    class u_save:
        def __init__(self, image, chunk):
            slot = lax.rem(chunk, 3)
            self.copies = [
                pltpu.make_async_copy(ubuf.at[slot, :, pl.ds(side * HALF, HALF)], d_s.at[image, chunk * 2 + side], usem.at[slot, side])
                for side in range(2)]

        def start(self):
            for copy in self.copies:
                copy.start()

        def wait(self):
            for copy in self.copies:
                copy.wait()

    def g_save(image, chunk):
        slot = lax.rem(chunk, 2)
        return pltpu.make_async_copy(gbuf.at[slot], g_s.at[image, :, pl.ds(pl.multiple_of(chunk * CHUNK, CHUNK), CHUNK)], gsem.at[slot])

    def p_save(image, group):
        slot = group % 2
        return pltpu.make_async_copy(pbuf.at[slot], p_s.at[image, pl.ds(group * GROUP, GROUP)], psem.at[slot])

    def top_copy(image, other):
        return pltpu.make_async_remote_copy(
            src_ref=mid.at[pl.ds(0, 16)], dst_ref=tops.at[image], send_sem=send_sem.at[1 + other], recv_sem=top_sem,
            device_id={"pp": other}, device_id_type=MESH)

    def next_copy(image, slot):
        return pltpu.make_async_remote_copy(
            src_ref=mid, dst_ref=xin.at[slot], send_sem=send_sem.at[0], recv_sem=recv_sem.at[slot],
            device_id={"pp": lax.rem(stage + 1, stages)}, device_id_type=MESH)

    def wait_sent(image):
        @pl.when(jnp.logical_not(is_last))
        def _():
            next_copy(image, 0).wait_send()

        @pl.when(is_last)
        def _():
            for other in range(stages - 1):
                top_copy(image, other).wait_send()

    def one_image(image, carry):
        slot = lax.rem(image, 2)
        save_x, save_a, save_qkv, save_c, save_h, save_n = saves(image, slot)
        emb_copy(image, slot).wait()
        save_x.start()

        @pl.when(image > 0)
        def _():
            save_n.wait()
            save_qkv.wait()

        def norm1(lines):
            act[lines, :] = layer_norm(xin[slot, lines, :], g1[...], b1[...])

        by_rows(rows, norm1)
        save_a.start()

        def qkv_part(part, carry):
            index = image * 3 + part
            qkv_copy(index).wait()
            low = (dot(act[...], vqkv[lax.rem(index, 2)], 1, 1) + bqkv[part]).astype(BF16)
            for at in range(heads):
                lane = part * (heads * LANES) + at * LANES
                qkv[:, pl.ds(pl.multiple_of(lane, LANES), head)] = low[:, at * head:(at + 1) * head]

            @pl.when(part == 0)
            def _():
                qkv_copy(index + 2).start()

            @pl.when(index == 0)
            def _():
                proj_copy.start()
                fc1_copy.start()
                fc2_copy.start()

            return carry

        lax.fori_loop(0, 3, qkv_part, 0)
        save_qkv.start()

        save_a.wait()

        @pl.when(image > 0)
        def _():
            p_save(image, 0).wait()
            p_save(image, 1).wait()

        def scores_of(number):
            q, k = (qkv[:, lane:lane + LANES] for lane in (number * LANES, (heads + number) * LANES))
            return dot(k, q, 1, 1)

        def attend(number, scores):
            group, inner = number // GROUP, number % GROUP
            if group >= 2 and inner == 0:
                p_save(image, group).wait()
            v = qkv[:, (2 * heads + number) * LANES:(2 * heads + number + 1) * LANES]
            top, tail = scores[:tokens - 1], scores[tokens - 1:]
            most = jnp.maximum(jnp.max(top, axis=0, keepdims=True), tail[:1])
            top = jnp.exp2((top - most) * scale2)
            real = lax.broadcasted_iota(jnp.int32, tail.shape, 0) < 1
            tail = jnp.where(real, jnp.exp2(jnp.minimum(tail - most, 0.0) * scale2), 0.0)
            inv = 1.0 / (jnp.sum(top, axis=0, keepdims=True) + jnp.sum(tail, axis=0, keepdims=True))
            probs = jnp.concatenate([top, tail], axis=0) * inv
            pbuf[group % 2, inner, :, :rows] = probs
            act[:, number * head:(number + 1) * head] = dot(probs.astype(BF16), v, 0, 0).astype(BF16)[:, :head]
            if inner == GROUP - 1:
                p_save(image, group).start()

        scores = scores_of(0)
        for number in range(heads):
            later = scores_of(number + 1) if number + 1 < heads else None
            attend(number, scores)
            scores = later
        save_c.start()

        @pl.when(image + 1 < images)
        def _():
            qkv_copy(image * 3 + 3).start()
            qkv_copy(image * 3 + 4).start()

        @pl.when(image == 0)
        def _():
            proj_copy.wait()

        @pl.when(image > 0)
        def _():
            wait_sent(image)

        mid[...] = (dot(act[...], vproj[...]) + bproj[...] + xin[slot].astype(F32)).astype(BF16)
        save_h.start()
        save_x.wait()

        @pl.when(jnp.logical_and(is_first, image + 2 < images))
        def _():
            emb_copy(image + 2, slot).start()

        @pl.when(jnp.logical_and(stage > 0, image + 2 < images))
        def _():
            pl.semaphore_signal(free_sem, inc=1, device_id={"pp": lax.rem(stage + stages - 1, stages)}, device_id_type=MESH)

        save_c.wait()

        def norm2(lines):
            hidden = mid[lines, :]
            act[lines, :] = layer_norm(hidden, g2[...], b2[...])
            yacc[lines, :] = hidden.astype(F32) + bfc2[...]

        by_rows(rows, norm2)
        save_n.start()

        @pl.when(image == 0)
        def _():
            fc1_copy.wait()
            fc2_copy.wait()

        @pl.when(image > 0)
        def _():
            for chunk in range(3):
                u_save(image, chunk).wait()
            for chunk in range(2):
                g_save(image, chunk).wait()

        def fc1(chunk):
            columns = pl.ds(pl.multiple_of(chunk * CHUNK, CHUNK), CHUNK)
            ubuf[lax.rem(chunk, 3)] = dot(act[...], vfc1[:, columns]) + bfc1[:, columns]

        def gelu(chunk):
            slot3, slot2 = lax.rem(chunk, 3), lax.rem(chunk, 2)
            pre = ubuf[slot3]
            cdf = 0.5 + 0.5 * lax.erf(pre * (0.5 ** 0.5))
            pdf = jnp.exp2(pre * pre * (-0.5 / math.log(2.0))) * ((2.0 * math.pi) ** -0.5)
            activ = (pre * cdf).astype(BF16)
            gbuf[slot2] = activ
            ubuf[slot3] = cdf + pre * pdf
            return activ

        def fc2(chunk, activ):
            yacc[...] += dot(activ, vfc2[pl.ds(pl.multiple_of(chunk * CHUNK, CHUNK), CHUNK), :])

        fc1(0)

        def mlp_step(chunk, carry):
            @pl.when(chunk >= 3)
            def _():
                u_save(image, chunk).wait()
                g_save(image, chunk - 1).wait()

            @pl.when(chunk >= 2)
            def _():
                u_save(image, chunk - 2).start()
                g_save(image, chunk - 2).start()

            activ = gelu(chunk - 1)
            fc1(chunk)
            fc2(chunk - 1, activ)
            return carry

        lax.fori_loop(1, chunks, mlp_step, 0)
        g_save(image, chunks - 1).wait()
        u_save(image, chunks - 2).start()
        g_save(image, chunks - 2).start()
        fc2(chunks - 1, gelu(chunks - 1))
        u_save(image, chunks - 1).start()
        g_save(image, chunks - 1).start()

        save_h.wait()
        mid[...] = yacc[...].astype(BF16)

        @pl.when(jnp.logical_and(jnp.logical_not(is_last), image >= 2))
        def _():
            pl.semaphore_wait(free_sem, 1)

        @pl.when(jnp.logical_not(is_last))
        def _():
            next_copy(image, slot).start()

        @pl.when(is_last)
        def _():
            for other in range(stages - 1):
                top_copy(image, other).start()
            tops[image] = mid[pl.ds(0, 16), :]

        return carry

    lax.fori_loop(0, images, one_image, 0)
    wait_sent(images - 1)
    _, _, save_qkv, _, _, save_n = saves(images - 1, 0)
    save_qkv.wait()
    save_n.wait()
    for chunk in range(3):
        u_save(images - 1, chunk).wait()
    for chunk in range(2):
        g_save(images - 1, chunk).wait()
        p_save(images - 1, chunk).wait()

    @pl.when(jnp.logical_not(is_last))
    def _():
        pltpu.make_async_copy(tops, tops, top_sem).wait()

    for image in range(images):
        tops_out[image:image + 1, :] = tops[image, 0:1, :]


def norm_backward(grad, hidden, gain):
    values = hidden.astype(F32)
    centered = values - jnp.mean(values, axis=-1, keepdims=True)
    inv = lax.rsqrt(jnp.mean(jnp.square(centered), axis=-1, keepdims=True) + EPS)
    unit = centered * inv
    scaled = grad * gain
    grad_in = inv * (scaled - jnp.mean(scaled, axis=-1, keepdims=True) - unit * jnp.mean(scaled * unit, axis=-1, keepdims=True))
    return grad_in, grad * unit


def backward_kernel(dims, *refs):
    (gtop, wqkv, wproj, wfc1, wfc2, low1, low2, x_s, qkv_s, h_s, d_s, p_s,
     gy_s, gpre_s, gmid_s, gqkv_s, gemb, *sums_out,
     vqkv, vproj, vfc1, vfc2, gin, acc, shared, abuf, gbuf, hid, gmid, gctx, qkv, gqkv, gout, g1, g2,
     sum1g, sum1b, sum2g, sum2b, sumproj, sumfc2, sumqkv, sumfc1,
     wsem, qsem, recv_sem, top_sem, send_sem, emb_sem, save_sem, load_sem, dsem, gsem, psem, free_sem) = refs
    stages, images, tokens, heads, head = dims
    rows, width = gmid.shape
    chunks = vfc1.shape[1] // CHUNK
    groups = heads // GROUP
    stage = lax.axis_index("pp")
    is_first = stage == 0
    is_last = stage == stages - 1
    scale = head ** -0.5

    pieces = ((0, vqkv.shape[1]), (vqkv.shape[1], width - vqkv.shape[1]))

    def qkv_copy(part, side):
        slot = lax.rem(part * 2 + side, 3)
        at, size = pieces[side]
        lines = pl.ds(pl.multiple_of(lax.rem(part, 3) * width + at, 128), size)
        return pltpu.make_async_copy(wqkv.at[lines], vqkv.at[slot, pl.ds(0, size)], qsem.at[slot])

    def top_copy(image, slot):
        return pltpu.make_async_copy(gtop.at[image], gin.at[slot, pl.ds(0, 16)], top_sem.at[slot])

    def d_load(image, chunk):
        slot = lax.rem(chunk, 4)
        return pltpu.make_async_copy(d_s.at[image, pl.ds(chunk * 2, 2)], shared.at[pl.ds(slot * 2, 2)], dsem.at[slot])

    def g_save(image, chunk):
        slot = lax.rem(chunk, 2)
        return pltpu.make_async_copy(gbuf.at[slot], gpre_s.at[image, :, pl.ds(pl.multiple_of(chunk * CHUNK, CHUNK), CHUNK)], gsem.at[slot])

    def p_load(image, group):
        slot = group % 2
        return pltpu.make_async_copy(p_s.at[image, pl.ds(group * GROUP, GROUP)], shared.at[pl.ds(slot * GROUP, GROUP)], psem.at[slot])

    def saves(image, slot):
        pairs = ((gin.at[slot], gy_s), (gmid, gmid_s), (gqkv, gqkv_s))
        return [pltpu.make_async_copy(src, dst.at[image], save_sem.at[at]) for at, (src, dst) in enumerate(pairs)]

    def loads(image):
        pairs = ((h_s, hid), (x_s, hid), (qkv_s, qkv))
        return [pltpu.make_async_copy(src.at[image], dst, load_sem.at[at]) for at, (src, dst) in enumerate(pairs)]

    def next_copy(slot):
        return pltpu.make_async_remote_copy(
            src_ref=gout, dst_ref=gin.at[slot], send_sem=send_sem.at[0], recv_sem=recv_sem.at[slot],
            device_id={"pp": lax.rem(stage + stages - 1, stages)}, device_id_type=MESH)

    def emb_send(image, other):
        return pltpu.make_async_remote_copy(
            src_ref=gout, dst_ref=gemb.at[image], send_sem=send_sem.at[other], recv_sem=emb_sem,
            device_id={"pp": other}, device_id_type=MESH)

    def emb_local(image):
        return pltpu.make_async_copy(gout, gemb.at[image], save_sem.at[3])

    def wait_sent(image):
        @pl.when(jnp.logical_not(is_first))
        def _():
            next_copy(0).wait_send()

        @pl.when(is_first)
        def _():
            for other in range(1, stages):
                emb_send(image, other).wait_send()
            emb_local(image).wait()

    @pl.when(is_last)
    def _():
        gin[...] = jnp.zeros_like(gin)
        top_copy(0, 0).start()
        top_copy(1, 1).start()

    def fc2_copy(chunk):
        lines = pl.ds(pl.multiple_of(chunk * CHUNK, CHUNK), CHUNK)
        return pltpu.make_async_copy(wfc2.at[lines], vfc2.at[lines], wsem.at[2, chunk])

    def fc1_copy(chunk):
        columns = pl.ds(pl.multiple_of(chunk * CHUNK, CHUNK), CHUNK)
        return pltpu.make_async_copy(wfc1.at[:, columns], vfc1.at[:, columns], wsem.at[1, chunk])

    proj_copy = pltpu.make_async_copy(wproj, vproj, wsem.at[0, 0])
    for chunk in range(chunks):
        fc2_copy(chunk).start()
        if chunk < 4:
            d_load(0, chunk).start()
        fc1_copy(chunk).start()
    loads(0)[0].start()
    proj_copy.start()
    qkv_copy(0, 0).start()
    qkv_copy(0, 1).start()
    qkv_copy(1, 0).start()
    gctx[...] = jnp.zeros_like(gctx)
    sums_out, totals = sums_out[:8], (sum1g, sum1b, sum2g, sum2b, sumproj, sumfc2, sumqkv, sumfc1)
    for total in totals:
        total[...] = jnp.zeros_like(total)
    g1[...] = low1[...].astype(F32)
    g2[...] = low2[...].astype(F32)
    everyone(stage, stages)

    def one_image(image, carry):
        slot = lax.rem(image, 2)
        more = image + 1 < images
        save_gy, save_mid, save_qkv = saves(image, slot)
        load_h, load_x, load_qkv = loads(image)

        @pl.when(is_last)
        def _():
            top_copy(image, slot).wait()

        @pl.when(jnp.logical_not(is_last))
        def _():
            next_copy(slot).wait_recv()

        save_gy.start()

        load_qkv.start()

        @pl.when(image == 0)
        def _():
            fc2_copy(0).wait()

        @pl.when(image > 0)
        def _():
            for chunk in range(2):
                g_save(image, chunk).wait()

        acc[...] = jnp.zeros_like(acc)

        def fc2(chunk):
            lines = pl.ds(pl.multiple_of(chunk * CHUNK, CHUNK), CHUNK)
            abuf[lax.rem(chunk, 2)] = dot(gin[slot], vfc2[lines, :], 1, 1).astype(BF16)

        def gelu(chunk):
            columns = pl.ds(pl.multiple_of(chunk * CHUNK, CHUNK), CHUNK)
            slot2 = lax.rem(chunk, 2)
            slot4 = lax.rem(chunk, 4)
            pre = abuf[slot2].astype(F32) * jnp.concatenate([shared[slot4 * 2], shared[slot4 * 2 + 1]], axis=1)
            sumfc1[:, columns] += fold(pre)
            low = pre.astype(BF16)
            gbuf[slot2] = low
            return low

        def fc1(chunk, low):
            columns = pl.ds(pl.multiple_of(chunk * CHUNK, CHUNK), CHUNK)
            acc[...] += dot(low, vfc1[:, columns], 1, 1)

        fc2(0)

        def mlp_step(chunk, carry):
            d_load(image, chunk - 1).wait()

            @pl.when(image == 0)
            def _():
                fc2_copy(chunk).wait()
                fc1_copy(chunk - 1).wait()

            @pl.when(chunk >= 3)
            def _():
                g_save(image, chunk - 1).wait()

            @pl.when(chunk >= 2)
            def _():
                g_save(image, chunk - 2).start()

                @pl.when(chunk + 2 < chunks)
                def _():
                    d_load(image, chunk + 2).start()

            low = gelu(chunk - 1)
            fc2(chunk)
            fc1(chunk - 1, low)
            return carry

        lax.fori_loop(1, chunks, mlp_step, 0)
        d_load(image, chunks - 1).wait()

        @pl.when(image == 0)
        def _():
            fc1_copy(chunks - 1).wait()

        g_save(image, chunks - 1).wait()
        g_save(image, chunks - 2).start()
        fc1(chunks - 1, gelu(chunks - 1))
        g_save(image, chunks - 1).start()

        for group in range(2):
            p_load(image, group).start()
        load_h.wait()

        @pl.when(image > 0)
        def _():
            save_mid.wait()
            save_qkv.wait()

        def back2(lines):
            grad = acc[lines, :].astype(BF16).astype(F32)
            grad_in, by_unit = norm_backward(grad, hid[lines, :], g2[...])
            sum2g[...] += fold(by_unit)
            sum2b[...] += fold(grad)
            top = gin[slot, lines, :].astype(F32)
            sumfc2[...] += fold(top)
            low = (top + grad_in).astype(BF16)
            gmid[lines, :] = low
            sumproj[...] += fold(low.astype(F32))

        by_rows(rows, back2)
        save_mid.start()
        load_x.start()
        save_gy.wait()

        @pl.when(jnp.logical_and(is_last, image + 2 < images))
        def _():
            top_copy(image + 2, slot).start()

        @pl.when(jnp.logical_and(stage < stages - 1, image + 2 < images))
        def _():
            pl.semaphore_signal(free_sem, inc=1, device_id={"pp": lax.rem(stage + 1, stages)}, device_id_type=MESH)

        @pl.when(image == 0)
        def _():
            proj_copy.wait()

        low = dot(gmid[...], vproj[...], 1, 1).astype(BF16)
        for number in range(heads):
            gctx[:, number * LANES:number * LANES + head] = low[:, number * head:(number + 1) * head]
        load_qkv.wait()
        def lanes_of(number):
            return slice(number * LANES, (number + 1) * LANES)

        def grad_probs_of(number):
            return dot(qkv[:, lanes_of(2 * heads + number)], gctx[:, lanes_of(number)], 1, 1)

        def attend(number, grad_probs):
            group, inner = number // GROUP, number % GROUP
            if inner == 0:
                p_load(image, group).wait()
            probs = shared[group % 2 * GROUP + inner, :, :rows]
            at = number * head
            mean = jnp.sum(grad_probs * probs, axis=0, keepdims=True)
            low = (probs * (grad_probs - mean) * scale).astype(BF16)
            value = dot(probs.astype(BF16), gctx[:, lanes_of(number)]).astype(BF16)
            gqkv[:, 2 * width + at:2 * width + at + head] = value[:, :head]
            key = dot(low, qkv[:, lanes_of(number)]).astype(BF16)
            gqkv[:, width + at:width + at + head] = key[:, :head]
            query = dot(low, qkv[:, lanes_of(heads + number)], 0, 0).astype(BF16)
            gqkv[:, at:at + head] = query[:, :head]

        grad_probs = grad_probs_of(0)
        for number in range(heads):
            later = grad_probs_of(number + 1) if number + 1 < heads else None
            attend(number, grad_probs)
            grad_probs = later
            if number % GROUP == GROUP - 1 and number // GROUP + 2 < groups:
                p_load(image, number // GROUP + 2).start()
        save_qkv.start()

        def qkv_part(part, carry):
            for side in range(2):
                at, size = pieces[side]
                index = image * 3 + part
                qkv_copy(index, side).wait()
                columns = pl.ds(pl.multiple_of(part * width + at, 128), size)
                piece = gqkv[:, columns]
                sumqkv[:, columns] += fold(piece.astype(F32))
                acc[...] += dot(piece, vqkv[lax.rem(index * 2 + side, 3), :size])

                @pl.when(index + 1 + side < images * 3)
                def _():
                    qkv_copy(index + 1 + side, 1 - side).start()

            return carry

        acc[...] = jnp.zeros_like(acc)
        lax.fori_loop(0, 3, qkv_part, 0)

        @pl.when(more)
        def _():
            for chunk in range(4):
                d_load(image + 1, chunk).start()

        load_x.wait()

        @pl.when(image > 0)
        def _():
            wait_sent(image)

        def back1(lines):
            grad = acc[lines, :].astype(BF16).astype(F32)
            grad_in, by_unit = norm_backward(grad, hid[lines, :], g1[...])
            sum1g[...] += fold(by_unit)
            sum1b[...] += fold(grad)
            gout[lines, :] = (gmid[lines, :].astype(F32) + grad_in).astype(BF16)

        by_rows(rows, back1)

        @pl.when(more)
        def _():
            loads(image + 1)[0].start()

        @pl.when(jnp.logical_and(jnp.logical_not(is_first), image >= 2))
        def _():
            pl.semaphore_wait(free_sem, 1)

        @pl.when(jnp.logical_not(is_first))
        def _():
            next_copy(slot).start()

        @pl.when(is_first)
        def _():
            for other in range(1, stages):
                emb_send(image, other).start()
            emb_local(image).start()

        return carry

    lax.fori_loop(0, images, one_image, 0)
    wait_sent(images - 1)
    _, save_mid, save_qkv = saves(images - 1, 0)
    save_mid.wait()
    save_qkv.wait()
    for chunk in range(2):
        g_save(images - 1, chunk).wait()

    for out, total in zip(sums_out, totals):
        out[...] = jnp.sum(total[...], axis=0, keepdims=True)

    @pl.when(jnp.logical_not(is_first))
    def _():
        pltpu.make_async_copy(gemb, gemb, emb_sem).wait()


ANY = pl.BlockSpec(memory_space=pl.ANY)
VMEM = pl.BlockSpec(memory_space=pltpu.VMEM)
LIMIT = 67_043_328
DMA = pltpu.SemaphoreType.DMA


def run_forward(dims, emb, wqkv, wproj, wfc1, wfc2, vectors):
    stages, images, tokens, heads, head = dims
    rows, width = emb.shape[1:]
    hidden = wfc1.shape[1]
    hbm = lambda *shape, dtype=BF16: jax.ShapeDtypeStruct((images, rows) + shape, dtype)
    return pl.pallas_call(
        functools.partial(forward_kernel, dims),
        out_shape=(
            hbm(width), hbm(width), hbm(3 * heads * LANES), hbm(width), hbm(width), hbm(width),
            jax.ShapeDtypeStruct((images, hidden // HALF, rows, HALF), F32), hbm(hidden),
            jax.ShapeDtypeStruct((images, heads, rows, HALF), F32), jax.ShapeDtypeStruct((images, width), BF16)),
        in_specs=[ANY] * 5 + [VMEM] * 8,
        out_specs=(ANY,) * 9 + (VMEM,),
        scratch_shapes=[
            pltpu.VMEM((2, width, width), BF16), pltpu.VMEM(wproj.shape, BF16), pltpu.VMEM(wfc1.shape, BF16), pltpu.VMEM(wfc2.shape, BF16),
            pltpu.VMEM((2, rows, width), BF16), pltpu.VMEM((rows, width), BF16), pltpu.VMEM((rows, 3 * heads * LANES), BF16),
            pltpu.VMEM((rows, width), BF16), pltpu.VMEM((rows, width), F32),
            pltpu.VMEM((3, rows, CHUNK), F32), pltpu.VMEM((2, rows, CHUNK), BF16), pltpu.VMEM((2, GROUP, rows, HALF), F32),
            pltpu.VMEM((images, 16, width), BF16),
            *(pltpu.VMEM(vector.shape, F32) for vector in vectors),
            DMA((3,)), DMA((2,)), DMA((2,)), DMA((stages,)), DMA(()), DMA((6,)), DMA((3, 2)), DMA((2,)), DMA((2,)),
            pltpu.SemaphoreType.REGULAR],
        compiler_params=pltpu.CompilerParams(collective_id=0, has_side_effects=True, vmem_limit_bytes=LIMIT),
        name="forward",
    )(emb, wqkv, wproj, wfc1, wfc2, *vectors)


def run_backward(dims, gtop, wqkv, wproj, wfc1, wfc2, g1, g2, x_s, qkv_s, h_s, d_s, p_s):
    stages, images, tokens, heads, head = dims
    rows, width = x_s.shape[1:]
    hidden = wfc1.shape[1]
    hbm = lambda *shape: jax.ShapeDtypeStruct((images, rows) + shape, BF16)
    sizes = (width,) * 6 + (3 * width, hidden)
    return pl.pallas_call(
        functools.partial(backward_kernel, dims),
        out_shape=(hbm(width), hbm(hidden), hbm(width), hbm(3 * width), hbm(width)) + tuple(jax.ShapeDtypeStruct((1, size), F32) for size in sizes),
        in_specs=[ANY] * 5 + [VMEM] * 2 + [ANY] * 5,
        out_specs=(ANY,) * 5 + (VMEM,) * 8,
        scratch_shapes=[
            pltpu.VMEM((3, -(-width // 256) * LANES, width), BF16), pltpu.VMEM(wproj.shape, BF16), pltpu.VMEM(wfc1.shape, BF16), pltpu.VMEM(wfc2.shape, BF16),
            pltpu.VMEM((2, rows, width), BF16), pltpu.VMEM((rows, width), F32), pltpu.VMEM((2 * GROUP, rows, HALF), F32),
            pltpu.VMEM((2, rows, CHUNK), BF16), pltpu.VMEM((2, rows, CHUNK), BF16),
            pltpu.VMEM((rows, width), BF16), pltpu.VMEM((rows, width), BF16), pltpu.VMEM((rows, heads * LANES), BF16),
            pltpu.VMEM((rows, 3 * heads * LANES), BF16), pltpu.VMEM((rows, 3 * width), BF16),
            pltpu.VMEM((rows, width), BF16), pltpu.VMEM((1, width), F32), pltpu.VMEM((1, width), F32),
            *(pltpu.VMEM((8, size), F32) for size in sizes),
            DMA((3, hidden // CHUNK)), DMA((3,)), DMA((2,)), DMA((2,)), DMA((stages,)), DMA(()), DMA((4,)), DMA((3,)), DMA((4,)), DMA((2,)), DMA((2,)),
            pltpu.SemaphoreType.REGULAR],
        compiler_params=pltpu.CompilerParams(collective_id=1, has_side_effects=True, vmem_limit_bytes=LIMIT),
        name="backward",
    )(gtop, wqkv, wproj, wfc1, wfc2, g1, g2, x_s, qkv_s, h_s, d_s, p_s)


def head_kernel(inv_count, tops, labels, gain, bias, w_head, b_head, loss, gtop, g_gain, g_bias, g_w_head, g_b_head):
    images, width = tops.shape
    line = lambda ref: ref[...].reshape(1, -1).astype(F32)
    wide_gain = line(gain)
    pooled = layer_norm(tops[...], wide_gain, line(bias))
    logits = dot(pooled, w_head[...], 1, 1) + line(b_head)
    shifted = logits - jnp.max(logits, axis=-1, keepdims=True)
    log_probs = shifted - jnp.log(jnp.sum(jnp.exp(shifted), axis=-1, keepdims=True))
    classes = logits.shape[-1]
    number = lax.broadcasted_iota(jnp.int32, (images, 1), 0)
    label = jnp.zeros((images, 1), jnp.int32)
    for image in range(images):
        label = jnp.where(number == image, labels[image % labels.shape[0], image // labels.shape[0]], label)
    chosen = (lax.broadcasted_iota(jnp.int32, logits.shape, 1) == label).astype(F32)
    target = (1.0 - SMOOTH) * chosen + SMOOTH / classes
    parts = jnp.sum(target * log_probs, axis=-1, keepdims=True)
    loss[...] = -jnp.sum(parts, axis=0, keepdims=True) * inv_count
    grad_logits = (jnp.exp(log_probs) - target) * inv_count
    low = grad_logits.astype(BF16)
    g_w_head[...] = dot(low, pooled, 0, 0)
    g_b_head[...] = jnp.sum(grad_logits, axis=0)
    grad = dot(low, w_head[...]).astype(BF16).astype(F32)
    grad_in, by_unit = norm_backward(grad, tops[...], wide_gain)
    g_gain[...] = jnp.sum(by_unit, axis=0)
    g_bias[...] = jnp.sum(grad, axis=0)
    gtop[...] = jnp.zeros_like(gtop)
    for image in range(images):
        gtop[image, 0:1, :] = grad_in[image:image + 1].astype(BF16)


def run_head(inv_count, tops, labels, gain, bias, w_head, b_head):
    images, width = tops.shape
    classes = w_head.shape[0]
    shape = lambda *dims, dtype=F32: jax.ShapeDtypeStruct(dims, dtype)
    return pl.pallas_call(
        functools.partial(head_kernel, inv_count),
        out_shape=(shape(1, 1), shape(images, 16, width, dtype=BF16), shape(width), shape(width), shape(classes, width), shape(classes)),
        in_specs=[VMEM, pl.BlockSpec(memory_space=pltpu.SMEM)] + [VMEM] * 4,
        out_specs=(VMEM,) * 6,
        compiler_params=pltpu.CompilerParams(vmem_limit_bytes=LIMIT),
        name="head",
    )(tops, labels, gain, bias, w_head, b_head)


def weight_kernel(*refs):
    count = (len(refs) - 15 - 11) // 2
    fc2_l, qkv_l, proj_l, patch_l, fc2_r, qkv_r, proj_r, patch_r, fc1_l, fc1_r = refs[:10]
    sums = refs[10:10 + count]
    fc2_o, qkv_o, proj_o, patch_o, fc1_o = refs[10 + count:15 + count]
    sums_out = refs[15 + count:15 + 2 * count]
    lhs, rhs, out, turned, block, wide, lsem, rsem, osem, bsem, wsem = refs[15 + 2 * count:]
    width = rhs.shape[2]
    size, wide_size = lhs.shape[2], block.shape[2]
    tail = width % size
    patches = patch_l.shape[1] // size + 1
    ends = [fc2_l.shape[1] // size]
    ends.append(ends[0] + qkv_l.shape[1] // size)
    ends.append(ends[1] + width // size + 1)
    ends.append(ends[2] + patches)
    starts = [0] + ends[:3]
    steps = ends[3]
    wide_steps = fc1_r.shape[1] // wide_size

    def lines(at, unit):
        return pl.ds(pl.multiple_of(at * unit, LANES), unit)

    def left_copy(step, act):
        slot = lax.rem(step, 2)
        for product, source in enumerate((fc2_l, qkv_l, proj_l, patch_l)):
            full = source.shape[1] // size
            first = starts[product]

            @pl.when(jnp.logical_and(step >= first, step < first + full))
            def _():
                act(pltpu.make_async_copy(source.at[:, lines(step - first, size)], lhs.at[slot], lsem.at[slot]))

            if source.shape[1] % size:
                @pl.when(step == first + full)
                def _():
                    act(pltpu.make_async_copy(source.at[:, pl.ds(full * size, tail)], lhs.at[slot, :, pl.ds(0, tail)], lsem.at[slot]))

    def out_copy(step, act):
        slot = lax.rem(step, 2)
        for product, target in enumerate((fc2_o, qkv_o, proj_o)):
            full = target.shape[0] // size
            first = starts[product]

            @pl.when(jnp.logical_and(step >= first, step < first + full))
            def _():
                act(pltpu.make_async_copy(out.at[slot], target.at[lines(step - first, size)], osem.at[slot]))

            if target.shape[0] % size:
                @pl.when(step == first + full)
                def _():
                    act(pltpu.make_async_copy(out.at[slot, pl.ds(0, tail)], target.at[pl.ds(full * size, tail)], osem.at[slot]))

    def right_copy(product):
        source = (fc2_r, qkv_r, proj_r, patch_r, fc1_l)[product]
        return pltpu.make_async_copy(source, rhs.at[product % 2], rsem.at[product % 2])

    def block_copy(step):
        slot = lax.rem(step, 2)
        return pltpu.make_async_copy(fc1_r.at[:, lines(step, wide_size)], block.at[slot], bsem.at[slot])

    def wide_copy(step):
        slot = lax.rem(step, 2)
        return pltpu.make_async_copy(wide.at[slot], fc1_o.at[:, lines(step, wide_size)], wsem.at[slot])

    start = lambda copy: copy.start()
    wait = lambda copy: copy.wait()
    left_copy(0, start)
    right_copy(0).start()
    right_copy(1).start()
    for given, passed in zip(sums, sums_out):
        passed[...] = given[...]

    def one_step(step, carry):
        slot = lax.rem(step, 2)

        @pl.when(step >= 1)
        def _():
            out_copy(step - 1, start)

        @pl.when(step >= 2)
        def _():
            out_copy(step - 2, wait)

        @pl.when(step + 1 < steps)
        def _():
            left_copy(step + 1, start)

        for product, first in enumerate(starts):
            @pl.when(step == first)
            def _(product=product):
                right_copy(product).wait()
                if product >= 1:
                    right_copy(product + 1).start()

        @pl.when(step == steps - 1)
        def _():
            block_copy(0).start()

        left_copy(step, wait)
        which = lax.rem(sum((step >= end).astype(jnp.int32) for end in ends[:3]), 2)
        out[slot] = dot(lhs[slot], rhs[which], 0, 0)
        for at in range(patches):
            count = min(size, patch_o.shape[0] - at * size)

            @pl.when(step == starts[3] + at)
            def _():
                patch_o[at * size:at * size + count, :] = out[slot, :count, :]

        return carry

    lax.fori_loop(0, steps, one_step, 0)
    right_copy(4).wait()
    turned[...] = rhs[0].T

    def wide_step(step, carry):
        slot = lax.rem(step, 2)

        @pl.when(step >= 1)
        def _():
            wide_copy(step - 1).start()

        @pl.when(step >= 2)
        def _():
            wide_copy(step - 2).wait()

        @pl.when(step + 1 < wide_steps)
        def _():
            block_copy(step + 1).start()

        block_copy(step).wait()
        wide[slot] = dot(turned[...], block[slot])
        return carry

    lax.fori_loop(0, wide_steps, wide_step, 0)
    wide_copy(wide_steps - 1).start()
    wide_copy(wide_steps - 2).wait()
    wide_copy(wide_steps - 1).wait()


def run_weights(lefts, rights, patch_size, sums):
    fc2_l, qkv_l, proj_l, patch_l, fc1_l = lefts
    fc2_r, qkv_r, proj_r, patch_r, fc1_r = rights
    rows, width = fc2_r.shape
    size, wide_size = 3 * LANES, 4 * LANES
    shapes = [(left.shape[1], right.shape[1]) for left, right in zip(lefts, rights)]
    shapes[3] = (patch_size, width)
    flops = sum(2 * rows * a * b for a, b in shapes)
    return pl.pallas_call(
        weight_kernel,
        out_shape=tuple(jax.ShapeDtypeStruct(shape, F32) for shape in shapes) + tuple(jax.ShapeDtypeStruct(total.shape, F32) for total in sums),
        in_specs=[ANY] * 10 + [VMEM] * len(sums),
        out_specs=(ANY,) * 3 + (VMEM, ANY) + (VMEM,) * len(sums),
        scratch_shapes=[
            pltpu.VMEM((2, rows, size), BF16), pltpu.VMEM((2, rows, width), BF16), pltpu.VMEM((2, size, width), F32),
            pltpu.VMEM((width, rows), BF16), pltpu.VMEM((2, rows, wide_size), BF16), pltpu.VMEM((2, width, wide_size), F32),
            DMA((2,)), DMA((2,)), DMA((2,)), DMA((2,)), DMA((2,))],
        compiler_params=pltpu.CompilerParams(vmem_limit_bytes=LIMIT),
        cost_estimate=pl.CostEstimate(flops=flops, bytes_accessed=4 * sum(a * b for a, b in shapes), transcendentals=0),
        name="weights",
    )(fc2_l, qkv_l, proj_l, patch_l, fc2_r, qkv_r, proj_r, patch_r, fc1_l, fc1_r, *sums)


def matmul_rows(spec, left, right):
    return jnp.einsum(spec, left, right, preferred_element_type=F32)


def solution(mesh):
    stages = mesh.shape["pp"]
    in_specs = (P("dp"), P("dp"), P(), P(), P(), P()) + (P("pp"),) * 12 + (P(),) * 4
    out_specs = (P("dp"),) * 5 + (P(("dp", "pp")),) * 12 + (P("dp"),) * 4

    def body(patches, labels, w_patch, b_patch, cls_token, pos_embed, *rest):
        ln1_gain, ln1_bias, w_qkv, b_qkv, w_proj, b_proj, ln2_gain, ln2_bias, w_fc1, b_fc1, w_fc2, b_fc2 = (tensor[0] for tensor in rest[:12])
        lnf_gain, lnf_bias, w_head, b_head = rest[12:]
        tokens, width = pos_embed.shape
        heads, head = w_qkv.shape[2:]
        images = labels.size
        inv_count = 1.0 / images
        rows = -(-tokens // 16) * 16
        dims = (stages, images, tokens, heads, head)

        patch_size = patches.shape[-1]
        spare = -patch_size % LANES
        patch_rows = jnp.pad(patches.reshape((images,) + patches.shape[2:]), ((0, 0), (1, rows - tokens), (0, spare)))
        w_embed = jnp.pad(w_patch, ((0, spare), (0, 0)))
        is_patch = lax.broadcasted_iota(jnp.int32, (rows, 1), 0) > 0
        base = jnp.pad(pos_embed, ((0, rows - tokens), (0, 0))).astype(F32) + jnp.where(is_patch, b_patch.astype(F32), cls_token.astype(F32))
        embedded = (matmul_rows("inp,pd->ind", patch_rows, w_embed) + base).astype(BF16)

        line = lambda tensor: tensor.reshape(1, -1)
        wqkv_t = jnp.transpose(w_qkv, (1, 2, 3, 0)).reshape(3 * width, width)
        big = (wqkv_t, w_proj.reshape(width, width), w_fc1, w_fc2)
        vectors = tuple(map(line, (ln1_gain, ln1_bias, b_qkv, b_proj, ln2_gain, ln2_bias, b_fc1, b_fc2)))
        vectors = vectors[:2] + (vectors[2].reshape(3, 1, width),) + vectors[3:]
        x_s, a_s, qkv_s, c_s, h_s, n_s, d_s, g_s, p_s, tops = run_forward(dims, embedded, *big, vectors)

        loss, gtop, g_lnf_gain, g_lnf_bias, g_w_head, g_b_head = run_head(
            inv_count, tops, jnp.transpose(labels), lnf_gain, lnf_bias, jnp.transpose(w_head), b_head)

        gy_s, gpre_s, gmid_s, gqkv_s, gemb, *sums = run_backward(dims, gtop, *big, vectors[0], vectors[4], x_s, qkv_s, h_s, d_s, p_s)
        flat = lambda array: array.reshape(images * rows, -1)
        g_w_fc2, g_w_qkv, g_w_proj, g_w_patch, g_w_fc1, *sums = run_weights(
            tuple(map(flat, (g_s, gqkv_s, c_s, patch_rows, n_s))), tuple(map(flat, (gy_s, a_s, gmid_s, gemb, gpre_s))), patch_size, sums)
        g_ln1_gain, g_ln1_bias, g_ln2_gain, g_ln2_bias, g_b_proj, g_b_fc2, g_b_qkv, g_b_fc1 = sums
        g_w_qkv = jnp.transpose(g_w_qkv.reshape(3, heads, head, width), (3, 0, 1, 2))[None]
        layer_grads = (
            g_ln1_gain, g_ln1_bias, g_w_qkv, g_b_qkv.reshape(1, 3, heads, head), g_w_proj.reshape(1, heads, head, width), g_b_proj,
            g_ln2_gain, g_ln2_bias, g_w_fc1[None], g_b_fc1, g_w_fc2[None], g_b_fc2,
        )
        g_pos_embed = jnp.sum(gemb[:, :tokens].astype(F32), axis=0)
        embed_grads = (
            g_w_patch, jnp.sum(g_pos_embed[1:], axis=0), g_pos_embed[0], g_pos_embed,
        )
        return (loss.reshape(1),) + embed_grads + layer_grads + (g_lnf_gain, g_lnf_bias, jnp.transpose(g_w_head), g_b_head)

    return jax.shard_map(body, mesh=mesh, in_specs=in_specs, out_specs=out_specs, check_vma=False)
```

```python
import functools
import math
import jax
import jax.numpy as jnp
from jax import lax
from jax.experimental import pallas as pl
from jax.experimental.pallas import tpu as pltpu
from jax.sharding import PartitionSpec as P

EPS = 1e-6
SMOOTH = 0.1
F32 = jnp.float32
BF16 = jnp.bfloat16
MESH = pl.DeviceIdType.MESH
LANES = 128
HALF = 384
CHUNK = 2 * HALF
GROUP = 4
BLOCK = 136
DOWN = {"axis": 0, "keepdims": True}
ACROSS = {"axis": -1, "keepdims": True}


def flip(index):
    return lax.rem(index, 2)


def third(index):
    return lax.rem(index, 3)


def layer_norm(hidden, gain, bias):
    values = hidden.astype(F32)
    centered = values - jnp.mean(values, **ACROSS)
    variance = jnp.mean(jnp.square(centered), **ACROSS)
    return (centered * lax.rsqrt(variance + EPS) * gain + bias).astype(BF16)


def dot(left, right, left_axis=1, right_axis=0):
    return lax.dot_general(left, right, (((left_axis,), (right_axis,)), ((), ())), preferred_element_type=F32)


def by_rows(rows, visit):
    def step(index, carry):
        visit(pl.ds(pl.multiple_of(index * BLOCK, BLOCK), BLOCK))
        return carry

    lax.fori_loop(0, rows // BLOCK, step, 0)
    if rows % BLOCK:
        visit(pl.ds(rows - rows % BLOCK, rows % BLOCK))


def fold(values):
    rows, columns = values.shape
    return jnp.sum(values.reshape(rows // 8, 8, columns), axis=0)


def everyone(stage, stages):
    barrier = pltpu.get_barrier_semaphore()
    for hop in range(1, stages):
        pl.semaphore_signal(barrier, device_id={"pp": lax.rem(stage + hop, stages)}, device_id_type=MESH)
    pl.semaphore_wait(barrier, stages - 1)


def weight_copies(wproj, wfc1, wfc2, vproj, vfc1, vfc2, sems, turned):
    def of_chunk(source, target, which, by_lines):
        def copy(chunk):
            span = pl.ds(pl.multiple_of(chunk * CHUNK, CHUNK), CHUNK)
            part = span if by_lines else (slice(None), span)
            return pltpu.make_async_copy(source.at[part], target.at[part], sems.at[which, chunk])
        return copy

    proj = pltpu.make_async_copy(wproj, vproj, sems.at[0, 0])
    return proj, of_chunk(wfc1, vfc1, 1, turned), of_chunk(wfc2, vfc2, 2, not turned)


def forward_kernel(dims, *refs):
    (emb, wqkv, wproj, wfc1, wfc2, *given,
     x_s, a_s, qkv_s, c_s, h_s, n_s, d_s, g_s, p_s, tops_out,
     vqkv, vproj, vfc1, vfc2, xin, act, qkv, mid, yacc, ubuf, gbuf, pbuf, tops,
     g1, b1, bqkv, bproj, g2, b2, bfc1, bfc2,
     wsem, qsem, recv_sem, send_sem, top_sem, save_sem, usem, gsem, psem, free_sem) = refs
    stages, images, tokens, heads, head = dims
    rows, width = mid.shape
    chunks = vfc1.shape[1] // CHUNK
    stage = lax.axis_index("pp")
    is_first = stage == 0
    is_last = stage == stages - 1
    scale2 = head ** -0.5 / math.log(2.0)


    def qkv_copy(index):
        slot = flip(index)
        lines = pl.ds(pl.multiple_of(third(index) * width, 128), width)
        return pltpu.make_async_copy(wqkv.at[lines], vqkv.at[slot], qsem.at[slot])

    def emb_copy(image, slot):
        return pltpu.make_async_copy(emb.at[image], xin.at[slot], recv_sem.at[slot])

    @pl.when(is_first)
    def _():
        emb_copy(0, 0).start()

    qkv_copy(0).start()

    @pl.when(is_first)
    def _():
        emb_copy(1, 1).start()

    qkv_copy(1).start()
    proj_copy, fc1_copy, fc2_copy = weight_copies(wproj, wfc1, wfc2, vproj, vfc1, vfc2, wsem, False)

    def load_rest():
        proj_copy.start()
        for chunk in range(chunks):
            fc1_copy(chunk).start()
            fc2_copy(chunk).start()

    @pl.when(jnp.logical_not(is_first))
    def _():
        load_rest()

    qkv[:] = jnp.zeros_like(qkv)
    for low, wide in zip(given, (g1, b1, bqkv, bproj, g2, b2, bfc1, bfc2)):
        wide[:] = low[:].astype(F32)
    everyone(stage, stages)

    def saves(image, slot):
        pairs = ((xin.at[slot], x_s), (act, a_s), (qkv, qkv_s), (act, c_s), (mid, h_s), (act, n_s))
        return [pltpu.make_async_copy(src, dst.at[image], save_sem.at[at]) for at, (src, dst) in enumerate(pairs)]

    class u_save:
        def __init__(self, image, chunk):
            slot = third(chunk)
            self.copies = [
                pltpu.make_async_copy(ubuf.at[slot, :, pl.ds(side * HALF, HALF)], d_s.at[image, chunk * 2 + side], usem.at[slot, side])
                for side in range(2)]

        def start(self):
            for copy in self.copies:
                copy.start()

        def wait(self):
            for copy in self.copies:
                copy.wait()

    def g_save(image, chunk):
        slot = flip(chunk)
        return pltpu.make_async_copy(gbuf.at[slot], g_s.at[image, :, pl.ds(pl.multiple_of(chunk * CHUNK, CHUNK), CHUNK)], gsem.at[slot])

    def p_save(image, group):
        slot = group % 2
        return pltpu.make_async_copy(pbuf.at[slot], p_s.at[image, pl.ds(group * GROUP, GROUP)], psem.at[slot])

    def top_copy(image, other):
        return pltpu.make_async_remote_copy(
            src_ref=mid.at[pl.ds(0, 16)], dst_ref=tops.at[image], send_sem=send_sem.at[1 + other], recv_sem=top_sem,
            device_id={"pp": other}, device_id_type=MESH)

    def next_copy(image, slot):
        return pltpu.make_async_remote_copy(
            src_ref=mid, dst_ref=xin.at[slot], send_sem=send_sem.at[0], recv_sem=recv_sem.at[slot],
            device_id={"pp": lax.rem(stage + 1, stages)}, device_id_type=MESH)

    def wait_sent(image):
        @pl.when(jnp.logical_not(is_last))
        def _():
            next_copy(image, 0).wait_send()

        @pl.when(is_last)
        def _():
            for other in range(stages - 1):
                top_copy(image, other).wait_send()

    def one_image(image, carry):
        slot = flip(image)
        save_x, save_a, save_qkv, save_c, save_h, save_n = saves(image, slot)
        emb_copy(image, slot).wait()
        save_x.start()

        @pl.when(image > 0)
        def _():
            save_n.wait()
            save_qkv.wait()

        def norm1(lines):
            act[lines, :] = layer_norm(xin[slot, lines, :], g1[:], b1[:])

        by_rows(rows, norm1)
        save_a.start()

        def qkv_part(part, carry):
            index = image * 3 + part
            qkv_copy(index).wait()
            low = (dot(act[:], vqkv[flip(index)], 1, 1) + bqkv[part]).astype(BF16)
            for at in range(heads):
                lane = part * (heads * LANES) + at * LANES
                qkv[:, pl.ds(pl.multiple_of(lane, LANES), head)] = low[:, at * head:(at + 1) * head]

            @pl.when(part == 0)
            def _():
                qkv_copy(index + 2).start()

            @pl.when(jnp.logical_and(is_first, index == 0))
            def _():
                load_rest()

            return carry

        lax.fori_loop(0, 3, qkv_part, 0)
        save_qkv.start()

        save_a.wait()

        @pl.when(image > 0)
        def _():
            p_save(image, 0).wait()
            p_save(image, 1).wait()

        def scores_of(number):
            q, k = (qkv[:, lane:lane + LANES] for lane in (number * LANES, (heads + number) * LANES))
            return dot(k, q, 1, 1)

        def attend(number, scores):
            group, inner = number // GROUP, number % GROUP
            if group >= 2 and inner == 0:
                p_save(image, group).wait()
            v = qkv[:, (2 * heads + number) * LANES:(2 * heads + number + 1) * LANES]
            top, tail = scores[:tokens - 1], scores[tokens - 1:]
            most = jnp.maximum(jnp.max(top, **DOWN), tail[:1])
            top = jnp.exp2((top - most) * scale2)
            real = lax.broadcasted_iota(jnp.int32, tail.shape, 0) < 1
            tail = jnp.where(real, jnp.exp2(jnp.minimum(tail - most, 0.0) * scale2), 0.0)
            inv = 1.0 / (jnp.sum(top, **DOWN) + jnp.sum(tail, **DOWN))
            probs = jnp.concatenate([top, tail], axis=0) * inv
            pbuf[group % 2, inner, :, :rows] = probs
            act[:, number * head:(number + 1) * head] = dot(probs.astype(BF16), v, 0, 0).astype(BF16)[:, :head]
            if inner == GROUP - 1:
                p_save(image, group).start()

        scores = scores_of(0)
        for number in range(heads):
            later = scores_of(number + 1) if number + 1 < heads else None
            attend(number, scores)
            scores = later
        save_c.start()

        @pl.when(image + 1 < images)
        def _():
            qkv_copy(image * 3 + 3).start()
            qkv_copy(image * 3 + 4).start()

        @pl.when(image == 0)
        def _():
            proj_copy.wait()

        @pl.when(image > 0)
        def _():
            wait_sent(image)

        mid[:] = (dot(act[:], vproj[:]) + bproj[:] + xin[slot].astype(F32)).astype(BF16)
        save_h.start()
        save_x.wait()

        @pl.when(jnp.logical_and(is_first, image + 2 < images))
        def _():
            emb_copy(image + 2, slot).start()

        @pl.when(jnp.logical_and(stage > 0, image + 2 < images))
        def _():
            pl.semaphore_signal(free_sem, device_id={"pp": lax.rem(stage + stages - 1, stages)}, device_id_type=MESH)

        save_c.wait()

        def norm2(lines):
            hidden = mid[lines, :]
            act[lines, :] = layer_norm(hidden, g2[:], b2[:])
            yacc[lines, :] = hidden.astype(F32) + bfc2[:]

        by_rows(rows, norm2)
        save_n.start()

        @pl.when(image == 0)
        def _():
            fc1_copy(0).wait()

        @pl.when(image > 0)
        def _():
            for chunk in range(3):
                u_save(image, chunk).wait()
            for chunk in range(2):
                g_save(image, chunk).wait()

        def fc1(chunk):
            columns = pl.ds(pl.multiple_of(chunk * CHUNK, CHUNK), CHUNK)
            ubuf[third(chunk)] = dot(act[:], vfc1[:, columns]) + bfc1[:, columns]

        def gelu(chunk):
            slot3, slot2 = third(chunk), flip(chunk)
            pre = ubuf[slot3]
            cdf = 0.5 + 0.5 * lax.erf(pre * (0.5 ** 0.5))
            pdf = jnp.exp2(pre * pre * (-0.5 / math.log(2.0))) * ((2.0 * math.pi) ** -0.5)
            activ = (pre * cdf).astype(BF16)
            gbuf[slot2] = activ
            ubuf[slot3] = cdf + pre * pdf
            return activ

        def fc2(chunk, activ):
            yacc[:] += dot(activ, vfc2[pl.ds(pl.multiple_of(chunk * CHUNK, CHUNK), CHUNK), :])

        fc1(0)

        def mlp_step(chunk, carry):
            @pl.when(chunk >= 3)
            def _():
                u_save(image, chunk).wait()
                g_save(image, chunk - 1).wait()

            @pl.when(image == 0)
            def _():
                fc1_copy(chunk).wait()
                fc2_copy(chunk - 1).wait()

            @pl.when(chunk >= 2)
            def _():
                u_save(image, chunk - 2).start()
                g_save(image, chunk - 2).start()

            activ = gelu(chunk - 1)
            fc1(chunk)
            fc2(chunk - 1, activ)
            return carry

        lax.fori_loop(1, chunks, mlp_step, 0)

        @pl.when(image == 0)
        def _():
            fc2_copy(chunks - 1).wait()

        g_save(image, chunks - 1).wait()
        u_save(image, chunks - 2).start()
        g_save(image, chunks - 2).start()
        fc2(chunks - 1, gelu(chunks - 1))
        u_save(image, chunks - 1).start()
        g_save(image, chunks - 1).start()

        save_h.wait()
        mid[:] = yacc[:].astype(BF16)

        @pl.when(jnp.logical_and(jnp.logical_not(is_last), image >= 2))
        def _():
            pl.semaphore_wait(free_sem, 1)

        @pl.when(jnp.logical_not(is_last))
        def _():
            next_copy(image, slot).start()

        @pl.when(is_last)
        def _():
            for other in range(stages - 1):
                top_copy(image, other).start()
            tops[image] = mid[pl.ds(0, 16), :]

        return carry

    lax.fori_loop(0, images, one_image, 0)
    wait_sent(images - 1)
    _, _, save_qkv, _, _, save_n = saves(images - 1, 0)
    save_qkv.wait()
    save_n.wait()
    for chunk in range(3):
        u_save(images - 1, chunk).wait()
    for chunk in range(2):
        g_save(images - 1, chunk).wait()
        p_save(images - 1, chunk).wait()

    @pl.when(jnp.logical_not(is_last))
    def _():
        pltpu.make_async_copy(tops, tops, top_sem).wait()

    for image in range(images):
        tops_out[image:image + 1, :] = tops[image, 0:1, :]


def norm_backward(grad, hidden, gain):
    values = hidden.astype(F32)
    centered = values - jnp.mean(values, **ACROSS)
    inv = lax.rsqrt(jnp.mean(jnp.square(centered), **ACROSS) + EPS)
    unit = centered * inv
    scaled = grad * gain
    grad_in = inv * (scaled - jnp.mean(scaled, **ACROSS) - unit * jnp.mean(scaled * unit, **ACROSS))
    return grad_in, grad * unit


def backward_kernel(dims, *refs):
    (gtop, wqkv, wproj, wfc1, wfc2, low1, low2, x_s, qkv_s, h_s, d_s, p_s,
     gy_s, gpre_s, gmid_s, gqkv_s, gemb, *sums_out,
     vqkv, vproj, vfc1, vfc2, gin, acc, shared, abuf, gbuf, hid, gmid, gctx, qkv, gqkv, gout, g1, g2,
     sum1g, sum1b, sum2g, sum2b, sumproj, sumfc2, sumqkv, sumfc1,
     wsem, qsem, recv_sem, top_sem, send_sem, emb_sem, save_sem, load_sem, dsem, gsem, psem, free_sem) = refs
    stages, images, tokens, heads, head = dims
    rows, width = gmid.shape
    chunks = vfc2.shape[1] // CHUNK
    groups = heads // GROUP
    stage = lax.axis_index("pp")
    is_first = stage == 0
    is_last = stage == stages - 1
    scale = head ** -0.5

    pieces = ((0, vqkv.shape[1]), (vqkv.shape[1], width - vqkv.shape[1]))

    def qkv_copy(part, side):
        slot = third(part * 2 + side)
        at, size = pieces[side]
        lines = pl.ds(pl.multiple_of(third(part) * width + at, 128), size)
        return pltpu.make_async_copy(wqkv.at[lines], vqkv.at[slot, pl.ds(0, size)], qsem.at[slot])

    def top_copy(image, slot):
        return pltpu.make_async_copy(gtop.at[image], gin.at[slot, pl.ds(0, 16)], top_sem.at[slot])

    def d_load(image, chunk):
        slot = lax.rem(chunk, 4)
        return pltpu.make_async_copy(d_s.at[image, pl.ds(chunk * 2, 2)], shared.at[pl.ds(slot * 2, 2)], dsem.at[slot])

    def g_save(image, chunk):
        slot = flip(chunk)
        return pltpu.make_async_copy(gbuf.at[slot], gpre_s.at[image, :, pl.ds(pl.multiple_of(chunk * CHUNK, CHUNK), CHUNK)], gsem.at[slot])

    def p_load(image, group):
        slot = group % 2
        return pltpu.make_async_copy(p_s.at[image, pl.ds(group * GROUP, GROUP)], shared.at[pl.ds(slot * GROUP, GROUP)], psem.at[slot])

    def saves(image, slot):
        pairs = ((gin.at[slot], gy_s), (gmid, gmid_s), (gqkv, gqkv_s))
        return [pltpu.make_async_copy(src, dst.at[image], save_sem.at[at]) for at, (src, dst) in enumerate(pairs)]

    def loads(image):
        pairs = ((h_s, hid), (x_s, hid), (qkv_s, qkv))
        return [pltpu.make_async_copy(src.at[image], dst, load_sem.at[at]) for at, (src, dst) in enumerate(pairs)]

    def next_copy(slot):
        return pltpu.make_async_remote_copy(
            src_ref=gout, dst_ref=gin.at[slot], send_sem=send_sem.at[0], recv_sem=recv_sem.at[slot],
            device_id={"pp": lax.rem(stage + stages - 1, stages)}, device_id_type=MESH)

    def emb_send(image, other):
        return pltpu.make_async_remote_copy(
            src_ref=gout, dst_ref=gemb.at[image], send_sem=send_sem.at[other], recv_sem=emb_sem,
            device_id={"pp": other}, device_id_type=MESH)

    def emb_local(image):
        return pltpu.make_async_copy(gout, gemb.at[image], save_sem.at[3])

    def wait_sent(image):
        @pl.when(jnp.logical_not(is_first))
        def _():
            next_copy(0).wait_send()

        @pl.when(is_first)
        def _():
            for other in range(1, stages):
                emb_send(image, other).wait_send()
            emb_local(image).wait()

    @pl.when(is_last)
    def _():
        gin[:] = jnp.zeros_like(gin)
        top_copy(0, 0).start()
        top_copy(1, 1).start()

    proj_copy, fc1_copy, fc2_copy = weight_copies(wproj, wfc1, wfc2, vproj, vfc1, vfc2, wsem, True)
    for chunk in range(chunks):
        fc2_copy(chunk).start()
        if chunk < 4:
            d_load(0, chunk).start()
        fc1_copy(chunk).start()
    loads(0)[0].start()
    proj_copy.start()
    qkv_copy(0, 0).start()
    qkv_copy(0, 1).start()
    qkv_copy(1, 0).start()
    gctx[:] = jnp.zeros_like(gctx)
    sums_out, totals = sums_out[:8], (sum1g, sum1b, sum2g, sum2b, sumproj, sumfc2, sumqkv, sumfc1)
    for total in totals:
        total[:] = jnp.zeros_like(total)
    g1[:] = low1[:].astype(F32)
    g2[:] = low2[:].astype(F32)
    everyone(stage, stages)

    def one_image(image, carry):
        slot = flip(image)
        more = image + 1 < images
        save_gy, save_mid, save_qkv = saves(image, slot)
        load_h, load_x, load_qkv = loads(image)

        @pl.when(is_last)
        def _():
            top_copy(image, slot).wait()

        @pl.when(jnp.logical_not(is_last))
        def _():
            next_copy(slot).wait_recv()

        save_gy.start()

        load_qkv.start()

        @pl.when(image == 0)
        def _():
            fc2_copy(0).wait()

        @pl.when(image > 0)
        def _():
            for chunk in range(2):
                g_save(image, chunk).wait()

        acc[:] = jnp.zeros_like(acc)

        def fc2(chunk):
            columns = pl.ds(pl.multiple_of(chunk * CHUNK, CHUNK), CHUNK)
            abuf[flip(chunk)] = dot(gin[slot], vfc2[:, columns]).astype(BF16)

        def gelu(chunk):
            columns = pl.ds(pl.multiple_of(chunk * CHUNK, CHUNK), CHUNK)
            slot2 = flip(chunk)
            slot4 = lax.rem(chunk, 4)
            pre = abuf[slot2].astype(F32) * jnp.concatenate([shared[slot4 * 2], shared[slot4 * 2 + 1]], axis=1)
            sumfc1[:, columns] += fold(pre)
            low = pre.astype(BF16)
            gbuf[slot2] = low
            return low

        def fc1(chunk, low):
            lines = pl.ds(pl.multiple_of(chunk * CHUNK, CHUNK), CHUNK)
            acc[:] += dot(low, vfc1[lines, :])

        fc2(0)

        def mlp_step(chunk, carry):
            d_load(image, chunk - 1).wait()

            @pl.when(image == 0)
            def _():
                fc2_copy(chunk).wait()
                fc1_copy(chunk - 1).wait()

            @pl.when(chunk >= 3)
            def _():
                g_save(image, chunk - 1).wait()

            @pl.when(chunk >= 2)
            def _():
                g_save(image, chunk - 2).start()

                @pl.when(chunk + 2 < chunks)
                def _():
                    d_load(image, chunk + 2).start()

            low = gelu(chunk - 1)
            fc2(chunk)
            fc1(chunk - 1, low)
            return carry

        lax.fori_loop(1, chunks, mlp_step, 0)
        d_load(image, chunks - 1).wait()

        @pl.when(image == 0)
        def _():
            fc1_copy(chunks - 1).wait()

        g_save(image, chunks - 1).wait()
        g_save(image, chunks - 2).start()
        fc1(chunks - 1, gelu(chunks - 1))
        g_save(image, chunks - 1).start()

        for group in range(2):
            p_load(image, group).start()
        load_h.wait()

        @pl.when(image > 0)
        def _():
            save_mid.wait()
            save_qkv.wait()

        def back2(lines):
            grad = acc[lines, :].astype(BF16).astype(F32)
            grad_in, by_unit = norm_backward(grad, hid[lines, :], g2[:])
            sum2g[:] += fold(by_unit)
            sum2b[:] += fold(grad)
            top = gin[slot, lines, :].astype(F32)
            sumfc2[:] += fold(top)
            low = (top + grad_in).astype(BF16)
            gmid[lines, :] = low
            sumproj[:] += fold(low.astype(F32))

        by_rows(rows, back2)
        save_mid.start()
        load_x.start()
        save_gy.wait()

        @pl.when(jnp.logical_and(is_last, image + 2 < images))
        def _():
            top_copy(image + 2, slot).start()

        @pl.when(jnp.logical_and(stage < stages - 1, image + 2 < images))
        def _():
            pl.semaphore_signal(free_sem, device_id={"pp": lax.rem(stage + 1, stages)}, device_id_type=MESH)

        @pl.when(image == 0)
        def _():
            proj_copy.wait()

        low = dot(gmid[:], vproj[:]).astype(BF16)
        for number in range(heads):
            gctx[:, number * LANES:number * LANES + head] = low[:, number * head:(number + 1) * head]
        load_qkv.wait()
        def lanes_of(number):
            return slice(number * LANES, (number + 1) * LANES)

        def grad_probs_of(number):
            return dot(qkv[:, lanes_of(2 * heads + number)], gctx[:, lanes_of(number)], 1, 1)

        def attend(number, grad_probs):
            group, inner = number // GROUP, number % GROUP
            if inner == 0:
                p_load(image, group).wait()
            probs = shared[group % 2 * GROUP + inner, :, :rows]
            at = number * head
            mean = jnp.sum(grad_probs * probs, **DOWN)
            low = (probs * (grad_probs - mean) * scale).astype(BF16)
            value = dot(probs.astype(BF16), gctx[:, lanes_of(number)]).astype(BF16)
            gqkv[:, 2 * width + at:2 * width + at + head] = value[:, :head]
            key = dot(low, qkv[:, lanes_of(number)]).astype(BF16)
            gqkv[:, width + at:width + at + head] = key[:, :head]
            query = dot(low, qkv[:, lanes_of(heads + number)], 0, 0).astype(BF16)
            gqkv[:, at:at + head] = query[:, :head]

        grad_probs = grad_probs_of(0)
        for number in range(heads):
            later = grad_probs_of(number + 1) if number + 1 < heads else None
            attend(number, grad_probs)
            grad_probs = later
            if number % GROUP == GROUP - 1 and number // GROUP + 2 < groups:
                p_load(image, number // GROUP + 2).start()
        save_qkv.start()

        def qkv_part(part, carry):
            for side in range(2):
                at, size = pieces[side]
                index = image * 3 + part
                qkv_copy(index, side).wait()
                columns = pl.ds(pl.multiple_of(part * width + at, 128), size)
                piece = gqkv[:, columns]
                sumqkv[:, columns] += fold(piece.astype(F32))
                acc[:] += dot(piece, vqkv[third(index * 2 + side), :size])

                @pl.when(index + 1 + side < images * 3)
                def _():
                    qkv_copy(index + 1 + side, 1 - side).start()

            return carry

        acc[:] = jnp.zeros_like(acc)
        lax.fori_loop(0, 3, qkv_part, 0)

        @pl.when(more)
        def _():
            for chunk in range(4):
                d_load(image + 1, chunk).start()

        load_x.wait()

        @pl.when(image > 0)
        def _():
            wait_sent(image)

        def back1(lines):
            grad = acc[lines, :].astype(BF16).astype(F32)
            grad_in, by_unit = norm_backward(grad, hid[lines, :], g1[:])
            sum1g[:] += fold(by_unit)
            sum1b[:] += fold(grad)
            gout[lines, :] = (gmid[lines, :].astype(F32) + grad_in).astype(BF16)

        by_rows(rows, back1)

        @pl.when(more)
        def _():
            loads(image + 1)[0].start()

        @pl.when(jnp.logical_and(jnp.logical_not(is_first), image >= 2))
        def _():
            pl.semaphore_wait(free_sem, 1)

        @pl.when(jnp.logical_not(is_first))
        def _():
            next_copy(slot).start()

        @pl.when(is_first)
        def _():
            for other in range(1, stages):
                emb_send(image, other).start()
            emb_local(image).start()

        return carry

    lax.fori_loop(0, images, one_image, 0)
    wait_sent(images - 1)
    _, save_mid, save_qkv = saves(images - 1, 0)
    save_mid.wait()
    save_qkv.wait()
    for chunk in range(2):
        g_save(images - 1, chunk).wait()

    for out, total in zip(sums_out, totals):
        out[:] = jnp.sum(total[:], **DOWN)

    @pl.when(jnp.logical_not(is_first))
    def _():
        pltpu.make_async_copy(gemb, gemb, emb_sem).wait()


ANY = pl.BlockSpec(memory_space=pl.ANY)
VMEM = pl.BlockSpec(memory_space=pltpu.VMEM)
LIMIT = 67_043_328
DMA = pltpu.SemaphoreType.DMA
PAIR = DMA((2,))
TRIPLE = DMA((3,))


def run_forward(dims, emb, wqkv, wproj, wfc1, wfc2, vectors):
    stages, images, tokens, heads, head = dims
    rows, width = emb.shape[1:]
    hidden = wfc1.shape[1]
    hbm = lambda *shape, dtype=BF16: jax.ShapeDtypeStruct((images, rows) + shape, dtype)
    return pl.pallas_call(
        functools.partial(forward_kernel, dims),
        out_shape=(
            hbm(width), hbm(width), hbm(3 * heads * LANES), hbm(width), hbm(width), hbm(width),
            jax.ShapeDtypeStruct((images, hidden // HALF, rows, HALF), F32), hbm(hidden),
            jax.ShapeDtypeStruct((images, heads, rows, HALF), F32), jax.ShapeDtypeStruct((images, width), BF16)),
        in_specs=[ANY] * 5 + [VMEM] * 8,
        out_specs=(ANY,) * 9 + (VMEM,),
        scratch_shapes=[
            pltpu.VMEM((2, width, width), BF16), pltpu.VMEM(wproj.shape, BF16), pltpu.VMEM(wfc1.shape, BF16), pltpu.VMEM(wfc2.shape, BF16),
            pltpu.VMEM((2, rows, width), BF16), pltpu.VMEM((rows, width), BF16), pltpu.VMEM((rows, 3 * heads * LANES), BF16),
            pltpu.VMEM((rows, width), BF16), pltpu.VMEM((rows, width), F32),
            pltpu.VMEM((3, rows, CHUNK), F32), pltpu.VMEM((2, rows, CHUNK), BF16), pltpu.VMEM((2, GROUP, rows, HALF), F32),
            pltpu.VMEM((images, 16, width), BF16),
            *(pltpu.VMEM(vector.shape, F32) for vector in vectors),
            DMA((3, hidden // CHUNK)), PAIR, PAIR, DMA((stages,)), DMA(()), DMA((6,)), DMA((3, 2)), PAIR, PAIR,
            pltpu.SemaphoreType.REGULAR],
        compiler_params=pltpu.CompilerParams(collective_id=0, has_side_effects=True, vmem_limit_bytes=LIMIT),
        name="forward",
    )(emb, wqkv, wproj, wfc1, wfc2, *vectors)


def run_backward(dims, gtop, wqkv, wproj, wfc1, wfc2, g1, g2, x_s, qkv_s, h_s, d_s, p_s):
    stages, images, tokens, heads, head = dims
    rows, width = x_s.shape[1:]
    hidden = wfc1.shape[0]
    hbm = lambda *shape: jax.ShapeDtypeStruct((images, rows) + shape, BF16)
    sizes = (width,) * 6 + (3 * width, hidden)
    return pl.pallas_call(
        functools.partial(backward_kernel, dims),
        out_shape=(hbm(width), hbm(hidden), hbm(width), hbm(3 * width), hbm(width)) + tuple(jax.ShapeDtypeStruct((1, size), F32) for size in sizes),
        in_specs=[ANY] * 5 + [VMEM] * 2 + [ANY] * 5,
        out_specs=(ANY,) * 5 + (VMEM,) * 8,
        scratch_shapes=[
            pltpu.VMEM((3, -(-width // 256) * LANES, width), BF16), pltpu.VMEM(wproj.shape, BF16), pltpu.VMEM(wfc1.shape, BF16), pltpu.VMEM(wfc2.shape, BF16),
            pltpu.VMEM((2, rows, width), BF16), pltpu.VMEM((rows, width), F32), pltpu.VMEM((2 * GROUP, rows, HALF), F32),
            pltpu.VMEM((2, rows, CHUNK), BF16), pltpu.VMEM((2, rows, CHUNK), BF16),
            pltpu.VMEM((rows, width), BF16), pltpu.VMEM((rows, width), BF16), pltpu.VMEM((rows, heads * LANES), BF16),
            pltpu.VMEM((rows, 3 * heads * LANES), BF16), pltpu.VMEM((rows, 3 * width), BF16),
            pltpu.VMEM((rows, width), BF16), pltpu.VMEM((1, width), F32), pltpu.VMEM((1, width), F32),
            *(pltpu.VMEM((8, size), F32) for size in sizes),
            DMA((3, hidden // CHUNK)), TRIPLE, PAIR, PAIR, DMA((stages,)), DMA(()), DMA((4,)), TRIPLE, DMA((4,)), PAIR, PAIR,
            pltpu.SemaphoreType.REGULAR],
        compiler_params=pltpu.CompilerParams(collective_id=1, has_side_effects=True, vmem_limit_bytes=LIMIT),
        name="backward",
    )(gtop, wqkv, wproj, wfc1, wfc2, g1, g2, x_s, qkv_s, h_s, d_s, p_s)


def head_kernel(inv_count, tops, labels, gain, bias, w_head, b_head, loss, gtop, g_gain, g_bias, g_w_head, g_b_head):
    images, width = tops.shape
    line = lambda ref: ref[:].reshape(1, -1).astype(F32)
    wide_gain = line(gain)
    pooled = layer_norm(tops[:], wide_gain, line(bias))
    logits = dot(pooled, w_head[:], 1, 1) + line(b_head)
    shifted = logits - jnp.max(logits, **ACROSS)
    log_probs = shifted - jnp.log(jnp.sum(jnp.exp(shifted), **ACROSS))
    classes = logits.shape[-1]
    number = lax.broadcasted_iota(jnp.int32, (images, 1), 0)
    label = jnp.zeros((images, 1), jnp.int32)
    for image in range(images):
        label = jnp.where(number == image, labels[image % labels.shape[0], image // labels.shape[0]], label)
    chosen = (lax.broadcasted_iota(jnp.int32, logits.shape, 1) == label).astype(F32)
    target = (1.0 - SMOOTH) * chosen + SMOOTH / classes
    parts = jnp.sum(target * log_probs, **ACROSS)
    loss[:] = -jnp.sum(parts, **DOWN) * inv_count
    grad_logits = (jnp.exp(log_probs) - target) * inv_count
    low = grad_logits.astype(BF16)
    g_w_head[:] = dot(low, pooled, 0, 0)
    g_b_head[:] = jnp.sum(grad_logits, axis=0)
    grad = dot(low, w_head[:]).astype(BF16).astype(F32)
    grad_in, by_unit = norm_backward(grad, tops[:], wide_gain)
    g_gain[:] = jnp.sum(by_unit, axis=0)
    g_bias[:] = jnp.sum(grad, axis=0)
    gtop[:] = jnp.zeros_like(gtop)
    for image in range(images):
        gtop[image, 0:1, :] = grad_in[image:image + 1].astype(BF16)


def run_head(inv_count, tops, labels, gain, bias, w_head, b_head):
    images, width = tops.shape
    classes = w_head.shape[0]
    shape = lambda *dims, dtype=F32: jax.ShapeDtypeStruct(dims, dtype)
    return pl.pallas_call(
        functools.partial(head_kernel, inv_count),
        out_shape=(shape(1, 1), shape(images, 16, width, dtype=BF16), shape(width), shape(width), shape(classes, width), shape(classes)),
        in_specs=[VMEM, pl.BlockSpec(memory_space=pltpu.SMEM)] + [VMEM] * 4,
        out_specs=(VMEM,) * 6,
        compiler_params=pltpu.CompilerParams(vmem_limit_bytes=LIMIT),
        name="head",
    )(tops, labels, gain, bias, w_head, b_head)


def weight_kernel(*refs):
    count = (len(refs) - 15 - 11) // 2
    fc2_l, qkv_l, proj_l, patch_l, fc2_r, qkv_r, proj_r, patch_r, fc1_l, fc1_r = refs[:10]
    sums = refs[10:10 + count]
    fc2_o, qkv_o, proj_o, patch_o, fc1_o = refs[10 + count:15 + count]
    sums_out = refs[15 + count:15 + 2 * count]
    lhs, rhs, out, turned, block, wide, lsem, rsem, osem, bsem, wsem = refs[15 + 2 * count:]
    width = rhs.shape[2]
    size, wide_size = lhs.shape[2], block.shape[2]
    tail = width % size
    patches = patch_l.shape[1] // size + 1
    ends = [fc2_l.shape[1] // size]
    ends.append(ends[0] + qkv_l.shape[1] // size)
    ends.append(ends[1] + width // size + 1)
    ends.append(ends[2] + patches)
    starts = [0] + ends[:3]
    steps = ends[3]
    wide_steps = fc1_r.shape[1] // wide_size

    def lines(at, unit):
        return pl.ds(pl.multiple_of(at * unit, LANES), unit)

    def left_copy(step, act):
        slot = flip(step)
        for product, source in enumerate((fc2_l, qkv_l, proj_l, patch_l)):
            full = source.shape[1] // size
            first = starts[product]

            @pl.when(jnp.logical_and(step >= first, step < first + full))
            def _():
                act(pltpu.make_async_copy(source.at[:, lines(step - first, size)], lhs.at[slot], lsem.at[slot]))

            if source.shape[1] % size:
                @pl.when(step == first + full)
                def _():
                    act(pltpu.make_async_copy(source.at[:, pl.ds(full * size, tail)], lhs.at[slot, :, pl.ds(0, tail)], lsem.at[slot]))

    def out_copy(step, act):
        slot = flip(step)
        for product, target in enumerate((fc2_o, qkv_o, proj_o)):
            full = target.shape[0] // size
            first = starts[product]

            @pl.when(jnp.logical_and(step >= first, step < first + full))
            def _():
                act(pltpu.make_async_copy(out.at[slot], target.at[lines(step - first, size)], osem.at[slot]))

            if target.shape[0] % size:
                @pl.when(step == first + full)
                def _():
                    act(pltpu.make_async_copy(out.at[slot, pl.ds(0, tail)], target.at[pl.ds(full * size, tail)], osem.at[slot]))

    def right_copy(product):
        source = (fc2_r, qkv_r, proj_r, patch_r, fc1_l)[product]
        return pltpu.make_async_copy(source, rhs.at[product % 2], rsem.at[product % 2])

    def block_copy(step):
        slot = flip(step)
        return pltpu.make_async_copy(fc1_r.at[:, lines(step, wide_size)], block.at[slot], bsem.at[slot])

    def wide_copy(step):
        slot = flip(step)
        return pltpu.make_async_copy(wide.at[slot], fc1_o.at[:, lines(step, wide_size)], wsem.at[slot])

    start = lambda copy: copy.start()
    wait = lambda copy: copy.wait()
    left_copy(0, start)
    right_copy(0).start()
    right_copy(1).start()
    for given, passed in zip(sums, sums_out):
        passed[:] = given[:]

    def one_step(step, carry):
        slot = flip(step)

        @pl.when(step >= 1)
        def _():
            out_copy(step - 1, start)

        @pl.when(step >= 2)
        def _():
            out_copy(step - 2, wait)

        @pl.when(step + 1 < steps)
        def _():
            left_copy(step + 1, start)

        for product, first in enumerate(starts):
            @pl.when(step == first)
            def _(product=product):
                right_copy(product).wait()
                if product >= 1:
                    right_copy(product + 1).start()

        @pl.when(step == steps - 1)
        def _():
            block_copy(0).start()

        left_copy(step, wait)
        which = lax.rem(sum((step >= end).astype(jnp.int32) for end in ends[:3]), 2)
        out[slot] = dot(lhs[slot], rhs[which], 0, 0)
        for at in range(patches):
            count = min(size, patch_o.shape[0] - at * size)

            @pl.when(step == starts[3] + at)
            def _():
                patch_o[at * size:at * size + count, :] = out[slot, :count, :]

        return carry

    lax.fori_loop(0, steps, one_step, 0)
    right_copy(4).wait()
    turned[:] = rhs[0].T

    def wide_step(step, carry):
        slot = flip(step)

        @pl.when(step >= 1)
        def _():
            wide_copy(step - 1).start()

        @pl.when(step >= 2)
        def _():
            wide_copy(step - 2).wait()

        @pl.when(step + 1 < wide_steps)
        def _():
            block_copy(step + 1).start()

        block_copy(step).wait()
        wide[slot] = dot(turned[:], block[slot])
        return carry

    lax.fori_loop(0, wide_steps, wide_step, 0)
    wide_copy(wide_steps - 1).start()
    wide_copy(wide_steps - 2).wait()
    wide_copy(wide_steps - 1).wait()


def run_weights(lefts, rights, patch_size, sums):
    fc2_l, qkv_l, proj_l, patch_l, fc1_l = lefts
    fc2_r, qkv_r, proj_r, patch_r, fc1_r = rights
    rows, width = fc2_r.shape
    size, wide_size = 3 * LANES, 4 * LANES
    shapes = [(left.shape[1], right.shape[1]) for left, right in zip(lefts, rights)]
    shapes[3] = (patch_size, width)
    flops = sum(2 * rows * a * b for a, b in shapes)
    return pl.pallas_call(
        weight_kernel,
        out_shape=tuple(jax.ShapeDtypeStruct(shape, F32) for shape in shapes) + tuple(jax.ShapeDtypeStruct(total.shape, F32) for total in sums),
        in_specs=[ANY] * 10 + [VMEM] * len(sums),
        out_specs=(ANY,) * 3 + (VMEM, ANY) + (VMEM,) * len(sums),
        scratch_shapes=[
            pltpu.VMEM((2, rows, size), BF16), pltpu.VMEM((2, rows, width), BF16), pltpu.VMEM((2, size, width), F32),
            pltpu.VMEM((width, rows), BF16), pltpu.VMEM((2, rows, wide_size), BF16), pltpu.VMEM((2, width, wide_size), F32),
            PAIR, PAIR, PAIR, PAIR, PAIR],
        compiler_params=pltpu.CompilerParams(vmem_limit_bytes=LIMIT),
        cost_estimate=pl.CostEstimate(flops=flops, bytes_accessed=4 * sum(a * b for a, b in shapes), transcendentals=0),
        name="weights",
    )(fc2_l, qkv_l, proj_l, patch_l, fc2_r, qkv_r, proj_r, patch_r, fc1_l, fc1_r, *sums)


def matmul_rows(spec, left, right):
    return jnp.einsum(spec, left, right, preferred_element_type=F32)


def solution(mesh):
    stages = mesh.shape["pp"]
    in_specs = (P("dp"), P("dp"), P(), P(), P(), P()) + (P("pp"),) * 12 + (P(),) * 4
    out_specs = (P("dp"),) * 5 + (P(("dp", "pp")),) * 12 + (P("dp"),) * 4

    def body(patches, labels, w_patch, b_patch, cls_token, pos_embed, *rest):
        ln1_gain, ln1_bias, w_qkv, b_qkv, w_proj, b_proj, ln2_gain, ln2_bias, w_fc1, b_fc1, w_fc2, b_fc2 = (tensor[0] for tensor in rest[:12])
        lnf_gain, lnf_bias, w_head, b_head = rest[12:]
        tokens, width = pos_embed.shape
        heads, head = w_qkv.shape[2:]
        images = labels.size
        inv_count = 1.0 / images
        rows = -(-tokens // 16) * 16
        dims = (stages, images, tokens, heads, head)

        patch_size = patches.shape[-1]
        spare = -patch_size % LANES
        patch_rows = jnp.pad(patches.reshape((images,) + patches.shape[2:]), ((0, 0), (1, rows - tokens), (0, spare)))
        w_embed = jnp.pad(w_patch, ((0, spare), (0, 0)))
        is_patch = lax.broadcasted_iota(jnp.int32, (rows, 1), 0) > 0
        base = jnp.pad(pos_embed, ((0, rows - tokens), (0, 0))).astype(F32) + jnp.where(is_patch, b_patch.astype(F32), cls_token.astype(F32))
        embedded = (matmul_rows("inp,pd->ind", patch_rows, w_embed) + base).astype(BF16)

        line = lambda tensor: tensor.reshape(1, -1)
        wqkv_t = jnp.transpose(w_qkv, (1, 2, 3, 0)).reshape(3 * width, width)
        big = (wqkv_t, w_proj.reshape(width, width), w_fc1, w_fc2)
        vectors = tuple(map(line, (ln1_gain, ln1_bias, b_qkv, b_proj, ln2_gain, ln2_bias, b_fc1, b_fc2)))
        vectors = vectors[:2] + (vectors[2].reshape(3, 1, width),) + vectors[3:]
        x_s, a_s, qkv_s, c_s, h_s, n_s, d_s, g_s, p_s, tops = run_forward(dims, embedded, *big, vectors)

        loss, gtop, g_lnf_gain, g_lnf_bias, g_w_head, g_b_head = run_head(
            inv_count, tops, jnp.transpose(labels), lnf_gain, lnf_bias, jnp.transpose(w_head), b_head)

        gy_s, gpre_s, gmid_s, gqkv_s, gemb, *sums = run_backward(dims, gtop, big[0], *map(jnp.transpose, big[1:]), vectors[0], vectors[4], x_s, qkv_s, h_s, d_s, p_s)
        flat = lambda array: array.reshape(images * rows, -1)
        g_w_fc2, g_w_qkv, g_w_proj, g_w_patch, g_w_fc1, *sums = run_weights(
            tuple(map(flat, (g_s, gqkv_s, c_s, patch_rows, n_s))), tuple(map(flat, (gy_s, a_s, gmid_s, gemb, gpre_s))), patch_size, sums)
        g_ln1_gain, g_ln1_bias, g_ln2_gain, g_ln2_bias, g_b_proj, g_b_fc2, g_b_qkv, g_b_fc1 = sums
        g_w_qkv = jnp.transpose(g_w_qkv.reshape(3, heads, head, width), (3, 0, 1, 2))[None]
        layer_grads = (
            g_ln1_gain, g_ln1_bias, g_w_qkv, g_b_qkv.reshape(1, 3, heads, head), g_w_proj.reshape(1, heads, head, width), g_b_proj,
            g_ln2_gain, g_ln2_bias, g_w_fc1[None], g_b_fc1, g_w_fc2[None], g_b_fc2,
        )
        g_pos_embed = jnp.sum(gemb[:, :tokens].astype(F32), axis=0)
        embed_grads = (
            g_w_patch, jnp.sum(g_pos_embed[1:], axis=0), g_pos_embed[0], g_pos_embed,
        )
        return (loss.reshape(1),) + embed_grads + layer_grads + (g_lnf_gain, g_lnf_bias, jnp.transpose(g_w_head), g_b_head)

    return jax.shard_map(body, mesh=mesh, in_specs=in_specs, out_specs=out_specs, check_vma=False)
```

```python
import functools
import math
import jax
import jax.numpy as jnp
from jax import lax
from jax.experimental import pallas as pl
from jax.experimental.pallas import tpu as pltpu
from jax.sharding import PartitionSpec as P

EPS = 1e-6
SMOOTH = 0.1
F32 = jnp.float32
BF16 = jnp.bfloat16
MESH = pl.DeviceIdType.MESH
LANES = 128
HALF = 384
CHUNK = 2 * HALF
GROUP = 4
BLOCK = 136
DOWN = {"axis": 0, "keepdims": True}
ACROSS = {"axis": -1, "keepdims": True}


def flip(index):
    return lax.rem(index, 2)


def third(index):
    return lax.rem(index, 3)


def layer_norm(hidden, gain, bias):
    values = hidden.astype(F32)
    centered = values - jnp.mean(values, **ACROSS)
    variance = jnp.mean(jnp.square(centered), **ACROSS)
    return (centered * lax.rsqrt(variance + EPS) * gain + bias).astype(BF16)


def dot(left, right, left_axis=1, right_axis=0):
    return lax.dot_general(left, right, (((left_axis,), (right_axis,)), ((), ())), preferred_element_type=F32)


def by_rows(rows, visit):
    def step(index, carry):
        visit(pl.ds(pl.multiple_of(index * BLOCK, BLOCK), BLOCK))
        return carry

    lax.fori_loop(0, rows // BLOCK, step, 0)
    if rows % BLOCK:
        visit(pl.ds(rows - rows % BLOCK, rows % BLOCK))


def fold(values):
    rows, columns = values.shape
    return jnp.sum(values.reshape(rows // 8, 8, columns), axis=0)


def everyone(stage, stages):
    barrier = pltpu.get_barrier_semaphore()
    for hop in range(1, stages):
        pl.semaphore_signal(barrier, device_id={"pp": lax.rem(stage + hop, stages)}, device_id_type=MESH)
    pl.semaphore_wait(barrier, stages - 1)


def weight_copies(wproj, wfc1, wfc2, vproj, vfc1, vfc2, sems):
    def of_chunk(source, target, which, by_lines):
        def copy(chunk):
            span = pl.ds(pl.multiple_of(chunk * CHUNK, CHUNK), CHUNK)
            part = span if by_lines else (slice(None), span)
            return pltpu.make_async_copy(source.at[part], target.at[part], sems.at[which, chunk])
        return copy

    proj = pltpu.make_async_copy(wproj, vproj, sems.at[0, 0])
    return proj, of_chunk(wfc1, vfc1, 1, False), of_chunk(wfc2, vfc2, 2, True)


def forward_kernel(dims, *refs):
    (emb, wqkv, wproj, wfc1, wfc2, *given,
     x_s, a_s, qkv_s, c_s, h_s, n_s, d_s, g_s, p_s, tops_out,
     vqkv, vproj, vfc1, vfc2, xin, act, qkv, mid, yacc, ubuf, gbuf, tops,
     g1, b1, bqkv, bproj, g2, b2, bfc2,
     wsem, qsem, recv_sem, send_sem, top_sem, save_sem, usem, gsem, psem, free_sem) = refs
    stages, images, tokens, heads, head = dims
    rows, width = mid.shape
    chunks = vfc1.shape[1] // CHUNK
    stage = lax.axis_index("pp")
    is_first = stage == 0
    is_last = stage == stages - 1
    scale2 = head ** -0.5 / math.log(2.0)


    def qkv_copy(part):
        lines = pl.ds(pl.multiple_of(part * width, LANES), width)
        return pltpu.make_async_copy(wqkv.at[lines], vqkv.at[lines], qsem.at[part])

    def emb_copy(image, slot):
        return pltpu.make_async_copy(emb.at[image], xin.at[slot], recv_sem.at[slot])

    @pl.when(is_first)
    def _():
        emb_copy(0, 0).start()
        emb_copy(1, 1).start()

    proj_copy, fc1_copy, fc2_copy = weight_copies(wproj, wfc1, wfc2, vproj, vfc1, vfc2, wsem)
    for part in range(3):
        qkv_copy(part).start()
    proj_copy.start()
    for chunk in range(chunks):
        fc1_copy(chunk).start()
        fc2_copy(chunk).start()
    qkv[:] = jnp.zeros_like(qkv)
    *lows, bfc1, low = given
    for low, wide in zip((*lows, low), (g1, b1, bqkv, bproj, g2, b2, bfc2)):
        wide[:] = low[:].astype(F32)
    everyone(stage, stages)

    def saves(image, slot):
        pairs = ((xin.at[slot], x_s), (act, a_s), (qkv, qkv_s), (act, c_s), (mid, h_s), (act, n_s))
        return [pltpu.make_async_copy(src, dst.at[image], save_sem.at[at]) for at, (src, dst) in enumerate(pairs)]

    class u_save:
        def __init__(self, image, chunk):
            slot = third(chunk)
            self.copies = [
                pltpu.make_async_copy(ubuf.at[slot, :, pl.ds(side * HALF, HALF)], d_s.at[image, chunk * 2 + side], usem.at[slot, side])
                for side in range(2)]

        def start(self):
            for copy in self.copies:
                copy.start()

        def wait(self):
            for copy in self.copies:
                copy.wait()

    def g_save(image, chunk):
        slot = flip(chunk)
        return pltpu.make_async_copy(gbuf.at[slot], g_s.at[image, :, pl.ds(pl.multiple_of(chunk * CHUNK, CHUNK), CHUNK)], gsem.at[slot])

    def p_slot(number):
        slot = number % 9
        if slot < 6:
            return ubuf.at[slot // 2, :, pl.ds(slot % 2 * HALF, HALF)]
        return yacc.at[:, pl.ds((slot - 6) * HALF, HALF)]

    def p_save(image, number):
        return pltpu.make_async_copy(p_slot(number), p_s.at[image, number], psem.at[number % 9])

    def top_copy(image, other):
        return pltpu.make_async_remote_copy(
            src_ref=mid.at[pl.ds(0, 8)], dst_ref=tops.at[image], send_sem=send_sem.at[1 + other], recv_sem=top_sem,
            device_id={"pp": other}, device_id_type=MESH)

    def next_copy(image, slot):
        return pltpu.make_async_remote_copy(
            src_ref=mid, dst_ref=xin.at[slot], send_sem=send_sem.at[0], recv_sem=recv_sem.at[slot],
            device_id={"pp": lax.rem(stage + 1, stages)}, device_id_type=MESH)

    def wait_sent(image):
        @pl.when(jnp.logical_not(is_last))
        def _():
            next_copy(image, 0).wait_send()

        @pl.when(is_last)
        def _():
            for other in range(stages - 1):
                top_copy(image, other).wait_send()

    def one_image(image, carry):
        slot = flip(image)
        save_x, save_a, save_qkv, save_c, save_h, save_n = saves(image, slot)
        emb_copy(image, slot).wait()
        save_x.start()

        @pl.when(image > 0)
        def _():
            save_n.wait()
            save_qkv.wait()

        def norm1(lines):
            act[lines, :] = layer_norm(xin[slot, lines, :], g1[:], b1[:])

        by_rows(rows, norm1)
        save_a.start()

        def qkv_part(part, carry):
            @pl.when(image == 0)
            def _():
                qkv_copy(part).wait()

            lines = pl.ds(pl.multiple_of(part * width, LANES), width)
            low = (dot(act[:], vqkv[lines, :], 1, 1) + bqkv[part]).astype(BF16)
            for at in range(heads):
                lane = part * (heads * LANES) + at * LANES
                qkv[:, pl.ds(pl.multiple_of(lane, LANES), head)] = low[:, at * head:(at + 1) * head]
            return carry

        lax.fori_loop(0, 3, qkv_part, 0)
        save_qkv.start()

        save_a.wait()

        @pl.when(image > 0)
        def _():
            for chunk in range(3):
                u_save(image, chunk).wait()

        def scores_of(number):
            q, k = (qkv[:, lane:lane + LANES] for lane in (number * LANES, (heads + number) * LANES))
            return dot(k, q, 1, 1)

        def attend(number, scores):
            if number == 9:
                for slot in range(6):
                    p_save(image, slot).wait()
            if number > 14:
                p_save(image, number - 9).wait()
            v = qkv[:, (2 * heads + number) * LANES:(2 * heads + number + 1) * LANES]
            top, tail = scores[:tokens - 1], scores[tokens - 1:]
            most = jnp.maximum(jnp.max(top, **DOWN), tail[:1])
            top = jnp.exp2((top - most) * scale2)
            real = lax.broadcasted_iota(jnp.int32, tail.shape, 0) < 1
            tail = jnp.where(real, jnp.exp2(jnp.minimum(tail - most, 0.0) * scale2), 0.0)
            inv = 1.0 / (jnp.sum(top, **DOWN) + jnp.sum(tail, **DOWN))
            probs = jnp.concatenate([top, tail], axis=0) * inv
            p_slot(number)[:, :rows] = probs
            act[:, number * head:(number + 1) * head] = dot(probs.astype(BF16), v, 0, 0).astype(BF16)[:, :head]
            p_save(image, number).start()

        scores = scores_of(0)
        for number in range(heads):
            later = scores_of(number + 1) if number + 1 < heads else None
            attend(number, scores)
            scores = later
        save_c.start()

        @pl.when(image == 0)
        def _():
            proj_copy.wait()

        @pl.when(image > 0)
        def _():
            wait_sent(image)

        mid[:] = (dot(act[:], vproj[:]) + bproj[:] + xin[slot].astype(F32)).astype(BF16)
        save_h.start()
        save_x.wait()

        @pl.when(jnp.logical_and(is_first, image + 2 < images))
        def _():
            emb_copy(image + 2, slot).start()

        @pl.when(jnp.logical_and(stage > 0, image + 2 < images))
        def _():
            pl.semaphore_signal(free_sem, device_id={"pp": lax.rem(stage + stages - 1, stages)}, device_id_type=MESH)

        save_c.wait()
        for number in (7, 8, 15):
            p_save(image, number).wait()

        def norm2(lines):
            hidden = mid[lines, :]
            act[lines, :] = layer_norm(hidden, g2[:], b2[:])
            yacc[lines, :] = hidden.astype(F32) + bfc2[:]

        by_rows(rows, norm2)
        save_n.start()

        @pl.when(image == 0)
        def _():
            fc1_copy(0).wait()

        for number in range(9, 15):
            p_save(image, number).wait()

        @pl.when(image > 0)
        def _():
            for chunk in range(2):
                g_save(image, chunk).wait()

        def fc1(chunk):
            columns = pl.ds(pl.multiple_of(chunk * CHUNK, CHUNK), CHUNK)
            ubuf[third(chunk)] = dot(act[:], vfc1[:, columns]) + bfc1[:, columns].astype(F32)

        def gelu(chunk):
            slot3, slot2 = third(chunk), flip(chunk)
            pre = ubuf[slot3]
            cdf = 0.5 + 0.5 * lax.erf(pre * (0.5 ** 0.5))
            pdf = jnp.exp2(pre * pre * (-0.5 / math.log(2.0))) * ((2.0 * math.pi) ** -0.5)
            activ = (pre * cdf).astype(BF16)
            gbuf[slot2] = activ
            ubuf[slot3] = cdf + pre * pdf
            return activ

        def fc2(chunk, activ):
            yacc[:] += dot(activ, vfc2[pl.ds(pl.multiple_of(chunk * CHUNK, CHUNK), CHUNK), :])

        fc1(0)

        def mlp_step(chunk, carry):
            @pl.when(chunk >= 3)
            def _():
                u_save(image, chunk).wait()
                g_save(image, chunk - 1).wait()

            @pl.when(image == 0)
            def _():
                fc1_copy(chunk).wait()
                fc2_copy(chunk - 1).wait()

            @pl.when(chunk >= 2)
            def _():
                u_save(image, chunk - 2).start()
                g_save(image, chunk - 2).start()

            activ = gelu(chunk - 1)
            fc1(chunk)
            fc2(chunk - 1, activ)
            return carry

        lax.fori_loop(1, chunks, mlp_step, 0)

        @pl.when(image == 0)
        def _():
            fc2_copy(chunks - 1).wait()

        g_save(image, chunks - 1).wait()
        u_save(image, chunks - 2).start()
        g_save(image, chunks - 2).start()
        fc2(chunks - 1, gelu(chunks - 1))
        u_save(image, chunks - 1).start()
        g_save(image, chunks - 1).start()

        save_h.wait()
        mid[:] = yacc[:].astype(BF16)

        @pl.when(jnp.logical_and(jnp.logical_not(is_last), image >= 2))
        def _():
            pl.semaphore_wait(free_sem, 1)

        @pl.when(jnp.logical_not(is_last))
        def _():
            next_copy(image, slot).start()

        @pl.when(is_last)
        def _():
            for other in range(stages - 1):
                top_copy(image, other).start()
            tops[image] = mid[pl.ds(0, 8), :]

        return carry

    lax.fori_loop(0, images, one_image, 0)
    wait_sent(images - 1)
    _, _, save_qkv, _, _, save_n = saves(images - 1, 0)
    save_qkv.wait()
    save_n.wait()
    for chunk in range(3):
        u_save(images - 1, chunk).wait()
    for chunk in range(2):
        g_save(images - 1, chunk).wait()

    @pl.when(jnp.logical_not(is_last))
    def _():
        pltpu.make_async_copy(tops, tops, top_sem).wait()

    for image in range(images):
        tops_out[image:image + 1, :] = tops[image, 0:1, :]


def norm_backward(grad, hidden, gain):
    values = hidden.astype(F32)
    centered = values - jnp.mean(values, **ACROSS)
    inv = lax.rsqrt(jnp.mean(jnp.square(centered), **ACROSS) + EPS)
    unit = centered * inv
    scaled = grad * gain
    grad_in = inv * (scaled - jnp.mean(scaled, **ACROSS) - unit * jnp.mean(scaled * unit, **ACROSS))
    return grad_in, grad * unit


def backward_kernel(dims, *refs):
    (gtop, wqkv, wproj, wfc1, wfc2, low1, low2, x_s, qkv_s, h_s, d_s, p_s,
     gy_s, gpre_s, gmid_s, gqkv_s, gemb, *sums_out,
     vqkv, vproj, vfc1, vfc2, gin, acc, shared, abuf, gbuf, hid, gmid, gctx, qkv, gqkv, gout, g1, g2,
     sum1g, sum1b, sum2g, sum2b, sumproj, sumfc2, sumqkv, sumfc1,
     wsem, qsem, recv_sem, top_sem, send_sem, emb_sem, relay_sem, save_sem, load_sem, dsem, gsem, psem, free_sem) = refs
    stages, images, tokens, heads, head = dims
    rows, width = gmid.shape
    chunks = vfc1.shape[1] // CHUNK
    groups = heads // GROUP
    stage = lax.axis_index("pp")
    is_first = stage == 0
    is_last = stage == stages - 1
    scale = head ** -0.5

    pieces = ((0, vqkv.shape[1]), (vqkv.shape[1], width - vqkv.shape[1]))

    def qkv_copy(part, side):
        slot = third(part * 2 + side)
        at, size = pieces[side]
        lines = pl.ds(pl.multiple_of(third(part) * width + at, 128), size)
        return pltpu.make_async_copy(wqkv.at[lines], vqkv.at[slot, pl.ds(0, size)], qsem.at[slot])

    def top_copy(image, slot):
        return pltpu.make_async_copy(gtop.at[image], gin.at[slot, pl.ds(0, 16)], top_sem.at[slot])

    def d_load(image, chunk):
        slot = lax.rem(chunk, 4)
        return pltpu.make_async_copy(d_s.at[image, pl.ds(chunk * 2, 2)], shared.at[pl.ds(slot * 2, 2)], dsem.at[slot])

    def g_save(image, chunk):
        slot = flip(chunk)
        return pltpu.make_async_copy(gbuf.at[slot], gpre_s.at[image, :, pl.ds(pl.multiple_of(chunk * CHUNK, CHUNK), CHUNK)], gsem.at[slot])

    def p_load(image, group):
        slot = group % 2
        return pltpu.make_async_copy(p_s.at[image, pl.ds(group * GROUP, GROUP)], shared.at[pl.ds(slot * GROUP, GROUP)], psem.at[slot])

    def saves(image, slot):
        pairs = ((gin.at[slot], gy_s), (gmid, gmid_s), (gqkv, gqkv_s))
        return [pltpu.make_async_copy(src, dst.at[image], save_sem.at[at]) for at, (src, dst) in enumerate(pairs)]

    def loads(image):
        pairs = ((h_s, hid), (x_s, hid), (qkv_s, qkv))
        return [pltpu.make_async_copy(src.at[image], dst, load_sem.at[at]) for at, (src, dst) in enumerate(pairs)]

    def next_copy(slot):
        return pltpu.make_async_remote_copy(
            src_ref=gout, dst_ref=gin.at[slot], send_sem=send_sem.at[0], recv_sem=recv_sem.at[slot],
            device_id={"pp": lax.rem(stage + stages - 1, stages)}, device_id_type=MESH)

    def emb_send(image, other):
        return pltpu.make_async_remote_copy(
            src_ref=gout, dst_ref=gemb.at[image], send_sem=send_sem.at[other], recv_sem=emb_sem.at[image],
            device_id={"pp": other}, device_id_type=MESH)

    def emb_relay(image):
        return pltpu.make_async_remote_copy(
            src_ref=gemb.at[image], dst_ref=gemb.at[image], send_sem=relay_sem.at[image], recv_sem=emb_sem.at[image],
            device_id={"pp": stages - 1}, device_id_type=MESH)

    def emb_local(image):
        return pltpu.make_async_copy(gout, gemb.at[image], save_sem.at[3])

    def wait_sent(image):
        @pl.when(jnp.logical_not(is_first))
        def _():
            next_copy(0).wait_send()

        @pl.when(is_first)
        def _():
            for other in range(1, stages - 1):
                emb_send(image, other).wait_send()
            emb_local(image).wait()

    @pl.when(is_last)
    def _():
        gin[:] = jnp.zeros_like(gin)
        top_copy(0, 0).start()
        top_copy(1, 1).start()

    proj_copy, fc1_copy, fc2_copy = weight_copies(wproj, wfc1, wfc2, vproj, vfc1, vfc2, wsem)
    for chunk in range(chunks):
        fc2_copy(chunk).start()
        if chunk < 4:
            d_load(0, chunk).start()
        fc1_copy(chunk).start()
    loads(0)[0].start()
    proj_copy.start()
    for part, side in ((0, 0), (0, 1), (1, 0)):
        qkv_copy(part, side).start()
    gctx[:] = jnp.zeros_like(gctx)
    sums_out, totals = sums_out[:8], (sum1g, sum1b, sum2g, sum2b, sumproj, sumfc2, sumqkv, sumfc1)
    for total in totals:
        total[:] = jnp.zeros_like(total)
    g1[:] = low1[:].astype(F32)
    g2[:] = low2[:].astype(F32)
    everyone(stage, stages)

    def one_image(image, carry):
        slot = flip(image)
        more = image + 1 < images
        save_gy, save_mid, save_qkv = saves(image, slot)
        load_h, load_x, load_qkv = loads(image)

        @pl.when(is_last)
        def _():
            top_copy(image, slot).wait()

        @pl.when(jnp.logical_not(is_last))
        def _():
            next_copy(slot).wait_recv()

        save_gy.start()

        load_qkv.start()

        @pl.when(image == 0)
        def _():
            fc2_copy(0).wait()

        @pl.when(image > 0)
        def _():
            for chunk in range(2):
                g_save(image, chunk).wait()

        acc[:] = jnp.zeros_like(acc)

        def fc2(chunk):
            lines = pl.ds(pl.multiple_of(chunk * CHUNK, CHUNK), CHUNK)
            abuf[flip(chunk)] = dot(gin[slot], vfc2[lines, :], 1, 1).astype(BF16)

        def gelu(chunk):
            columns = pl.ds(pl.multiple_of(chunk * CHUNK, CHUNK), CHUNK)
            slot2 = flip(chunk)
            slot4 = lax.rem(chunk, 4)
            pre = abuf[slot2].astype(F32) * jnp.concatenate([shared[slot4 * 2], shared[slot4 * 2 + 1]], axis=1)
            sumfc1[:, columns] += fold(pre)
            low = pre.astype(BF16)
            gbuf[slot2] = low
            return low

        def fc1(chunk, low):
            columns = pl.ds(pl.multiple_of(chunk * CHUNK, CHUNK), CHUNK)
            acc[:] += dot(low, vfc1[:, columns], 1, 1)

        fc2(0)

        def mlp_step(chunk, carry):
            d_load(image, chunk - 1).wait()

            @pl.when(image == 0)
            def _():
                fc2_copy(chunk).wait()
                fc1_copy(chunk - 1).wait()

            @pl.when(chunk >= 3)
            def _():
                g_save(image, chunk - 1).wait()

            @pl.when(chunk >= 2)
            def _():
                g_save(image, chunk - 2).start()

                @pl.when(chunk + 2 < chunks)
                def _():
                    d_load(image, chunk + 2).start()

            low = gelu(chunk - 1)
            fc2(chunk)
            fc1(chunk - 1, low)
            return carry

        lax.fori_loop(1, chunks, mlp_step, 0)
        d_load(image, chunks - 1).wait()

        @pl.when(image == 0)
        def _():
            fc1_copy(chunks - 1).wait()

        g_save(image, chunks - 1).wait()
        g_save(image, chunks - 2).start()
        fc1(chunks - 1, gelu(chunks - 1))
        g_save(image, chunks - 1).start()

        for group in range(2):
            p_load(image, group).start()
        load_h.wait()

        @pl.when(image > 0)
        def _():
            save_mid.wait()
            save_qkv.wait()

        def back2(lines):
            grad = acc[lines, :].astype(BF16).astype(F32)
            grad_in, by_unit = norm_backward(grad, hid[lines, :], g2[:])
            sum2g[:] += fold(by_unit)
            sum2b[:] += fold(grad)
            top = gin[slot, lines, :].astype(F32)
            sumfc2[:] += fold(top)
            low = (top + grad_in).astype(BF16)
            gmid[lines, :] = low
            sumproj[:] += fold(low.astype(F32))

        by_rows(rows, back2)
        save_mid.start()
        load_x.start()
        save_gy.wait()

        @pl.when(jnp.logical_and(is_last, image + 2 < images))
        def _():
            top_copy(image + 2, slot).start()

        @pl.when(jnp.logical_and(stage < stages - 1, image + 2 < images))
        def _():
            pl.semaphore_signal(free_sem, device_id={"pp": lax.rem(stage + 1, stages)}, device_id_type=MESH)

        @pl.when(image == 0)
        def _():
            proj_copy.wait()

        low = dot(gmid[:], vproj[:], 1, 1).astype(BF16)
        for number in range(heads):
            gctx[:, number * LANES:number * LANES + head] = low[:, number * head:(number + 1) * head]
        load_qkv.wait()
        def lanes_of(number):
            return slice(number * LANES, (number + 1) * LANES)

        def grad_probs_of(number):
            return dot(qkv[:, lanes_of(2 * heads + number)], gctx[:, lanes_of(number)], 1, 1)

        def attend(number, grad_probs):
            group, inner = number // GROUP, number % GROUP
            if inner == 0:
                p_load(image, group).wait()
            probs = shared[group % 2 * GROUP + inner, :, :rows]
            at = number * head
            mean = jnp.sum(grad_probs * probs, **DOWN)
            low = (probs * (grad_probs - mean) * scale).astype(BF16)
            value = dot(probs.astype(BF16), gctx[:, lanes_of(number)]).astype(BF16)
            gqkv[:, 2 * width + at:2 * width + at + head] = value[:, :head]
            key = dot(low, qkv[:, lanes_of(number)]).astype(BF16)
            gqkv[:, width + at:width + at + head] = key[:, :head]
            query = dot(low, qkv[:, lanes_of(heads + number)], 0, 0).astype(BF16)
            gqkv[:, at:at + head] = query[:, :head]

        grad_probs = grad_probs_of(0)
        for number in range(heads):
            later = grad_probs_of(number + 1) if number + 1 < heads else None
            attend(number, grad_probs)
            grad_probs = later
            if number % GROUP == GROUP - 1 and number // GROUP + 2 < groups:
                p_load(image, number // GROUP + 2).start()
        save_qkv.start()

        def qkv_part(part, carry):
            for side in range(2):
                at, size = pieces[side]
                index = image * 3 + part
                qkv_copy(index, side).wait()
                columns = pl.ds(pl.multiple_of(part * width + at, 128), size)
                piece = gqkv[:, columns]
                sumqkv[:, columns] += fold(piece.astype(F32))
                acc[:] += dot(piece, vqkv[third(index * 2 + side), :size])

                @pl.when(index + 1 + side < images * 3)
                def _():
                    qkv_copy(index + 1 + side, 1 - side).start()

            return carry

        acc[:] = jnp.zeros_like(acc)
        lax.fori_loop(0, 3, qkv_part, 0)

        @pl.when(more)
        def _():
            for chunk in range(4):
                d_load(image + 1, chunk).start()

        load_x.wait()

        @pl.when(image > 0)
        def _():
            wait_sent(image)

        def back1(lines):
            grad = acc[lines, :].astype(BF16).astype(F32)
            grad_in, by_unit = norm_backward(grad, hid[lines, :], g1[:])
            sum1g[:] += fold(by_unit)
            sum1b[:] += fold(grad)
            gout[lines, :] = (gmid[lines, :].astype(F32) + grad_in).astype(BF16)

        by_rows(rows, back1)

        @pl.when(more)
        def _():
            loads(image + 1)[0].start()

        @pl.when(jnp.logical_and(jnp.logical_not(is_first), image >= 2))
        def _():
            pl.semaphore_wait(free_sem, 1)

        @pl.when(jnp.logical_not(is_first))
        def _():
            next_copy(slot).start()

        @pl.when(is_first)
        def _():
            for other in range(1, stages - 1):
                emb_send(image, other).start()
            emb_local(image).start()

        return carry

    lax.fori_loop(0, images, one_image, 0)
    wait_sent(images - 1)
    _, save_mid, save_qkv = saves(images - 1, 0)
    save_mid.wait()
    save_qkv.wait()
    for chunk in range(2):
        g_save(images - 1, chunk).wait()

    for out, total in zip(sums_out, totals):
        out[:] = jnp.sum(total[:], **DOWN)

    @pl.when(jnp.logical_not(is_first))
    def _():
        for image in range(images):
            emb_relay(image).wait_recv()

            @pl.when(stage == stages - 2)
            def _():
                emb_relay(image).start()

    @pl.when(stage == stages - 2)
    def _():
        for image in range(images):
            emb_relay(image).wait_send()


ANY = pl.BlockSpec(memory_space=pl.ANY)
VMEM = pl.BlockSpec(memory_space=pltpu.VMEM)
LIMIT = 67_043_328
DMA = pltpu.SemaphoreType.DMA
PAIR = DMA((2,))
TRIPLE = DMA((3,))


def run_forward(dims, emb, wqkv, wproj, wfc1, wfc2, vectors):
    stages, images, tokens, heads, head = dims
    rows, width = emb.shape[1:]
    hidden = wfc1.shape[1]
    hbm = lambda *shape, dtype=BF16: jax.ShapeDtypeStruct((images, rows) + shape, dtype)
    return pl.pallas_call(
        functools.partial(forward_kernel, dims),
        out_shape=(
            hbm(width), hbm(width), hbm(3 * heads * LANES), hbm(width), hbm(width), hbm(width),
            jax.ShapeDtypeStruct((images, hidden // HALF, rows, HALF), F32), hbm(hidden),
            jax.ShapeDtypeStruct((images, heads, rows, HALF), F32), jax.ShapeDtypeStruct((images, width), BF16)),
        in_specs=[ANY] * 5 + [VMEM] * 8,
        out_specs=(ANY,) * 9 + (VMEM,),
        scratch_shapes=[
            pltpu.VMEM(wqkv.shape, BF16), pltpu.VMEM(wproj.shape, BF16), pltpu.VMEM(wfc1.shape, BF16), pltpu.VMEM(wfc2.shape, BF16),
            pltpu.VMEM((2, rows, width), BF16), pltpu.VMEM((rows, width), BF16), pltpu.VMEM((rows, 3 * heads * LANES), BF16),
            pltpu.VMEM((rows, width), BF16), pltpu.VMEM((rows, width), F32),
            pltpu.VMEM((3, rows, CHUNK), F32), pltpu.VMEM((2, rows, CHUNK), BF16),
            pltpu.VMEM((images, 8, width), BF16),
            *(pltpu.VMEM(vector.shape, F32) for vector in vectors[:6]), pltpu.VMEM(vectors[7].shape, F32),
            DMA((3, hidden // CHUNK)), TRIPLE, PAIR, DMA((stages,)), DMA(()), DMA((6,)), DMA((3, 2)), PAIR, DMA((9,)),
            pltpu.SemaphoreType.REGULAR],
        compiler_params=pltpu.CompilerParams(collective_id=0, has_side_effects=True, vmem_limit_bytes=LIMIT),
        name="forward",
    )(emb, wqkv, wproj, wfc1, wfc2, *vectors)


def run_backward(dims, gtop, wqkv, wproj, wfc1, wfc2, g1, g2, x_s, qkv_s, h_s, d_s, p_s):
    stages, images, tokens, heads, head = dims
    rows, width = x_s.shape[1:]
    hidden = wfc1.shape[1]
    hbm = lambda *shape: jax.ShapeDtypeStruct((images, rows) + shape, BF16)
    sizes = (width,) * 6 + (3 * width, hidden)
    return pl.pallas_call(
        functools.partial(backward_kernel, dims),
        out_shape=(hbm(width), hbm(hidden), hbm(width), hbm(3 * width), hbm(width)) + tuple(jax.ShapeDtypeStruct((1, size), F32) for size in sizes),
        in_specs=[ANY] * 5 + [VMEM] * 2 + [ANY] * 5,
        out_specs=(ANY,) * 5 + (VMEM,) * 8,
        scratch_shapes=[
            pltpu.VMEM((3, -(-width // 256) * LANES, width), BF16), pltpu.VMEM(wproj.shape, BF16), pltpu.VMEM(wfc1.shape, BF16), pltpu.VMEM(wfc2.shape, BF16),
            pltpu.VMEM((2, rows, width), BF16), pltpu.VMEM((rows, width), F32), pltpu.VMEM((2 * GROUP, rows, HALF), F32),
            pltpu.VMEM((2, rows, CHUNK), BF16), pltpu.VMEM((2, rows, CHUNK), BF16),
            pltpu.VMEM((rows, width), BF16), pltpu.VMEM((rows, width), BF16), pltpu.VMEM((rows, heads * LANES), BF16),
            pltpu.VMEM((rows, 3 * heads * LANES), BF16), pltpu.VMEM((rows, 3 * width), BF16),
            pltpu.VMEM((rows, width), BF16), pltpu.VMEM((1, width), F32), pltpu.VMEM((1, width), F32),
            *(pltpu.VMEM((8, size), F32) for size in sizes),
            DMA((3, hidden // CHUNK)), TRIPLE, PAIR, PAIR, DMA((stages,)), DMA((images,)), DMA((images,)), DMA((4,)), TRIPLE, DMA((4,)), PAIR, PAIR,
            pltpu.SemaphoreType.REGULAR],
        compiler_params=pltpu.CompilerParams(collective_id=1, has_side_effects=True, vmem_limit_bytes=LIMIT),
        name="backward",
    )(gtop, wqkv, wproj, wfc1, wfc2, g1, g2, x_s, qkv_s, h_s, d_s, p_s)


def head_kernel(inv_count, tops, labels, gain, bias, w_head, b_head, loss, gtop, g_gain, g_bias, g_w_head, g_b_head):
    images, width = tops.shape
    line = lambda ref: ref[:].reshape(1, -1).astype(F32)
    wide_gain = line(gain)
    pooled = layer_norm(tops[:], wide_gain, line(bias))
    logits = dot(pooled, w_head[:], 1, 1) + line(b_head)
    shifted = logits - jnp.max(logits, **ACROSS)
    log_probs = shifted - jnp.log(jnp.sum(jnp.exp(shifted), **ACROSS))
    classes = logits.shape[-1]
    number = lax.broadcasted_iota(jnp.int32, (images, 1), 0)
    label = jnp.zeros((images, 1), jnp.int32)
    for image in range(images):
        label = jnp.where(number == image, labels[image % labels.shape[0], image // labels.shape[0]], label)
    chosen = (lax.broadcasted_iota(jnp.int32, logits.shape, 1) == label).astype(F32)
    target = (1.0 - SMOOTH) * chosen + SMOOTH / classes
    parts = jnp.sum(target * log_probs, **ACROSS)
    loss[:] = -jnp.sum(parts, **DOWN) * inv_count
    grad_logits = (jnp.exp(log_probs) - target) * inv_count
    low = grad_logits.astype(BF16)
    g_w_head[:] = dot(low, pooled, 0, 0)
    g_b_head[:] = jnp.sum(grad_logits, axis=0)
    grad = dot(low, w_head[:]).astype(BF16).astype(F32)
    grad_in, by_unit = norm_backward(grad, tops[:], wide_gain)
    g_gain[:] = jnp.sum(by_unit, axis=0)
    g_bias[:] = jnp.sum(grad, axis=0)
    gtop[:] = jnp.zeros_like(gtop)
    for image in range(images):
        gtop[image, 0:1, :] = grad_in[image:image + 1].astype(BF16)


def run_head(inv_count, tops, labels, gain, bias, w_head, b_head):
    images, width = tops.shape
    classes = w_head.shape[0]
    shape = lambda *dims, dtype=F32: jax.ShapeDtypeStruct(dims, dtype)
    return pl.pallas_call(
        functools.partial(head_kernel, inv_count),
        out_shape=(shape(1, 1), shape(images, 16, width, dtype=BF16), shape(width), shape(width), shape(classes, width), shape(classes)),
        in_specs=[VMEM, pl.BlockSpec(memory_space=pltpu.SMEM)] + [VMEM] * 4,
        out_specs=(VMEM,) * 6,
        compiler_params=pltpu.CompilerParams(vmem_limit_bytes=LIMIT),
        name="head",
    )(tops, labels, gain, bias, w_head, b_head)


def weight_kernel(*refs):
    count = (len(refs) - 15 - 11) // 2
    fc2_l, qkv_l, proj_l, patch_l, fc2_r, qkv_r, proj_r, patch_r, fc1_l, fc1_r = refs[:10]
    sums = refs[10:10 + count]
    fc2_o, qkv_o, proj_o, patch_o, fc1_o = refs[10 + count:15 + count]
    sums_out = refs[15 + count:15 + 2 * count]
    lhs, rhs, out, turned, block, wide, lsem, rsem, osem, bsem, wsem = refs[15 + 2 * count:]
    width = rhs.shape[2]
    size, wide_size = lhs.shape[2], block.shape[2]
    tail = width % size
    patches = patch_l.shape[1] // size + 1
    ends = [fc2_l.shape[1] // size]
    ends.append(ends[0] + qkv_l.shape[1] // size)
    ends.append(ends[1] + width // size + 1)
    ends.append(ends[2] + patches)
    starts = [0] + ends[:3]
    steps = ends[3]
    wide_steps = fc1_r.shape[1] // wide_size

    def lines(at, unit):
        return pl.ds(pl.multiple_of(at * unit, LANES), unit)

    def left_copy(step, act):
        slot = flip(step)
        for product, source in enumerate((fc2_l, qkv_l, proj_l, patch_l)):
            full = source.shape[1] // size
            first = starts[product]

            @pl.when(jnp.logical_and(step >= first, step < first + full))
            def _():
                act(pltpu.make_async_copy(source.at[:, lines(step - first, size)], lhs.at[slot], lsem.at[slot]))

            if source.shape[1] % size:
                @pl.when(step == first + full)
                def _():
                    act(pltpu.make_async_copy(source.at[:, pl.ds(full * size, tail)], lhs.at[slot, :, pl.ds(0, tail)], lsem.at[slot]))

    def out_copy(step, act):
        slot = flip(step)
        for product, target in enumerate((fc2_o, qkv_o, proj_o)):
            full = target.shape[0] // size
            first = starts[product]

            @pl.when(jnp.logical_and(step >= first, step < first + full))
            def _():
                act(pltpu.make_async_copy(out.at[slot], target.at[lines(step - first, size)], osem.at[slot]))

            if target.shape[0] % size:
                @pl.when(step == first + full)
                def _():
                    act(pltpu.make_async_copy(out.at[slot, pl.ds(0, tail)], target.at[pl.ds(full * size, tail)], osem.at[slot]))

    def right_copy(product):
        source = (fc2_r, qkv_r, proj_r, patch_r, fc1_l)[product]
        return pltpu.make_async_copy(source, rhs.at[product % 2], rsem.at[product % 2])

    def block_copy(step):
        slot = flip(step)
        return pltpu.make_async_copy(fc1_r.at[:, lines(step, wide_size)], block.at[slot], bsem.at[slot])

    def wide_copy(step):
        slot = flip(step)
        return pltpu.make_async_copy(wide.at[slot], fc1_o.at[:, lines(step, wide_size)], wsem.at[slot])

    start = lambda copy: copy.start()
    wait = lambda copy: copy.wait()
    left_copy(0, start)
    right_copy(0).start()
    right_copy(1).start()
    for given, passed in zip(sums, sums_out):
        passed[:] = given[:]

    def one_step(step, carry):
        slot = flip(step)

        @pl.when(step >= 1)
        def _():
            out_copy(step - 1, start)

        @pl.when(step >= 2)
        def _():
            out_copy(step - 2, wait)

        @pl.when(step + 1 < steps)
        def _():
            left_copy(step + 1, start)

        for product, first in enumerate(starts):
            @pl.when(step == first)
            def _(product=product):
                right_copy(product).wait()
                if product >= 1:
                    right_copy(product + 1).start()

        @pl.when(step == steps - 1)
        def _():
            block_copy(0).start()

        left_copy(step, wait)
        which = lax.rem(sum((step >= end).astype(jnp.int32) for end in ends[:3]), 2)
        out[slot] = dot(lhs[slot], rhs[which], 0, 0)
        for at in range(patches):
            count = min(size, patch_o.shape[0] - at * size)

            @pl.when(step == starts[3] + at)
            def _():
                patch_o[at * size:at * size + count, :] = out[slot, :count, :]

        return carry

    lax.fori_loop(0, steps, one_step, 0)
    right_copy(4).wait()
    turned[:] = rhs[0].T

    def wide_step(step, carry):
        slot = flip(step)

        @pl.when(step >= 1)
        def _():
            wide_copy(step - 1).start()

        @pl.when(step >= 2)
        def _():
            wide_copy(step - 2).wait()

        @pl.when(step + 1 < wide_steps)
        def _():
            block_copy(step + 1).start()

        block_copy(step).wait()
        wide[slot] = dot(turned[:], block[slot])
        return carry

    lax.fori_loop(0, wide_steps, wide_step, 0)
    wide_copy(wide_steps - 1).start()
    wide_copy(wide_steps - 2).wait()
    wide_copy(wide_steps - 1).wait()


def run_weights(lefts, rights, patch_size, sums):
    fc2_l, qkv_l, proj_l, patch_l, fc1_l = lefts
    fc2_r, qkv_r, proj_r, patch_r, fc1_r = rights
    rows, width = fc2_r.shape
    size, wide_size = 3 * LANES, 4 * LANES
    shapes = [(left.shape[1], right.shape[1]) for left, right in zip(lefts, rights)]
    shapes[3] = (patch_size, width)
    flops = sum(2 * rows * a * b for a, b in shapes)
    return pl.pallas_call(
        weight_kernel,
        out_shape=tuple(jax.ShapeDtypeStruct(shape, F32) for shape in shapes) + tuple(jax.ShapeDtypeStruct(total.shape, F32) for total in sums),
        in_specs=[ANY] * 10 + [VMEM] * len(sums),
        out_specs=(ANY,) * 3 + (VMEM, ANY) + (VMEM,) * len(sums),
        scratch_shapes=[
            pltpu.VMEM((2, rows, size), BF16), pltpu.VMEM((2, rows, width), BF16), pltpu.VMEM((2, size, width), F32),
            pltpu.VMEM((width, rows), BF16), pltpu.VMEM((2, rows, wide_size), BF16), pltpu.VMEM((2, width, wide_size), F32),
            PAIR, PAIR, PAIR, PAIR, PAIR],
        compiler_params=pltpu.CompilerParams(vmem_limit_bytes=LIMIT),
        cost_estimate=pl.CostEstimate(flops=flops, bytes_accessed=4 * sum(a * b for a, b in shapes), transcendentals=0),
        name="weights",
    )(fc2_l, qkv_l, proj_l, patch_l, fc2_r, qkv_r, proj_r, patch_r, fc1_l, fc1_r, *sums)


def matmul_rows(spec, left, right):
    return jnp.einsum(spec, left, right, preferred_element_type=F32)


def solution(mesh):
    stages = mesh.shape["pp"]
    in_specs = (P("dp"), P("dp"), P(), P(), P(), P()) + (P("pp"),) * 12 + (P(),) * 4
    out_specs = (P("dp"),) * 5 + (P(("dp", "pp")),) * 12 + (P("dp"),) * 4

    def body(patches, labels, w_patch, b_patch, cls_token, pos_embed, *rest):
        ln1_gain, ln1_bias, w_qkv, b_qkv, w_proj, b_proj, ln2_gain, ln2_bias, w_fc1, b_fc1, w_fc2, b_fc2 = (tensor[0] for tensor in rest[:12])
        lnf_gain, lnf_bias, w_head, b_head = rest[12:]
        tokens, width = pos_embed.shape
        heads, head = w_qkv.shape[2:]
        images = labels.size
        inv_count = 1.0 / images
        rows = -(-tokens // 16) * 16
        dims = (stages, images, tokens, heads, head)

        patch_size = patches.shape[-1]
        spare = -patch_size % LANES
        patch_rows = jnp.pad(patches.reshape((images,) + patches.shape[2:]), ((0, 0), (1, rows - tokens), (0, spare)))
        w_embed = jnp.pad(w_patch, ((0, spare), (0, 0)))
        is_patch = lax.broadcasted_iota(jnp.int32, (rows, 1), 0) > 0
        base = jnp.pad(pos_embed, ((0, rows - tokens), (0, 0))).astype(F32) + jnp.where(is_patch, b_patch.astype(F32), cls_token.astype(F32))
        embedded = (matmul_rows("inp,pd->ind", patch_rows, w_embed) + base).astype(BF16)

        line = lambda tensor: tensor.reshape(1, -1)
        wqkv_t = jnp.transpose(w_qkv, (1, 2, 3, 0)).reshape(3 * width, width)
        big = (wqkv_t, w_proj.reshape(width, width), w_fc1, w_fc2)
        vectors = tuple(map(line, (ln1_gain, ln1_bias, b_qkv, b_proj, ln2_gain, ln2_bias, b_fc1, b_fc2)))
        vectors = vectors[:2] + (vectors[2].reshape(3, 1, width),) + vectors[3:]
        x_s, a_s, qkv_s, c_s, h_s, n_s, d_s, g_s, p_s, tops = run_forward(dims, embedded, *big, vectors)

        loss, gtop, g_lnf_gain, g_lnf_bias, g_w_head, g_b_head = run_head(
            inv_count, tops, jnp.transpose(labels), lnf_gain, lnf_bias, jnp.transpose(w_head), b_head)

        gy_s, gpre_s, gmid_s, gqkv_s, gemb, *sums = run_backward(dims, gtop, *big, vectors[0], vectors[4], x_s, qkv_s, h_s, d_s, p_s)
        flat = lambda array: array.reshape(images * rows, -1)
        g_w_fc2, g_w_qkv, g_w_proj, g_w_patch, g_w_fc1, *sums = run_weights(
            tuple(map(flat, (g_s, gqkv_s, c_s, patch_rows, n_s))), tuple(map(flat, (gy_s, a_s, gmid_s, gemb, gpre_s))), patch_size, sums)
        g_ln1_gain, g_ln1_bias, g_ln2_gain, g_ln2_bias, g_b_proj, g_b_fc2, g_b_qkv, g_b_fc1 = sums
        g_w_qkv = jnp.transpose(g_w_qkv.reshape(3, heads, head, width), (3, 0, 1, 2))[None]
        layer_grads = (
            g_ln1_gain, g_ln1_bias, g_w_qkv, g_b_qkv.reshape(1, 3, heads, head), g_w_proj.reshape(1, heads, head, width), g_b_proj,
            g_ln2_gain, g_ln2_bias, g_w_fc1[None], g_b_fc1, g_w_fc2[None], g_b_fc2,
        )
        g_pos_embed = jnp.sum(gemb[:, :tokens].astype(F32), axis=0)
        embed_grads = (
            g_w_patch, jnp.sum(g_pos_embed[1:], axis=0), g_pos_embed[0], g_pos_embed,
        )
        return (loss.reshape(1),) + embed_grads + layer_grads + (g_lnf_gain, g_lnf_bias, jnp.transpose(g_w_head), g_b_head)

    return jax.shard_map(body, mesh=mesh, in_specs=in_specs, out_specs=out_specs, check_vma=False)
```

```python
import functools
import math
import jax
import jax.numpy as jnp
from jax import lax
from jax.experimental import pallas as pl
from jax.experimental.pallas import tpu as pltpu
from jax.sharding import PartitionSpec as P

EPS = 1e-6
SMOOTH = 0.1
F32 = jnp.float32
BF16 = jnp.bfloat16
MESH = pl.DeviceIdType.MESH
LANES = 128
HALF = 384
CHUNK = 2 * HALF
GROUP = 4
BLOCK = 136
DOWN = {"axis": 0, "keepdims": True}
ACROSS = {"axis": -1, "keepdims": True}


def flip(index):
    return lax.rem(index, 2)


def third(index):
    return lax.rem(index, 3)


def layer_norm(hidden, gain, bias):
    values = hidden.astype(F32)
    centered = values - jnp.mean(values, **ACROSS)
    variance = jnp.mean(jnp.square(centered), **ACROSS)
    return (centered * lax.rsqrt(variance + EPS) * gain + bias).astype(BF16)


def dot(left, right, left_axis=1, right_axis=0):
    return lax.dot_general(left, right, (((left_axis,), (right_axis,)), ((), ())), preferred_element_type=F32)


def by_rows(rows, visit):
    def step(index, carry):
        visit(pl.ds(pl.multiple_of(index * BLOCK, BLOCK), BLOCK))
        return carry

    lax.fori_loop(0, rows // BLOCK, step, 0)
    if rows % BLOCK:
        visit(pl.ds(rows - rows % BLOCK, rows % BLOCK))


def fold(values):
    rows, columns = values.shape
    return jnp.sum(values.reshape(rows // 8, 8, columns), axis=0)


def everyone(stage, stages):
    barrier = pltpu.get_barrier_semaphore()
    for hop in range(1, stages):
        pl.semaphore_signal(barrier, device_id={"pp": lax.rem(stage + hop, stages)}, device_id_type=MESH)
    pl.semaphore_wait(barrier, stages - 1)


def weight_copies(wproj, wfc1, wfc2, vproj, vfc1, vfc2, sems):
    def of_chunk(source, target, which, by_lines):
        def copy(chunk):
            span = pl.ds(pl.multiple_of(chunk * CHUNK, CHUNK), CHUNK)
            part = span if by_lines else (slice(None), span)
            return pltpu.make_async_copy(source.at[part], target.at[part], sems.at[which, chunk])
        return copy

    proj = pltpu.make_async_copy(wproj, vproj, sems.at[0, 0])
    return proj, of_chunk(wfc1, vfc1, 1, False), of_chunk(wfc2, vfc2, 2, True)


def forward_kernel(dims, *refs):
    (emb, wqkv, wproj, wfc1, wfc2, *given,
     x_s, a_s, qkv_s, c_s, h_s, n_s, d_s, g_s, p_s, tops_out,
     vqkv, vproj, vfc1, vfc2, xin, act, qkv, mid, yacc, ubuf, gbuf, tops,
     g1, b1, bqkv, bproj, g2, b2, bfc2,
     wsem, qsem, recv_sem, send_sem, top_sem, save_sem, usem, gsem, psem, free_sem) = refs
    stages, images, tokens, heads, head = dims
    rows, width = mid.shape
    chunks = vfc1.shape[1] // CHUNK
    stage = lax.axis_index("pp")
    is_first = stage == 0
    is_last = stage == stages - 1
    scale2 = head ** -0.5 / math.log(2.0)


    def qkv_copy(part):
        lines = pl.ds(pl.multiple_of(part * width, LANES), width)
        return pltpu.make_async_copy(wqkv.at[lines], vqkv.at[lines], qsem.at[part])

    def emb_copy(image, slot):
        return pltpu.make_async_copy(emb.at[image], xin.at[slot], recv_sem.at[slot])

    @pl.when(is_first)
    def _():
        emb_copy(0, 0).start()
        emb_copy(1, 1).start()

    proj_copy, fc1_copy, fc2_copy = weight_copies(wproj, wfc1, wfc2, vproj, vfc1, vfc2, wsem)
    for part in range(3):
        qkv_copy(part).start()
    proj_copy.start()
    for chunk in range(chunks):
        fc1_copy(chunk).start()
        fc2_copy(chunk).start()
    qkv[:] = jnp.zeros_like(qkv)
    *lows, bfc1, low = given
    for low, wide in zip((*lows, low), (g1, b1, bqkv, bproj, g2, b2, bfc2)):
        wide[:] = low[:].astype(F32)
    everyone(stage, stages)

    def saves(image, slot):
        pairs = ((xin.at[slot], x_s), (act, a_s), (qkv, qkv_s), (act, c_s), (mid, h_s), (act, n_s))
        return [pltpu.make_async_copy(src, dst.at[image], save_sem.at[at]) for at, (src, dst) in enumerate(pairs)]

    class u_save:
        def __init__(self, image, chunk):
            slot = third(chunk)
            self.copies = [
                pltpu.make_async_copy(ubuf.at[slot, :, pl.ds(side * HALF, HALF)], d_s.at[image, chunk * 2 + side], usem.at[slot, side])
                for side in range(2)]

        def start(self):
            for copy in self.copies:
                copy.start()

        def wait(self):
            for copy in self.copies:
                copy.wait()

    def g_save(image, chunk):
        slot = flip(chunk)
        return pltpu.make_async_copy(gbuf.at[slot], g_s.at[image, :, pl.ds(pl.multiple_of(chunk * CHUNK, CHUNK), CHUNK)], gsem.at[slot])

    def p_slot(number):
        slot = number % 9
        if slot < 6:
            return ubuf.at[slot // 2, :, pl.ds(slot % 2 * HALF, HALF)]
        return yacc.at[:, pl.ds((slot - 6) * HALF, HALF)]

    def p_save(image, number):
        return pltpu.make_async_copy(p_slot(number), p_s.at[image, number], psem.at[number % 9])

    def top_copy(image, other):
        return pltpu.make_async_remote_copy(
            src_ref=mid.at[pl.ds(0, 8)], dst_ref=tops.at[image], send_sem=send_sem.at[1 + other], recv_sem=top_sem,
            device_id={"pp": other}, device_id_type=MESH)

    def next_copy(image, slot):
        return pltpu.make_async_remote_copy(
            src_ref=mid, dst_ref=xin.at[slot], send_sem=send_sem.at[0], recv_sem=recv_sem.at[slot],
            device_id={"pp": lax.rem(stage + 1, stages)}, device_id_type=MESH)

    def wait_sent(image):
        @pl.when(jnp.logical_not(is_last))
        def _():
            next_copy(image, 0).wait_send()

        @pl.when(is_last)
        def _():
            for other in range(stages - 1):
                top_copy(image, other).wait_send()

    def one_image(image, carry):
        slot = flip(image)
        save_x, save_a, save_qkv, save_c, save_h, save_n = saves(image, slot)
        emb_copy(image, slot).wait()
        save_x.start()

        @pl.when(image > 0)
        def _():
            save_n.wait()
            save_qkv.wait()

        def norm1(lines):
            act[lines, :] = layer_norm(xin[slot, lines, :], g1[:], b1[:])

        by_rows(rows, norm1)
        save_a.start()

        @pl.when(image == 0)
        def _():
            for part in range(3):
                qkv_copy(part).wait()

        low = (dot(act[:], vqkv[:], 1, 1) + bqkv[:]).astype(BF16)
        for at in range(3 * heads):
            qkv[:, at * LANES:at * LANES + head] = low[:, at * head:(at + 1) * head]
        save_qkv.start()

        save_a.wait()

        @pl.when(image > 0)
        def _():
            for chunk in range(3):
                u_save(image, chunk).wait()

        def scores_of(number):
            q, k = (qkv[:, lane:lane + LANES] for lane in (number * LANES, (heads + number) * LANES))
            return dot(k, q, 1, 1)

        def attend(number, scores):
            if number == 9:
                for slot in range(6):
                    p_save(image, slot).wait()
            if number > 14:
                p_save(image, number - 9).wait()
            v = qkv[:, (2 * heads + number) * LANES:(2 * heads + number + 1) * LANES]
            top, tail = scores[:tokens - 1], scores[tokens - 1:]
            most = jnp.maximum(jnp.max(top, **DOWN), tail[:1])
            top = jnp.exp2((top - most) * scale2)
            real = lax.broadcasted_iota(jnp.int32, tail.shape, 0) < 1
            tail = jnp.where(real, jnp.exp2(jnp.minimum(tail - most, 0.0) * scale2), 0.0)
            inv = 1.0 / (jnp.sum(top, **DOWN) + jnp.sum(tail, **DOWN))
            probs = jnp.concatenate([top, tail], axis=0) * inv
            p_slot(number)[:, :rows] = probs
            act[:, number * head:(number + 1) * head] = dot(probs.astype(BF16), v, 0, 0).astype(BF16)[:, :head]
            p_save(image, number).start()

        scores = scores_of(0)
        for number in range(heads):
            later = scores_of(number + 1) if number + 1 < heads else None
            attend(number, scores)
            scores = later
        save_c.start()

        @pl.when(image == 0)
        def _():
            proj_copy.wait()

        @pl.when(image > 0)
        def _():
            wait_sent(image)

        mid[:] = (dot(act[:], vproj[:]) + bproj[:] + xin[slot].astype(F32)).astype(BF16)
        save_h.start()
        save_x.wait()

        @pl.when(jnp.logical_and(is_first, image + 2 < images))
        def _():
            emb_copy(image + 2, slot).start()

        @pl.when(jnp.logical_and(stage > 0, image + 2 < images))
        def _():
            pl.semaphore_signal(free_sem, device_id={"pp": lax.rem(stage + stages - 1, stages)}, device_id_type=MESH)

        save_c.wait()
        for number in (7, 8, 15):
            p_save(image, number).wait()

        def norm2(lines):
            hidden = mid[lines, :]
            act[lines, :] = layer_norm(hidden, g2[:], b2[:])
            yacc[lines, :] = hidden.astype(F32) + bfc2[:]

        by_rows(rows, norm2)
        save_n.start()

        @pl.when(image == 0)
        def _():
            fc1_copy(0).wait()

        for number in range(9, 15):
            p_save(image, number).wait()

        @pl.when(image > 0)
        def _():
            for chunk in range(2):
                g_save(image, chunk).wait()

        def fc1(chunk):
            columns = pl.ds(pl.multiple_of(chunk * CHUNK, CHUNK), CHUNK)
            ubuf[third(chunk)] = dot(act[:], vfc1[:, columns]) + bfc1[:, columns].astype(F32)

        def gelu(chunk):
            slot3, slot2 = third(chunk), flip(chunk)
            pre = ubuf[slot3]
            cdf = 0.5 + 0.5 * lax.erf(pre * (0.5 ** 0.5))
            pdf = jnp.exp2(pre * pre * (-0.5 / math.log(2.0))) * ((2.0 * math.pi) ** -0.5)
            activ = (pre * cdf).astype(BF16)
            gbuf[slot2] = activ
            ubuf[slot3] = cdf + pre * pdf
            return activ

        def fc2(chunk, activ):
            yacc[:] += dot(activ, vfc2[pl.ds(pl.multiple_of(chunk * CHUNK, CHUNK), CHUNK), :])

        fc1(0)

        def mlp_step(chunk, carry):
            @pl.when(chunk >= 3)
            def _():
                u_save(image, chunk).wait()
                g_save(image, chunk - 1).wait()

            @pl.when(image == 0)
            def _():
                fc1_copy(chunk).wait()
                fc2_copy(chunk - 1).wait()

            @pl.when(chunk >= 2)
            def _():
                u_save(image, chunk - 2).start()
                g_save(image, chunk - 2).start()

            activ = gelu(chunk - 1)
            fc1(chunk)
            fc2(chunk - 1, activ)
            return carry

        lax.fori_loop(1, chunks, mlp_step, 0)

        @pl.when(image == 0)
        def _():
            fc2_copy(chunks - 1).wait()

        g_save(image, chunks - 1).wait()
        u_save(image, chunks - 2).start()
        g_save(image, chunks - 2).start()
        fc2(chunks - 1, gelu(chunks - 1))
        u_save(image, chunks - 1).start()
        g_save(image, chunks - 1).start()

        save_h.wait()
        mid[:] = yacc[:].astype(BF16)

        @pl.when(jnp.logical_and(jnp.logical_not(is_last), image >= 2))
        def _():
            pl.semaphore_wait(free_sem, 1)

        @pl.when(jnp.logical_not(is_last))
        def _():
            next_copy(image, slot).start()

        @pl.when(is_last)
        def _():
            for other in range(stages - 1):
                top_copy(image, other).start()
            tops[image] = mid[pl.ds(0, 8), :]

        return carry

    lax.fori_loop(0, images, one_image, 0)
    wait_sent(images - 1)
    _, _, save_qkv, _, _, save_n = saves(images - 1, 0)
    save_qkv.wait()
    save_n.wait()
    for chunk in range(3):
        u_save(images - 1, chunk).wait()
    for chunk in range(2):
        g_save(images - 1, chunk).wait()

    @pl.when(jnp.logical_not(is_last))
    def _():
        pltpu.make_async_copy(tops, tops, top_sem).wait()

    for image in range(images):
        tops_out[image:image + 1, :] = tops[image, 0:1, :]


def norm_backward(grad, hidden, gain):
    values = hidden.astype(F32)
    centered = values - jnp.mean(values, **ACROSS)
    inv = lax.rsqrt(jnp.mean(jnp.square(centered), **ACROSS) + EPS)
    unit = centered * inv
    scaled = grad * gain
    grad_in = inv * (scaled - jnp.mean(scaled, **ACROSS) - unit * jnp.mean(scaled * unit, **ACROSS))
    return grad_in, grad * unit


def backward_kernel(dims, *refs):
    (gtop, wqkv, wproj, wfc1, wfc2, low1, low2, x_s, qkv_s, h_s, d_s, p_s,
     gy_s, gpre_s, gmid_s, gqkv_s, gemb, *sums_out,
     vqkv, vproj, vfc1, vfc2, gin, acc, shared, abuf, gbuf, hid, gmid, gctx, qkv, gqkv, gout, g1, g2,
     sum1g, sum1b, sum2g, sum2b, sumproj, sumfc2, sumqkv, sumfc1,
     wsem, qsem, recv_sem, top_sem, send_sem, emb_sem, relay_sem, save_sem, load_sem, dsem, gsem, psem, free_sem) = refs
    stages, images, tokens, heads, head = dims
    rows, width = gmid.shape
    chunks = vfc1.shape[1] // CHUNK
    stage = lax.axis_index("pp")
    is_first = stage == 0
    is_last = stage == stages - 1
    scale = head ** -0.5

    pieces = ((0, vqkv.shape[1]), (vqkv.shape[1], width - vqkv.shape[1]))

    def qkv_copy(part, side):
        slot = third(part * 2 + side)
        at, size = pieces[side]
        lines = pl.ds(pl.multiple_of(third(part) * width + at, 128), size)
        return pltpu.make_async_copy(wqkv.at[lines], vqkv.at[slot, pl.ds(0, size)], qsem.at[slot])

    def top_copy(image, slot):
        return pltpu.make_async_copy(gtop.at[image], gin.at[slot, pl.ds(0, 16)], top_sem.at[slot])

    def d_load(image, chunk):
        slot = lax.rem(chunk, 4)
        return pltpu.make_async_copy(d_s.at[image, pl.ds(chunk * 2, 2)], shared.at[pl.ds(slot * 2, 2)], dsem.at[slot])

    def g_save(image, chunk):
        slot = flip(chunk)
        return pltpu.make_async_copy(gbuf.at[slot], gpre_s.at[image, :, pl.ds(pl.multiple_of(chunk * CHUNK, CHUNK), CHUNK)], gsem.at[slot])

    held = shared.shape[0] + 3

    def p_slot(number):
        slot = number % held
        if slot < shared.shape[0]:
            return shared.at[slot]
        return acc.at[:, pl.ds((slot - shared.shape[0]) * HALF, HALF)]

    def p_load(image, number):
        return pltpu.make_async_copy(p_s.at[image, number], p_slot(number), psem.at[number % held])

    def saves(image, slot):
        pairs = ((gin.at[slot], gy_s), (gmid, gmid_s), (gqkv, gqkv_s))
        return [pltpu.make_async_copy(src, dst.at[image], save_sem.at[at]) for at, (src, dst) in enumerate(pairs)]

    def loads(image):
        pairs = ((h_s, hid), (x_s, hid), (qkv_s, qkv))
        return [pltpu.make_async_copy(src.at[image], dst, load_sem.at[at]) for at, (src, dst) in enumerate(pairs)]

    def next_copy(slot):
        return pltpu.make_async_remote_copy(
            src_ref=gout, dst_ref=gin.at[slot], send_sem=send_sem.at[0], recv_sem=recv_sem.at[slot],
            device_id={"pp": lax.rem(stage + stages - 1, stages)}, device_id_type=MESH)

    def emb_send(image, other):
        return pltpu.make_async_remote_copy(
            src_ref=gout, dst_ref=gemb.at[image], send_sem=send_sem.at[other], recv_sem=emb_sem.at[image],
            device_id={"pp": other}, device_id_type=MESH)

    def emb_relay(image):
        return pltpu.make_async_remote_copy(
            src_ref=gemb.at[image], dst_ref=gemb.at[image], send_sem=relay_sem.at[image], recv_sem=emb_sem.at[image],
            device_id={"pp": stages - 1}, device_id_type=MESH)

    def emb_local(image):
        return pltpu.make_async_copy(gout, gemb.at[image], save_sem.at[3])

    def wait_sent(image):
        @pl.when(jnp.logical_not(is_first))
        def _():
            next_copy(0).wait_send()

        @pl.when(is_first)
        def _():
            for other in range(1, stages - 1):
                emb_send(image, other).wait_send()
            emb_local(image).wait()

    @pl.when(is_last)
    def _():
        gin[:] = jnp.zeros_like(gin)
        top_copy(0, 0).start()
        top_copy(1, 1).start()

    proj_copy, fc1_copy, fc2_copy = weight_copies(wproj, wfc1, wfc2, vproj, vfc1, vfc2, wsem)
    for chunk in range(chunks):
        fc2_copy(chunk).start()
        if chunk < 4:
            d_load(0, chunk).start()
        fc1_copy(chunk).start()
    loads(0)[0].start()
    proj_copy.start()
    for part, side in ((0, 0), (0, 1), (1, 0)):
        qkv_copy(part, side).start()
    gctx[:] = jnp.zeros_like(gctx)
    sums_out, totals = sums_out[:8], (sum1g, sum1b, sum2g, sum2b, sumproj, sumfc2, sumqkv, sumfc1)
    for total in totals:
        total[:] = jnp.zeros_like(total)
    g1[:] = low1[:].astype(F32)
    g2[:] = low2[:].astype(F32)
    everyone(stage, stages)

    def one_image(image, carry):
        slot = flip(image)
        more = image + 1 < images
        save_gy, save_mid, save_qkv = saves(image, slot)
        load_h, load_x, load_qkv = loads(image)

        @pl.when(is_last)
        def _():
            top_copy(image, slot).wait()

        @pl.when(jnp.logical_not(is_last))
        def _():
            next_copy(slot).wait_recv()

        save_gy.start()

        load_qkv.start()

        @pl.when(image == 0)
        def _():
            fc2_copy(0).wait()

        @pl.when(image > 0)
        def _():
            for chunk in range(2):
                g_save(image, chunk).wait()

        acc[:] = jnp.zeros_like(acc)

        def fc2(chunk):
            lines = pl.ds(pl.multiple_of(chunk * CHUNK, CHUNK), CHUNK)
            abuf[flip(chunk)] = dot(gin[slot], vfc2[lines, :], 1, 1).astype(BF16)

        def gelu(chunk):
            columns = pl.ds(pl.multiple_of(chunk * CHUNK, CHUNK), CHUNK)
            slot2 = flip(chunk)
            slot4 = lax.rem(chunk, 4)
            pre = abuf[slot2].astype(F32) * jnp.concatenate([shared[slot4 * 2], shared[slot4 * 2 + 1]], axis=1)
            sumfc1[:, columns] += fold(pre)
            low = pre.astype(BF16)
            gbuf[slot2] = low
            return low

        def fc1(chunk, low):
            columns = pl.ds(pl.multiple_of(chunk * CHUNK, CHUNK), CHUNK)
            acc[:] += dot(low, vfc1[:, columns], 1, 1)

        fc2(0)

        def mlp_step(chunk, carry):
            d_load(image, chunk - 1).wait()

            @pl.when(image == 0)
            def _():
                fc2_copy(chunk).wait()
                fc1_copy(chunk - 1).wait()

            @pl.when(chunk >= 3)
            def _():
                g_save(image, chunk - 1).wait()

            @pl.when(chunk >= 2)
            def _():
                g_save(image, chunk - 2).start()

                @pl.when(chunk + 2 < chunks)
                def _():
                    d_load(image, chunk + 2).start()

            low = gelu(chunk - 1)
            fc2(chunk)
            fc1(chunk - 1, low)
            return carry

        lax.fori_loop(1, chunks, mlp_step, 0)
        d_load(image, chunks - 1).wait()

        @pl.when(image == 0)
        def _():
            fc1_copy(chunks - 1).wait()

        g_save(image, chunks - 1).wait()
        g_save(image, chunks - 2).start()
        fc1(chunks - 1, gelu(chunks - 1))
        g_save(image, chunks - 1).start()

        for number in range(shared.shape[0]):
            p_load(image, number).start()
        load_h.wait()

        @pl.when(image > 0)
        def _():
            save_mid.wait()
            save_qkv.wait()

        def back2(lines):
            grad = acc[lines, :].astype(BF16).astype(F32)
            grad_in, by_unit = norm_backward(grad, hid[lines, :], g2[:])
            sum2g[:] += fold(by_unit)
            sum2b[:] += fold(grad)
            top = gin[slot, lines, :].astype(F32)
            sumfc2[:] += fold(top)
            low = (top + grad_in).astype(BF16)
            gmid[lines, :] = low
            sumproj[:] += fold(low.astype(F32))

        by_rows(rows, back2)
        for number in range(shared.shape[0], held):
            p_load(image, number).start()
        save_mid.start()
        load_x.start()
        save_gy.wait()

        @pl.when(jnp.logical_and(is_last, image + 2 < images))
        def _():
            top_copy(image + 2, slot).start()

        @pl.when(jnp.logical_and(stage < stages - 1, image + 2 < images))
        def _():
            pl.semaphore_signal(free_sem, device_id={"pp": lax.rem(stage + 1, stages)}, device_id_type=MESH)

        @pl.when(image == 0)
        def _():
            proj_copy.wait()

        low = dot(gmid[:], vproj[:], 1, 1).astype(BF16)
        for number in range(heads):
            gctx[:, number * LANES:number * LANES + head] = low[:, number * head:(number + 1) * head]
        load_qkv.wait()
        for number in range(held):
            p_load(image, number).wait()
        def lanes_of(number):
            return slice(number * LANES, (number + 1) * LANES)

        def grad_probs_of(number):
            return dot(qkv[:, lanes_of(2 * heads + number)], gctx[:, lanes_of(number)], 1, 1)

        def attend(number, grad_probs):
            if number == held:
                for later in range(held, heads):
                    p_load(image, later).wait()
            probs = p_slot(number)[:, :rows]
            at = number * head
            mean = jnp.sum(grad_probs * probs, **DOWN)
            low = (probs * (grad_probs - mean) * scale).astype(BF16)
            value = dot(probs.astype(BF16), gctx[:, lanes_of(number)]).astype(BF16)
            gqkv[:, 2 * width + at:2 * width + at + head] = value[:, :head]
            key = dot(low, qkv[:, lanes_of(number)]).astype(BF16)
            gqkv[:, width + at:width + at + head] = key[:, :head]
            query = dot(low, qkv[:, lanes_of(heads + number)], 0, 0).astype(BF16)
            gqkv[:, at:at + head] = query[:, :head]

        grad_probs = grad_probs_of(0)
        for number in range(heads):
            later = grad_probs_of(number + 1) if number + 1 < heads else None
            attend(number, grad_probs)
            grad_probs = later
            if number + held < heads:
                p_load(image, number + held).start()
        save_qkv.start()

        def qkv_part(part, carry):
            for side in range(2):
                at, size = pieces[side]
                index = image * 3 + part
                qkv_copy(index, side).wait()
                columns = pl.ds(pl.multiple_of(part * width + at, 128), size)
                piece = gqkv[:, columns]
                sumqkv[:, columns] += fold(piece.astype(F32))
                acc[:] += dot(piece, vqkv[third(index * 2 + side), :size])

                @pl.when(index + 1 + side < images * 3)
                def _():
                    qkv_copy(index + 1 + side, 1 - side).start()

            return carry

        acc[:] = jnp.zeros_like(acc)
        lax.fori_loop(0, 3, qkv_part, 0)

        @pl.when(more)
        def _():
            for chunk in range(4):
                d_load(image + 1, chunk).start()

        load_x.wait()

        @pl.when(image > 0)
        def _():
            wait_sent(image)

        def back1(lines):
            grad = acc[lines, :].astype(BF16).astype(F32)
            grad_in, by_unit = norm_backward(grad, hid[lines, :], g1[:])
            sum1g[:] += fold(by_unit)
            sum1b[:] += fold(grad)
            gout[lines, :] = (gmid[lines, :].astype(F32) + grad_in).astype(BF16)

        by_rows(rows, back1)

        @pl.when(more)
        def _():
            loads(image + 1)[0].start()

        @pl.when(jnp.logical_and(jnp.logical_not(is_first), image >= 2))
        def _():
            pl.semaphore_wait(free_sem, 1)

        @pl.when(jnp.logical_not(is_first))
        def _():
            next_copy(slot).start()

        @pl.when(is_first)
        def _():
            for other in range(1, stages - 1):
                emb_send(image, other).start()
            emb_local(image).start()

        return carry

    lax.fori_loop(0, images, one_image, 0)
    wait_sent(images - 1)
    _, save_mid, save_qkv = saves(images - 1, 0)
    save_mid.wait()
    save_qkv.wait()
    for chunk in range(2):
        g_save(images - 1, chunk).wait()

    for out, total in zip(sums_out, totals):
        out[:] = jnp.sum(total[:], **DOWN)

    @pl.when(jnp.logical_not(is_first))
    def _():
        for image in range(images):
            emb_relay(image).wait_recv()

            @pl.when(stage == stages - 2)
            def _():
                emb_relay(image).start()

    @pl.when(stage == stages - 2)
    def _():
        for image in range(images):
            emb_relay(image).wait_send()


ANY = pl.BlockSpec(memory_space=pl.ANY)
VMEM = pl.BlockSpec(memory_space=pltpu.VMEM)
LIMIT = 67_043_328
DMA = pltpu.SemaphoreType.DMA
PAIR = DMA((2,))
TRIPLE = DMA((3,))


def run_forward(dims, emb, wqkv, wproj, wfc1, wfc2, vectors):
    stages, images, tokens, heads, head = dims
    rows, width = emb.shape[1:]
    hidden = wfc1.shape[1]
    hbm = lambda *shape, dtype=BF16: jax.ShapeDtypeStruct((images, rows) + shape, dtype)
    return pl.pallas_call(
        functools.partial(forward_kernel, dims),
        out_shape=(
            hbm(width), hbm(width), hbm(3 * heads * LANES), hbm(width), hbm(width), hbm(width),
            jax.ShapeDtypeStruct((images, hidden // HALF, rows, HALF), F32), hbm(hidden),
            jax.ShapeDtypeStruct((images, heads, rows, HALF), F32), jax.ShapeDtypeStruct((images, width), BF16)),
        in_specs=[ANY] * 5 + [VMEM] * 8,
        out_specs=(ANY,) * 9 + (VMEM,),
        scratch_shapes=[
            pltpu.VMEM(wqkv.shape, BF16), pltpu.VMEM(wproj.shape, BF16), pltpu.VMEM(wfc1.shape, BF16), pltpu.VMEM(wfc2.shape, BF16),
            pltpu.VMEM((2, rows, width), BF16), pltpu.VMEM((rows, width), BF16), pltpu.VMEM((rows, 3 * heads * LANES), BF16),
            pltpu.VMEM((rows, width), BF16), pltpu.VMEM((rows, width), F32),
            pltpu.VMEM((3, rows, CHUNK), F32), pltpu.VMEM((2, rows, CHUNK), BF16),
            pltpu.VMEM((images, 8, width), BF16),
            *(pltpu.VMEM(vector.shape, F32) for vector in vectors[:6]), pltpu.VMEM(vectors[7].shape, F32),
            DMA((3, hidden // CHUNK)), TRIPLE, PAIR, DMA((stages,)), DMA(()), DMA((6,)), DMA((3, 2)), PAIR, DMA((9,)),
            pltpu.SemaphoreType.REGULAR],
        compiler_params=pltpu.CompilerParams(collective_id=0, has_side_effects=True, vmem_limit_bytes=LIMIT),
        name="forward",
    )(emb, wqkv, wproj, wfc1, wfc2, *vectors)


def run_backward(dims, gtop, wqkv, wproj, wfc1, wfc2, g1, g2, x_s, qkv_s, h_s, d_s, p_s):
    stages, images, tokens, heads, head = dims
    rows, width = x_s.shape[1:]
    hidden = wfc1.shape[1]
    hbm = lambda *shape: jax.ShapeDtypeStruct((images, rows) + shape, BF16)
    sizes = (width,) * 6 + (3 * width, hidden)
    return pl.pallas_call(
        functools.partial(backward_kernel, dims),
        out_shape=(hbm(width), hbm(hidden), hbm(width), hbm(3 * width), hbm(width)) + tuple(jax.ShapeDtypeStruct((1, size), F32) for size in sizes),
        in_specs=[ANY] * 5 + [VMEM] * 2 + [ANY] * 5,
        out_specs=(ANY,) * 5 + (VMEM,) * 8,
        scratch_shapes=[
            pltpu.VMEM((3, -(-width // 256) * LANES, width), BF16), pltpu.VMEM(wproj.shape, BF16), pltpu.VMEM(wfc1.shape, BF16), pltpu.VMEM(wfc2.shape, BF16),
            pltpu.VMEM((2, rows, width), BF16), pltpu.VMEM((rows, width), F32), pltpu.VMEM((2 * GROUP, rows, HALF), F32),
            pltpu.VMEM((2, rows, CHUNK), BF16), pltpu.VMEM((2, rows, CHUNK), BF16),
            pltpu.VMEM((rows, width), BF16), pltpu.VMEM((rows, width), BF16), pltpu.VMEM((rows, heads * LANES), BF16),
            pltpu.VMEM((rows, 3 * heads * LANES), BF16), pltpu.VMEM((rows, 3 * width), BF16),
            pltpu.VMEM((rows, width), BF16), pltpu.VMEM((1, width), F32), pltpu.VMEM((1, width), F32),
            *(pltpu.VMEM((8, size), F32) for size in sizes),
            DMA((3, hidden // CHUNK)), TRIPLE, PAIR, PAIR, DMA((stages,)), DMA((images,)), DMA((images,)), DMA((4,)), TRIPLE, DMA((4,)), PAIR, DMA((2 * GROUP + 3,)),
            pltpu.SemaphoreType.REGULAR],
        compiler_params=pltpu.CompilerParams(collective_id=1, has_side_effects=True, vmem_limit_bytes=LIMIT),
        name="backward",
    )(gtop, wqkv, wproj, wfc1, wfc2, g1, g2, x_s, qkv_s, h_s, d_s, p_s)


def head_kernel(inv_count, tops, labels, gain, bias, w_head, b_head, loss, gtop, g_gain, g_bias, low_out, pooled_out, g_b_head):
    images, width = tops.shape
    line = lambda ref: ref[:].reshape(1, -1).astype(F32)
    wide_gain = line(gain)
    pooled = layer_norm(tops[:], wide_gain, line(bias))
    logits = dot(pooled, w_head[:], 1, 1) + line(b_head)
    shifted = logits - jnp.max(logits, **ACROSS)
    log_probs = shifted - jnp.log(jnp.sum(jnp.exp(shifted), **ACROSS))
    classes = logits.shape[-1]
    number = lax.broadcasted_iota(jnp.int32, (images, 1), 0)
    label = jnp.zeros((images, 1), jnp.int32)
    for image in range(images):
        label = jnp.where(number == image, labels[image % labels.shape[0], image // labels.shape[0]], label)
    chosen = (lax.broadcasted_iota(jnp.int32, logits.shape, 1) == label).astype(F32)
    target = (1.0 - SMOOTH) * chosen + SMOOTH / classes
    parts = jnp.sum(target * log_probs, **ACROSS)
    loss[:] = -jnp.sum(parts, **DOWN) * inv_count
    grad_logits = (jnp.exp(log_probs) - target) * inv_count
    low = grad_logits.astype(BF16)
    low_out[:] = low
    pooled_out[:] = pooled
    g_b_head[:] = jnp.sum(grad_logits, axis=0)
    grad = dot(low, w_head[:]).astype(BF16).astype(F32)
    grad_in, by_unit = norm_backward(grad, tops[:], wide_gain)
    g_gain[:] = jnp.sum(by_unit, axis=0)
    g_bias[:] = jnp.sum(grad, axis=0)
    gtop[:] = jnp.zeros_like(gtop)
    for image in range(images):
        gtop[image, 0:1, :] = grad_in[image:image + 1].astype(BF16)


def run_head(inv_count, tops, labels, gain, bias, w_head, b_head):
    images, width = tops.shape
    classes = w_head.shape[0]
    shape = lambda *dims, dtype=F32: jax.ShapeDtypeStruct(dims, dtype)
    return pl.pallas_call(
        functools.partial(head_kernel, inv_count),
        out_shape=(shape(1, 1), shape(images, 16, width, dtype=BF16), shape(width), shape(width),
            shape(images, classes, dtype=BF16), shape(images, width, dtype=BF16), shape(classes)),
        in_specs=[VMEM, pl.BlockSpec(memory_space=pltpu.SMEM)] + [VMEM] * 4,
        out_specs=(VMEM,) * 7,
        compiler_params=pltpu.CompilerParams(vmem_limit_bytes=LIMIT),
        name="head",
    )(tops, labels, gain, bias, w_head, b_head)


def weight_kernel(rows, given, made, *refs):
    fc2_l, qkv_l, proj_l, patch_l, fc2_r, qkv_r, proj_r, patch_r, fc1_l, fc1_r, logit_l, logit_r, *sums = refs[:given]
    fc2_o, qkv_o, proj_o, fc1_o, head_o, patch_o, pos_o, bias_o, first_o, *sums_out = refs[given:given + made]
    lhs, rhs, out, turned, block, wide, logit, lsem, rsem, osem, bsem, wsem, hsem = refs[given + made:]
    width = rhs.shape[2]
    size, wide_size = lhs.shape[2], block.shape[2]
    tail = width % size
    patches = patch_l.shape[1] // size + 1
    ends = [fc2_l.shape[1] // size]
    ends.append(ends[0] + qkv_l.shape[1] // size)
    ends.append(ends[1] + width // size + 1)
    ends.append(ends[2] + patches)
    starts = [0] + ends[:3]
    steps = ends[3]
    wide_steps = fc1_r.shape[1] // wide_size

    def lines(at, unit):
        return pl.ds(pl.multiple_of(at * unit, LANES), unit)

    def left_copy(step, act):
        slot = flip(step)
        for product, source in enumerate((fc2_l, qkv_l, proj_l, patch_l)):
            full = source.shape[1] // size
            first = starts[product]

            @pl.when(jnp.logical_and(step >= first, step < first + full))
            def _():
                act(pltpu.make_async_copy(source.at[:, lines(step - first, size)], lhs.at[slot], lsem.at[slot]))

            if source.shape[1] % size:
                @pl.when(step == first + full)
                def _():
                    act(pltpu.make_async_copy(source.at[:, pl.ds(full * size, tail)], lhs.at[slot, :, pl.ds(0, tail)], lsem.at[slot]))

    def out_copy(step, act):
        slot = flip(step)
        for product, target in enumerate((fc2_o, qkv_o, proj_o)):
            full = target.shape[0] // size
            first = starts[product]

            @pl.when(jnp.logical_and(step >= first, step < first + full))
            def _():
                act(pltpu.make_async_copy(out.at[slot], target.at[lines(step - first, size)], osem.at[slot]))

            if target.shape[0] % size:
                @pl.when(step == first + full)
                def _():
                    act(pltpu.make_async_copy(out.at[slot, pl.ds(0, tail)], target.at[pl.ds(full * size, tail)], osem.at[slot]))

    def right_copy(product):
        source = (fc2_r, qkv_r, proj_r, patch_r, fc1_l)[product]
        return pltpu.make_async_copy(source, rhs.at[product % 2], rsem.at[product % 2])

    def block_copy(step):
        slot = flip(step)
        return pltpu.make_async_copy(fc1_r.at[:, lines(step, wide_size)], block.at[slot], bsem.at[slot])

    def wide_copy(step):
        slot = flip(step)
        return pltpu.make_async_copy(wide.at[slot], fc1_o.at[:, lines(step, wide_size)], wsem.at[slot])

    start = lambda copy: copy.start()
    wait = lambda copy: copy.wait()
    left_copy(0, start)
    right_copy(0).start()
    right_copy(1).start()
    for total, passed in zip(sums, sums_out):
        passed[:] = total[:]
    logit[:] = dot(logit_l[:], logit_r[:], 0, 0)
    head_copy = pltpu.make_async_copy(logit, head_o, hsem)
    head_copy.start()

    def embedding_sums(source):
        bias = jnp.zeros_like(bias_o)
        for at in range(0, rows, BLOCK):
            total = sum(source[image + at:image + at + BLOCK, :].astype(F32) for image in range(0, source.shape[0], rows))
            count = min(BLOCK, pos_o.shape[0] - at)
            pos_o[at:at + count, :] = total[:count]
            is_first = lax.broadcasted_iota(jnp.int32, total.shape, 0) + at < 1
            bias = bias + jnp.sum(jnp.where(is_first, 0.0, total), axis=0)
            if at == 0:
                first_o[:] = jnp.sum(jnp.where(is_first, total, 0.0), axis=0)
        bias_o[:] = bias

    def one_step(step, carry):
        slot = flip(step)

        @pl.when(step >= 1)
        def _():
            out_copy(step - 1, start)

        @pl.when(step >= 2)
        def _():
            out_copy(step - 2, wait)

        @pl.when(step + 1 < steps)
        def _():
            left_copy(step + 1, start)

        for product, first in enumerate(starts):
            @pl.when(step == first)
            def _(product=product):
                right_copy(product).wait()
                if product >= 1:
                    right_copy(product + 1).start()
                if product == 3:
                    embedding_sums(rhs.at[1])

        @pl.when(step == steps - 1)
        def _():
            block_copy(0).start()

        left_copy(step, wait)
        which = lax.rem(sum((step >= end).astype(jnp.int32) for end in ends[:3]), 2)
        out[slot] = dot(lhs[slot], rhs[which], 0, 0)
        for at in range(patches):
            count = min(size, patch_o.shape[0] - at * size)

            @pl.when(step == starts[3] + at)
            def _():
                patch_o[at * size:at * size + count, :] = out[slot, :count, :]

        return carry

    lax.fori_loop(0, steps, one_step, 0)
    right_copy(4).wait()
    turned[:] = rhs[0].T

    def wide_step(step, carry):
        slot = flip(step)

        @pl.when(step >= 1)
        def _():
            wide_copy(step - 1).start()

        @pl.when(step >= 2)
        def _():
            wide_copy(step - 2).wait()

        @pl.when(step + 1 < wide_steps)
        def _():
            block_copy(step + 1).start()

        block_copy(step).wait()
        wide[slot] = dot(turned[:], block[slot])
        return carry

    lax.fori_loop(0, wide_steps, wide_step, 0)
    wide_copy(wide_steps - 1).start()
    wide_copy(wide_steps - 2).wait()
    wide_copy(wide_steps - 1).wait()
    head_copy.wait()


def run_weights(lefts, rights, logit_parts, patch_size, tokens, images, sums):
    fc2_l, qkv_l, proj_l, patch_l, fc1_l = lefts
    fc2_r, qkv_r, proj_r, patch_r, fc1_r = rights
    rows, width = fc2_r.shape
    size, wide_size = 3 * LANES, 4 * LANES
    classes = logit_parts[0].shape[1]
    outs = [(left.shape[1], right.shape[1]) for left, right in zip(lefts, rights)]
    outs = outs[:3] + outs[4:]
    flops = sum(2 * rows * a * b for a, b in outs)
    stored = sum(4 * a * b for a, b in outs)
    outs += [(classes, width), (patch_size, width), (tokens, width), (width,), (width,)] + [total.shape for total in sums]
    inputs = (fc2_l, qkv_l, proj_l, patch_l, fc2_r, qkv_r, proj_r, patch_r, fc1_l, fc1_r, *logit_parts, *sums)
    return pl.pallas_call(
        functools.partial(weight_kernel, rows // images, len(inputs), len(outs)),
        out_shape=tuple(jax.ShapeDtypeStruct(shape, F32) for shape in outs),
        in_specs=[ANY] * 10 + [VMEM] * (2 + len(sums)),
        out_specs=(ANY,) * 5 + (VMEM,) * (len(outs) - 5),
        scratch_shapes=[
            pltpu.VMEM((2, rows, size), BF16), pltpu.VMEM((2, rows, width), BF16), pltpu.VMEM((2, size, width), F32),
            pltpu.VMEM((width, rows), BF16), pltpu.VMEM((2, rows, wide_size), BF16), pltpu.VMEM((2, width, wide_size), F32),
            pltpu.VMEM((classes, width), F32), PAIR, PAIR, PAIR, PAIR, PAIR, DMA(())],
        compiler_params=pltpu.CompilerParams(vmem_limit_bytes=LIMIT),
        cost_estimate=pl.CostEstimate(flops=flops, bytes_accessed=stored, transcendentals=0),
        name="weights",
    )(*inputs)


def matmul_rows(spec, left, right):
    return jnp.einsum(spec, left, right, preferred_element_type=F32)


def solution(mesh):
    stages = mesh.shape["pp"]
    in_specs = (P("dp"), P("dp"), P(), P(), P(), P()) + (P("pp"),) * 12 + (P(),) * 4
    out_specs = (P("dp"),) * 5 + (P(("dp", "pp")),) * 12 + (P("dp"),) * 4

    def body(patches, labels, w_patch, b_patch, cls_token, pos_embed, *rest):
        ln1_gain, ln1_bias, w_qkv, b_qkv, w_proj, b_proj, ln2_gain, ln2_bias, w_fc1, b_fc1, w_fc2, b_fc2 = (tensor[0] for tensor in rest[:12])
        lnf_gain, lnf_bias, w_head, b_head = rest[12:]
        tokens, width = pos_embed.shape
        heads, head = w_qkv.shape[2:]
        images = labels.size
        inv_count = 1.0 / images
        rows = -(-tokens // 16) * 16
        dims = (stages, images, tokens, heads, head)

        patch_size = patches.shape[-1]
        spare = -patch_size % LANES
        patch_rows = jnp.pad(patches.reshape((images,) + patches.shape[2:]), ((0, 0), (1, rows - tokens), (0, spare)))
        w_embed = jnp.pad(w_patch, ((0, spare), (0, 0)))
        is_patch = lax.broadcasted_iota(jnp.int32, (rows, 1), 0) > 0
        base = jnp.pad(pos_embed, ((0, rows - tokens), (0, 0))).astype(F32) + jnp.where(is_patch, b_patch.astype(F32), cls_token.astype(F32))
        embedded = (matmul_rows("inp,pd->ind", patch_rows, w_embed) + base).astype(BF16)

        line = lambda tensor: tensor.reshape(1, -1)
        wqkv_t = jnp.transpose(w_qkv, (1, 2, 3, 0)).reshape(3 * width, width)
        big = (wqkv_t, w_proj.reshape(width, width), w_fc1, w_fc2)
        vectors = tuple(map(line, (ln1_gain, ln1_bias, b_qkv, b_proj, ln2_gain, ln2_bias, b_fc1, b_fc2)))
        x_s, a_s, qkv_s, c_s, h_s, n_s, d_s, g_s, p_s, tops = run_forward(dims, embedded, *big, vectors)

        loss, gtop, g_lnf_gain, g_lnf_bias, *logit_parts, g_b_head = run_head(
            inv_count, tops, jnp.transpose(labels), lnf_gain, lnf_bias, jnp.transpose(w_head), b_head)

        gy_s, gpre_s, gmid_s, gqkv_s, gemb, *sums = run_backward(dims, gtop, *big, vectors[0], vectors[4], x_s, qkv_s, h_s, d_s, p_s)
        flat = lambda array: array.reshape(images * rows, -1)
        g_w_fc2, g_w_qkv, g_w_proj, g_w_fc1, g_w_head, g_w_patch, g_pos_embed, g_b_patch, g_cls_token, *sums = run_weights(
            tuple(map(flat, (g_s, gqkv_s, c_s, patch_rows, n_s))), tuple(map(flat, (gy_s, a_s, gmid_s, gemb, gpre_s))),
            logit_parts, patch_size, tokens, images, sums)
        g_ln1_gain, g_ln1_bias, g_ln2_gain, g_ln2_bias, g_b_proj, g_b_fc2, g_b_qkv, g_b_fc1 = sums
        g_w_qkv = jnp.transpose(g_w_qkv.reshape(3, heads, head, width), (3, 0, 1, 2))[None]
        layer_grads = (
            g_ln1_gain, g_ln1_bias, g_w_qkv, g_b_qkv.reshape(1, 3, heads, head), g_w_proj.reshape(1, heads, head, width), g_b_proj,
            g_ln2_gain, g_ln2_bias, g_w_fc1[None], g_b_fc1, g_w_fc2[None], g_b_fc2,
        )
        embed_grads = (g_w_patch, g_b_patch, g_cls_token, g_pos_embed)
        return (loss.reshape(1),) + embed_grads + layer_grads + (g_lnf_gain, g_lnf_bias, jnp.transpose(g_w_head), g_b_head)

    return jax.shard_map(body, mesh=mesh, in_specs=in_specs, out_specs=out_specs, check_vma=False)
```

```python
import functools
import math
import jax
import jax.numpy as jnp
from jax import lax
from jax.experimental import pallas as pl
from jax.experimental.pallas import tpu as pltpu
from jax.sharding import PartitionSpec as P

EPS = 1e-6
SMOOTH = 0.1
F32 = jnp.float32
BF16 = jnp.bfloat16
MESH = pl.DeviceIdType.MESH
LANES = 128
HALF = 384
CHUNK = 2 * HALF
GROUP = 4
BLOCK = 136
DOWN = {"axis": 0, "keepdims": True}
ACROSS = {"axis": -1, "keepdims": True}


def flip(index):
    return lax.rem(index, 2)


def third(index):
    return lax.rem(index, 3)


def layer_norm(hidden, gain, bias):
    values = hidden.astype(F32)
    centered = values - jnp.mean(values, **ACROSS)
    variance = jnp.mean(jnp.square(centered), **ACROSS)
    return (centered * lax.rsqrt(variance + EPS) * gain + bias).astype(BF16)


def dot(left, right, left_axis=1, right_axis=0):
    return lax.dot_general(left, right, (((left_axis,), (right_axis,)), ((), ())), preferred_element_type=F32)


def by_rows(rows, visit):
    def step(index, carry):
        visit(pl.ds(pl.multiple_of(index * BLOCK, BLOCK), BLOCK))
        return carry

    lax.fori_loop(0, rows // BLOCK, step, 0)
    if rows % BLOCK:
        visit(pl.ds(rows - rows % BLOCK, rows % BLOCK))


def fold(values):
    rows, columns = values.shape
    return jnp.sum(values.reshape(rows // 8, 8, columns), axis=0)


def everyone(stage, stages):
    barrier = pltpu.get_barrier_semaphore()
    for hop in range(1, stages):
        pl.semaphore_signal(barrier, device_id={"pp": lax.rem(stage + hop, stages)}, device_id_type=MESH)
    pl.semaphore_wait(barrier, stages - 1)


def weight_copies(wproj, wfc1, wfc2, vproj, vfc1, vfc2, sems):
    def of_chunk(source, target, which, by_lines):
        def copy(chunk):
            span = pl.ds(pl.multiple_of(chunk * CHUNK, CHUNK), CHUNK)
            part = span if by_lines else (slice(None), span)
            return pltpu.make_async_copy(source.at[part], target.at[part], sems.at[which, chunk])
        return copy

    proj = pltpu.make_async_copy(wproj, vproj, sems.at[0, 0])
    return proj, of_chunk(wfc1, vfc1, 1, False), of_chunk(wfc2, vfc2, 2, True)


def forward_kernel(dims, *refs):
    (emb, wqkv, wproj, wfc1, wfc2, *given,
     x_s, a_s, qkv_s, c_s, h_s, n_s, d_s, g_s, p_s, tops_out,
     vqkv, vproj, vfc1, vfc2, xin, act, qkv, mid, yacc, ubuf, gbuf, tops,
     g1, b1, bqkv, bproj, g2, b2, bfc2,
     wsem, qsem, recv_sem, send_sem, top_sem, save_sem, usem, gsem, psem, free_sem) = refs
    stages, images, tokens, heads, head = dims
    rows, width = mid.shape
    chunks = vfc1.shape[1] // CHUNK
    stage = lax.axis_index("pp")
    is_first = stage == 0
    is_last = stage == stages - 1
    scale2 = head ** -0.5 / math.log(2.0)


    def qkv_copy(part):
        lines = pl.ds(pl.multiple_of(part * width, LANES), width)
        return pltpu.make_async_copy(wqkv.at[lines], vqkv.at[lines], qsem.at[part])

    def emb_copy(image, slot):
        return pltpu.make_async_copy(emb.at[image], xin.at[slot], recv_sem.at[slot])

    @pl.when(is_first)
    def _():
        emb_copy(0, 0).start()
        emb_copy(1, 1).start()

    proj_copy, fc1_copy, fc2_copy = weight_copies(wproj, wfc1, wfc2, vproj, vfc1, vfc2, wsem)
    for part in range(3):
        qkv_copy(part).start()
    proj_copy.start()
    for chunk in range(chunks):
        fc1_copy(chunk).start()
        fc2_copy(chunk).start()
    qkv[:] = jnp.zeros_like(qkv)
    *lows, bfc1, low = given
    for low, wide in zip((*lows, low), (g1, b1, bqkv, bproj, g2, b2, bfc2)):
        wide[:] = low[:].astype(F32)
    everyone(stage, stages)

    def saves(image, slot):
        pairs = ((xin.at[slot], x_s), (act, a_s), (qkv, qkv_s), (act, c_s), (mid, h_s), (act, n_s))
        return [pltpu.make_async_copy(src, dst.at[image], save_sem.at[at]) for at, (src, dst) in enumerate(pairs)]

    class u_save:
        def __init__(self, image, chunk):
            slot = third(chunk)
            self.copies = [
                pltpu.make_async_copy(ubuf.at[slot, :, pl.ds(side * HALF, HALF)], d_s.at[image, chunk * 2 + side], usem.at[slot, side])
                for side in range(2)]

        def start(self):
            for copy in self.copies:
                copy.start()

        def wait(self):
            for copy in self.copies:
                copy.wait()

    def g_save(image, chunk):
        slot = flip(chunk)
        return pltpu.make_async_copy(gbuf.at[slot], g_s.at[image, :, pl.ds(pl.multiple_of(chunk * CHUNK, CHUNK), CHUNK)], gsem.at[slot])

    def p_slot(number):
        slot = number % 9
        if slot < 6:
            return ubuf.at[slot // 2, :, pl.ds(slot % 2 * HALF, HALF)]
        return yacc.at[:, pl.ds((slot - 6) * HALF, HALF)]

    def p_save(image, number):
        return pltpu.make_async_copy(p_slot(number), p_s.at[image, number], psem.at[number % 9])

    def top_copy(image, other):
        return pltpu.make_async_remote_copy(
            src_ref=mid.at[pl.ds(0, 8)], dst_ref=tops.at[image], send_sem=send_sem.at[1 + other], recv_sem=top_sem,
            device_id={"pp": other}, device_id_type=MESH)

    def next_copy(image, slot):
        return pltpu.make_async_remote_copy(
            src_ref=mid, dst_ref=xin.at[slot], send_sem=send_sem.at[0], recv_sem=recv_sem.at[slot],
            device_id={"pp": lax.rem(stage + 1, stages)}, device_id_type=MESH)

    def wait_sent(image):
        @pl.when(jnp.logical_not(is_last))
        def _():
            next_copy(image, 0).wait_send()

        @pl.when(is_last)
        def _():
            for other in range(stages - 1):
                top_copy(image, other).wait_send()

    def one_image(image, carry):
        slot = flip(image)
        save_x, save_a, save_qkv, save_c, save_h, save_n = saves(image, slot)
        emb_copy(image, slot).wait()
        save_x.start()

        @pl.when(image > 0)
        def _():
            save_n.wait()
            save_qkv.wait()

        def norm1(lines):
            act[lines, :] = layer_norm(xin[slot, lines, :], g1[:], b1[:])

        by_rows(rows, norm1)
        save_a.start()

        @pl.when(image == 0)
        def _():
            for part in range(3):
                qkv_copy(part).wait()

        low = (dot(act[:], vqkv[:], 1, 1) + bqkv[:]).astype(BF16)
        for at in range(3 * heads):
            qkv[:, at * LANES:at * LANES + head] = low[:, at * head:(at + 1) * head]
        save_qkv.start()

        save_a.wait()

        @pl.when(image > 0)
        def _():
            for chunk in range(3):
                u_save(image, chunk).wait()

        def scores_of(number):
            q, k = (qkv[:, lane:lane + LANES] for lane in (number * LANES, (heads + number) * LANES))
            return dot(k, q, 1, 1)

        def attend(number, scores):
            if number == 9:
                for slot in range(6):
                    p_save(image, slot).wait()
            if number > 14:
                p_save(image, number - 9).wait()
            v = qkv[:, (2 * heads + number) * LANES:(2 * heads + number + 1) * LANES]
            top, tail = scores[:tokens - 1], scores[tokens - 1:]
            most = jnp.maximum(jnp.max(top, **DOWN), tail[:1])
            top = jnp.exp2((top - most) * scale2)
            real = lax.broadcasted_iota(jnp.int32, tail.shape, 0) < 1
            tail = jnp.where(real, jnp.exp2(jnp.minimum(tail - most, 0.0) * scale2), 0.0)
            inv = 1.0 / (jnp.sum(top, **DOWN) + jnp.sum(tail, **DOWN))
            probs = jnp.concatenate([top, tail], axis=0) * inv
            p_slot(number)[:, :rows] = probs
            act[:, number * head:(number + 1) * head] = dot(probs.astype(BF16), v, 0, 0).astype(BF16)[:, :head]
            p_save(image, number).start()

        scores = scores_of(0)
        for number in range(heads):
            later = scores_of(number + 1) if number + 1 < heads else None
            attend(number, scores)
            scores = later
        save_c.start()

        @pl.when(image == 0)
        def _():
            proj_copy.wait()

        @pl.when(image > 0)
        def _():
            wait_sent(image)

        mid[:] = (dot(act[:], vproj[:]) + bproj[:] + xin[slot].astype(F32)).astype(BF16)
        save_h.start()
        save_x.wait()

        @pl.when(jnp.logical_and(is_first, image + 2 < images))
        def _():
            emb_copy(image + 2, slot).start()

        @pl.when(jnp.logical_and(stage > 0, image + 2 < images))
        def _():
            pl.semaphore_signal(free_sem, device_id={"pp": lax.rem(stage + stages - 1, stages)}, device_id_type=MESH)

        save_c.wait()
        for number in (7, 8, 15):
            p_save(image, number).wait()

        def norm2(lines):
            hidden = mid[lines, :]
            act[lines, :] = layer_norm(hidden, g2[:], b2[:])
            yacc[lines, :] = hidden.astype(F32) + bfc2[:]

        by_rows(rows, norm2)
        save_n.start()

        @pl.when(image == 0)
        def _():
            fc1_copy(0).wait()

        for number in range(9, 15):
            p_save(image, number).wait()

        @pl.when(image > 0)
        def _():
            for chunk in range(2):
                g_save(image, chunk).wait()

        def fc1(chunk):
            columns = pl.ds(pl.multiple_of(chunk * CHUNK, CHUNK), CHUNK)
            ubuf[third(chunk)] = dot(act[:], vfc1[:, columns]) + bfc1[:, columns].astype(F32)

        def gelu(chunk):
            slot3, slot2 = third(chunk), flip(chunk)
            pre = ubuf[slot3]
            cdf = 0.5 + 0.5 * lax.erf(pre * (0.5 ** 0.5))
            pdf = jnp.exp2(pre * pre * (-0.5 / math.log(2.0))) * ((2.0 * math.pi) ** -0.5)
            activ = (pre * cdf).astype(BF16)
            gbuf[slot2] = activ
            ubuf[slot3] = cdf + pre * pdf
            return activ

        def fc2(chunk, activ):
            yacc[:] += dot(activ, vfc2[pl.ds(pl.multiple_of(chunk * CHUNK, CHUNK), CHUNK), :])

        fc1(0)

        def mlp_step(chunk, carry):
            @pl.when(chunk >= 3)
            def _():
                u_save(image, chunk).wait()
                g_save(image, chunk - 1).wait()

            @pl.when(image == 0)
            def _():
                fc1_copy(chunk).wait()
                fc2_copy(chunk - 1).wait()

            @pl.when(chunk >= 2)
            def _():
                u_save(image, chunk - 2).start()
                g_save(image, chunk - 2).start()

            activ = gelu(chunk - 1)
            fc1(chunk)
            fc2(chunk - 1, activ)
            return carry

        lax.fori_loop(1, chunks, mlp_step, 0)

        @pl.when(image == 0)
        def _():
            fc2_copy(chunks - 1).wait()

        g_save(image, chunks - 1).wait()
        u_save(image, chunks - 2).start()
        g_save(image, chunks - 2).start()
        fc2(chunks - 1, gelu(chunks - 1))
        u_save(image, chunks - 1).start()
        g_save(image, chunks - 1).start()

        save_h.wait()
        mid[:] = yacc[:].astype(BF16)

        @pl.when(jnp.logical_and(jnp.logical_not(is_last), image >= 2))
        def _():
            pl.semaphore_wait(free_sem, 1)

        @pl.when(jnp.logical_not(is_last))
        def _():
            next_copy(image, slot).start()

        @pl.when(is_last)
        def _():
            for other in range(stages - 1):
                top_copy(image, other).start()
            tops[image] = mid[pl.ds(0, 8), :]

        return carry

    lax.fori_loop(0, images, one_image, 0)
    wait_sent(images - 1)
    _, _, save_qkv, _, _, save_n = saves(images - 1, 0)
    save_qkv.wait()
    save_n.wait()
    for chunk in range(3):
        u_save(images - 1, chunk).wait()
    for chunk in range(2):
        g_save(images - 1, chunk).wait()

    @pl.when(jnp.logical_not(is_last))
    def _():
        pltpu.make_async_copy(tops, tops, top_sem).wait()

    for image in range(images):
        tops_out[image:image + 1, :] = tops[image, 0:1, :]


def norm_backward(grad, hidden, gain):
    values = hidden.astype(F32)
    centered = values - jnp.mean(values, **ACROSS)
    inv = lax.rsqrt(jnp.mean(jnp.square(centered), **ACROSS) + EPS)
    unit = centered * inv
    scaled = grad * gain
    grad_in = inv * (scaled - jnp.mean(scaled, **ACROSS) - unit * jnp.mean(scaled * unit, **ACROSS))
    return grad_in, grad * unit


def backward_kernel(dims, *refs):
    (gtop, wqkv, wproj, wfc1, wfc2, low1, low2, x_s, qkv_s, h_s, d_s, p_s,
     gy_s, gpre_s, gmid_s, gqkv_s, gemb, *sums_out,
     vqkv, vproj, vfc1, vfc2, gin, acc, shared, gbuf, gmid, gctx, qkv, gqkv, g1, g2,
     sum1g, sum1b, sum2g, sum2b, sumproj, sumfc2, sumqkv, sumfc1,
     wsem, qsem, recv_sem, top_sem, send_sem, emb_sem, relay_sem, save_sem, load_sem, dsem, gsem, psem, free_sem) = refs
    stages, images, tokens, heads, head = dims
    rows, width = gmid.shape
    hid, old, gout = gqkv.at[:, :width], qkv.at[:, :width], gctx.at[:, :width]

    def abuf(chunk):
        return gqkv.at[:, pl.ds(pl.multiple_of(width + flip(chunk) * CHUNK, LANES), CHUNK)]

    chunks = vfc1.shape[1] // CHUNK
    stage = lax.axis_index("pp")
    is_first = stage == 0
    is_last = stage == stages - 1
    scale = head ** -0.5

    pieces = ((0, vqkv.shape[1]), (vqkv.shape[1], width - vqkv.shape[1]))

    def qkv_copy(part, side):
        slot = flip(part) * 2 + side
        at, size = pieces[side]
        lines = pl.ds(pl.multiple_of(third(part) * width + at, 128), size)
        return pltpu.make_async_copy(wqkv.at[lines], vqkv.at[slot, pl.ds(0, size)], qsem.at[slot])

    def top_copy(image, slot):
        return pltpu.make_async_copy(gtop.at[image], gin.at[slot, pl.ds(0, 16)], top_sem.at[slot])

    def d_load(image, chunk):
        slot = lax.rem(chunk, 4)
        return pltpu.make_async_copy(d_s.at[image, pl.ds(chunk * 2, 2)], shared.at[pl.ds(slot * 2, 2)], dsem.at[slot])

    def g_save(image, chunk):
        slot = flip(chunk)
        return pltpu.make_async_copy(gbuf.at[slot], gpre_s.at[image, :, pl.ds(pl.multiple_of(chunk * CHUNK, CHUNK), CHUNK)], gsem.at[slot])

    held = shared.shape[0] + 3

    def p_slot(number):
        slot = number % held
        if slot < shared.shape[0]:
            return shared.at[slot]
        return acc.at[:, pl.ds((slot - shared.shape[0]) * HALF, HALF)]

    def p_load(image, number):
        return pltpu.make_async_copy(p_s.at[image, number], p_slot(number), psem.at[number % held])

    def saves(image, slot):
        pairs = ((gin.at[slot], gy_s), (gmid, gmid_s), (gqkv, gqkv_s))
        return [pltpu.make_async_copy(src, dst.at[image], save_sem.at[at]) for at, (src, dst) in enumerate(pairs)]

    def loads(image):
        pairs = ((h_s, hid), (x_s, old), (qkv_s, qkv))
        return [pltpu.make_async_copy(src.at[image], dst, load_sem.at[at]) for at, (src, dst) in enumerate(pairs)]

    def next_copy(slot):
        return pltpu.make_async_remote_copy(
            src_ref=gout, dst_ref=gin.at[slot], send_sem=send_sem.at[0], recv_sem=recv_sem.at[slot],
            device_id={"pp": lax.rem(stage + stages - 1, stages)}, device_id_type=MESH)

    def emb_send(image, other):
        return pltpu.make_async_remote_copy(
            src_ref=gout, dst_ref=gemb.at[image], send_sem=send_sem.at[other], recv_sem=emb_sem.at[image],
            device_id={"pp": other}, device_id_type=MESH)

    def emb_relay(image):
        return pltpu.make_async_remote_copy(
            src_ref=gemb.at[image], dst_ref=gemb.at[image], send_sem=relay_sem.at[image], recv_sem=emb_sem.at[image],
            device_id={"pp": stages - 1}, device_id_type=MESH)

    def emb_local(image):
        return pltpu.make_async_copy(gout, gemb.at[image], save_sem.at[3])

    def wait_sent(image):
        @pl.when(jnp.logical_not(is_first))
        def _():
            next_copy(0).wait_send()

        @pl.when(is_first)
        def _():
            for other in range(1, stages - 1):
                emb_send(image, other).wait_send()
            emb_local(image).wait()

    @pl.when(is_last)
    def _():
        gin[:] = jnp.zeros_like(gin)
        top_copy(0, 0).start()
        top_copy(1, 1).start()

    proj_copy, fc1_copy, fc2_copy = weight_copies(wproj, wfc1, wfc2, vproj, vfc1, vfc2, wsem)
    for chunk in range(chunks):
        fc2_copy(chunk).start()
        if chunk < 4:
            d_load(0, chunk).start()
        fc1_copy(chunk).start()
    proj_copy.start()
    for part in range(2):
        for side in range(2):
            qkv_copy(part, side).start()
    gctx[:] = jnp.zeros_like(gctx)
    sums_out, totals = sums_out[:8], (sum1g, sum1b, sum2g, sum2b, sumproj, sumfc2, sumqkv, sumfc1)
    for total in totals:
        total[:] = jnp.zeros_like(total)
    g1[:] = low1[:].astype(F32)
    g2[:] = low2[:].astype(F32)
    everyone(stage, stages)

    def one_image(image, carry):
        slot = flip(image)
        more = image + 1 < images
        save_gy, save_mid, save_qkv = saves(image, slot)
        load_h, load_x, load_qkv = loads(image)

        @pl.when(is_last)
        def _():
            top_copy(image, slot).wait()

        @pl.when(jnp.logical_not(is_last))
        def _():
            next_copy(slot).wait_recv()

        save_gy.start()

        load_qkv.start()

        @pl.when(image > 0)
        def _():
            save_qkv.wait()

        load_h.start()

        @pl.when(image == 0)
        def _():
            fc2_copy(0).wait()

        @pl.when(image > 0)
        def _():
            for chunk in range(2):
                g_save(image, chunk).wait()

        acc[:] = jnp.zeros_like(acc)

        def fc2(chunk):
            lines = pl.ds(pl.multiple_of(chunk * CHUNK, CHUNK), CHUNK)
            abuf(chunk)[:] = dot(gin[slot], vfc2[lines, :], 1, 1).astype(BF16)

        def gelu(chunk):
            columns = pl.ds(pl.multiple_of(chunk * CHUNK, CHUNK), CHUNK)
            slot2 = flip(chunk)
            slot4 = lax.rem(chunk, 4)
            pre = abuf(chunk)[:].astype(F32) * jnp.concatenate([shared[slot4 * 2], shared[slot4 * 2 + 1]], axis=1)
            sumfc1[:, columns] += fold(pre)
            low = pre.astype(BF16)
            gbuf[slot2] = low
            return low

        def fc1(chunk, low):
            columns = pl.ds(pl.multiple_of(chunk * CHUNK, CHUNK), CHUNK)
            acc[:] += dot(low, vfc1[:, columns], 1, 1)

        fc2(0)

        def mlp_step(chunk, carry):
            d_load(image, chunk - 1).wait()

            @pl.when(image == 0)
            def _():
                fc2_copy(chunk).wait()
                fc1_copy(chunk - 1).wait()

            @pl.when(chunk >= 3)
            def _():
                g_save(image, chunk - 1).wait()

            @pl.when(chunk >= 2)
            def _():
                g_save(image, chunk - 2).start()

                @pl.when(chunk + 2 < chunks)
                def _():
                    d_load(image, chunk + 2).start()

            low = gelu(chunk - 1)
            fc2(chunk)
            fc1(chunk - 1, low)
            return carry

        lax.fori_loop(1, chunks, mlp_step, 0)
        d_load(image, chunks - 1).wait()

        @pl.when(image == 0)
        def _():
            fc1_copy(chunks - 1).wait()

        g_save(image, chunks - 1).wait()
        g_save(image, chunks - 2).start()
        fc1(chunks - 1, gelu(chunks - 1))
        g_save(image, chunks - 1).start()

        for number in range(shared.shape[0]):
            p_load(image, number).start()
        load_h.wait()

        @pl.when(image > 0)
        def _():
            save_mid.wait()

        def back2(lines):
            grad = acc[lines, :].astype(BF16).astype(F32)
            grad_in, by_unit = norm_backward(grad, hid[lines, :], g2[:])
            sum2g[:] += fold(by_unit)
            sum2b[:] += fold(grad)
            top = gin[slot, lines, :].astype(F32)
            sumfc2[:] += fold(top)
            low = (top + grad_in).astype(BF16)
            gmid[lines, :] = low
            sumproj[:] += fold(low.astype(F32))

        by_rows(rows, back2)
        for number in range(shared.shape[0], held):
            p_load(image, number).start()
        save_mid.start()
        save_gy.wait()

        @pl.when(jnp.logical_and(is_last, image + 2 < images))
        def _():
            top_copy(image + 2, slot).start()

        @pl.when(jnp.logical_and(stage < stages - 1, image + 2 < images))
        def _():
            pl.semaphore_signal(free_sem, device_id={"pp": lax.rem(stage + 1, stages)}, device_id_type=MESH)

        @pl.when(image == 0)
        def _():
            proj_copy.wait()


        @pl.when(image > 0)
        def _():
            wait_sent(image)

        low = dot(gmid[:], vproj[:], 1, 1).astype(BF16)
        for number in range(heads):
            gctx[:, number * LANES:number * LANES + head] = low[:, number * head:(number + 1) * head]
        load_qkv.wait()
        for number in range(held):
            p_load(image, number).wait()
        def lanes_of(number):
            return slice(number * LANES, (number + 1) * LANES)

        def grad_probs_of(number):
            return dot(qkv[:, lanes_of(2 * heads + number)], gctx[:, lanes_of(number)], 1, 1)

        def attend(number, grad_probs):
            if number == held:
                for later in range(held, heads):
                    p_load(image, later).wait()
            probs = p_slot(number)[:, :rows]
            at = number * head
            mean = jnp.sum(grad_probs * probs, **DOWN)
            low = (probs * (grad_probs - mean) * scale).astype(BF16)
            value = dot(probs.astype(BF16), gctx[:, lanes_of(number)]).astype(BF16)
            gqkv[:, 2 * width + at:2 * width + at + head] = value[:, :head]
            key = dot(low, qkv[:, lanes_of(number)]).astype(BF16)
            gqkv[:, width + at:width + at + head] = key[:, :head]
            query = dot(low, qkv[:, lanes_of(heads + number)], 0, 0).astype(BF16)
            gqkv[:, at:at + head] = query[:, :head]

        grad_probs = grad_probs_of(0)
        for number in range(heads):
            later = grad_probs_of(number + 1) if number + 1 < heads else None
            attend(number, grad_probs)
            grad_probs = later
            if number + held < heads:
                p_load(image, number + held).start()
        save_qkv.start()
        load_x.start()

        def qkv_part(part, carry):
            index = image * 3 + part
            for side in range(2):
                qkv_copy(index, side).wait()
            for side in range(2):
                at, size = pieces[side]
                columns = pl.ds(pl.multiple_of(part * width + at, LANES), size)
                piece = gqkv[:, columns]
                sumqkv[:, columns] += fold(piece.astype(F32))
                acc[:] += dot(piece, vqkv[flip(index) * 2 + side, :size])

            @pl.when(index + 2 < images * 3)
            def _():
                for side in range(2):
                    qkv_copy(index + 2, side).start()

            return carry

        acc[:] = jnp.zeros_like(acc)
        lax.fori_loop(0, 3, qkv_part, 0)

        @pl.when(more)
        def _():
            for chunk in range(4):
                d_load(image + 1, chunk).start()

        load_x.wait()

        def back1(lines):
            grad = acc[lines, :].astype(BF16).astype(F32)
            grad_in, by_unit = norm_backward(grad, old[lines, :], g1[:])
            sum1g[:] += fold(by_unit)
            sum1b[:] += fold(grad)
            gout[lines, :] = (gmid[lines, :].astype(F32) + grad_in).astype(BF16)

        by_rows(rows, back1)

        @pl.when(jnp.logical_and(jnp.logical_not(is_first), image >= 2))
        def _():
            pl.semaphore_wait(free_sem, 1)

        @pl.when(jnp.logical_not(is_first))
        def _():
            next_copy(slot).start()

        @pl.when(is_first)
        def _():
            for other in range(1, stages - 1):
                emb_send(image, other).start()
            emb_local(image).start()

        return carry

    lax.fori_loop(0, images, one_image, 0)
    wait_sent(images - 1)
    _, save_mid, save_qkv = saves(images - 1, 0)
    save_mid.wait()
    save_qkv.wait()
    for chunk in range(2):
        g_save(images - 1, chunk).wait()

    for out, total in zip(sums_out, totals):
        out[:] = jnp.sum(total[:], **DOWN)

    @pl.when(jnp.logical_not(is_first))
    def _():
        for image in range(images):
            emb_relay(image).wait_recv()

            @pl.when(stage == stages - 2)
            def _():
                emb_relay(image).start()

    @pl.when(stage == stages - 2)
    def _():
        for image in range(images):
            emb_relay(image).wait_send()


ANY = pl.BlockSpec(memory_space=pl.ANY)
VMEM = pl.BlockSpec(memory_space=pltpu.VMEM)
LIMIT = 67_043_328
DMA = pltpu.SemaphoreType.DMA
PAIR = DMA((2,))
TRIPLE = DMA((3,))


def run_forward(dims, emb, wqkv, wproj, wfc1, wfc2, vectors):
    stages, images, tokens, heads, head = dims
    rows, width = emb.shape[1:]
    hidden = wfc1.shape[1]
    hbm = lambda *shape, dtype=BF16: jax.ShapeDtypeStruct((images, rows) + shape, dtype)
    return pl.pallas_call(
        functools.partial(forward_kernel, dims),
        out_shape=(
            hbm(width), hbm(width), hbm(3 * heads * LANES), hbm(width), hbm(width), hbm(width),
            jax.ShapeDtypeStruct((images, hidden // HALF, rows, HALF), F32), hbm(hidden),
            jax.ShapeDtypeStruct((images, heads, rows, HALF), F32), jax.ShapeDtypeStruct((images, width), BF16)),
        in_specs=[ANY] * 5 + [VMEM] * 8,
        out_specs=(ANY,) * 9 + (VMEM,),
        scratch_shapes=[
            pltpu.VMEM(wqkv.shape, BF16), pltpu.VMEM(wproj.shape, BF16), pltpu.VMEM(wfc1.shape, BF16), pltpu.VMEM(wfc2.shape, BF16),
            pltpu.VMEM((2, rows, width), BF16), pltpu.VMEM((rows, width), BF16), pltpu.VMEM((rows, 3 * heads * LANES), BF16),
            pltpu.VMEM((rows, width), BF16), pltpu.VMEM((rows, width), F32),
            pltpu.VMEM((3, rows, CHUNK), F32), pltpu.VMEM((2, rows, CHUNK), BF16),
            pltpu.VMEM((images, 8, width), BF16),
            *(pltpu.VMEM(vector.shape, F32) for vector in vectors[:6]), pltpu.VMEM(vectors[7].shape, F32),
            DMA((3, hidden // CHUNK)), TRIPLE, PAIR, DMA((stages,)), DMA(()), DMA((6,)), DMA((3, 2)), PAIR, DMA((9,)),
            pltpu.SemaphoreType.REGULAR],
        compiler_params=pltpu.CompilerParams(collective_id=0, has_side_effects=True, vmem_limit_bytes=LIMIT),
        name="forward",
    )(emb, wqkv, wproj, wfc1, wfc2, *vectors)


def run_backward(dims, gtop, wqkv, wproj, wfc1, wfc2, g1, g2, x_s, qkv_s, h_s, d_s, p_s):
    stages, images, tokens, heads, head = dims
    rows, width = x_s.shape[1:]
    hidden = wfc1.shape[1]
    hbm = lambda *shape: jax.ShapeDtypeStruct((images, rows) + shape, BF16)
    sizes = (width,) * 6 + (3 * width, hidden)
    return pl.pallas_call(
        functools.partial(backward_kernel, dims),
        out_shape=(hbm(width), hbm(hidden), hbm(width), hbm(3 * width), hbm(width)) + tuple(jax.ShapeDtypeStruct((1, size), F32) for size in sizes),
        in_specs=[ANY] * 5 + [VMEM] * 2 + [ANY] * 5,
        out_specs=(ANY,) * 5 + (VMEM,) * 8,
        scratch_shapes=[
            pltpu.VMEM((4, -(-width // 256) * LANES, width), BF16), pltpu.VMEM(wproj.shape, BF16), pltpu.VMEM(wfc1.shape, BF16), pltpu.VMEM(wfc2.shape, BF16),
            pltpu.VMEM((2, rows, width), BF16), pltpu.VMEM((rows, width), F32), pltpu.VMEM((2 * GROUP, rows, HALF), F32),
            pltpu.VMEM((2, rows, CHUNK), BF16),
            pltpu.VMEM((rows, width), BF16), pltpu.VMEM((rows, heads * LANES), BF16),
            pltpu.VMEM((rows, 3 * heads * LANES), BF16), pltpu.VMEM((rows, 3 * width), BF16),
            pltpu.VMEM((1, width), F32), pltpu.VMEM((1, width), F32),
            *(pltpu.VMEM((8, size), F32) for size in sizes),
            DMA((3, hidden // CHUNK)), DMA((4,)), PAIR, PAIR, DMA((stages,)), DMA((images,)), DMA((images,)), DMA((4,)), TRIPLE, DMA((4,)), PAIR, DMA((2 * GROUP + 3,)),
            pltpu.SemaphoreType.REGULAR],
        compiler_params=pltpu.CompilerParams(collective_id=1, has_side_effects=True, vmem_limit_bytes=LIMIT),
        name="backward",
    )(gtop, wqkv, wproj, wfc1, wfc2, g1, g2, x_s, qkv_s, h_s, d_s, p_s)


def head_kernel(inv_count, tops, labels, gain, bias, w_head, b_head, loss, gtop, g_gain, g_bias, low_out, pooled_out, g_b_head):
    images, width = tops.shape
    line = lambda ref: ref[:].reshape(1, -1).astype(F32)
    wide_gain = line(gain)
    pooled = layer_norm(tops[:], wide_gain, line(bias))
    logits = dot(pooled, w_head[:], 1, 1) + line(b_head)
    shifted = logits - jnp.max(logits, **ACROSS)
    log_probs = shifted - jnp.log(jnp.sum(jnp.exp(shifted), **ACROSS))
    classes = logits.shape[-1]
    number = lax.broadcasted_iota(jnp.int32, (images, 1), 0)
    label = jnp.zeros((images, 1), jnp.int32)
    for image in range(images):
        label = jnp.where(number == image, labels[image % labels.shape[0], image // labels.shape[0]], label)
    chosen = (lax.broadcasted_iota(jnp.int32, logits.shape, 1) == label).astype(F32)
    target = (1.0 - SMOOTH) * chosen + SMOOTH / classes
    parts = jnp.sum(target * log_probs, **ACROSS)
    loss[:] = -jnp.sum(parts, **DOWN) * inv_count
    grad_logits = (jnp.exp(log_probs) - target) * inv_count
    low = grad_logits.astype(BF16)
    low_out[:] = low
    pooled_out[:] = pooled
    g_b_head[:] = jnp.sum(grad_logits, axis=0)
    grad = dot(low, w_head[:]).astype(BF16).astype(F32)
    grad_in, by_unit = norm_backward(grad, tops[:], wide_gain)
    g_gain[:] = jnp.sum(by_unit, axis=0)
    g_bias[:] = jnp.sum(grad, axis=0)
    gtop[:] = jnp.zeros_like(gtop)
    for image in range(images):
        gtop[image, 0:1, :] = grad_in[image:image + 1].astype(BF16)


def run_head(inv_count, tops, labels, gain, bias, w_head, b_head):
    images, width = tops.shape
    classes = w_head.shape[0]
    shape = lambda *dims, dtype=F32: jax.ShapeDtypeStruct(dims, dtype)
    return pl.pallas_call(
        functools.partial(head_kernel, inv_count),
        out_shape=(shape(1, 1), shape(images, 16, width, dtype=BF16), shape(width), shape(width),
            shape(images, classes, dtype=BF16), shape(images, width, dtype=BF16), shape(classes)),
        in_specs=[VMEM, pl.BlockSpec(memory_space=pltpu.SMEM)] + [VMEM] * 4,
        out_specs=(VMEM,) * 7,
        compiler_params=pltpu.CompilerParams(vmem_limit_bytes=LIMIT),
        name="head",
    )(tops, labels, gain, bias, w_head, b_head)


def weight_kernel(rows, given, made, *refs):
    fc2_l, qkv_l, proj_l, patch_l, fc2_r, qkv_r, proj_r, patch_r, fc1_l, fc1_r, logit_l, logit_r, *sums = refs[:given]
    fc2_o, qkv_o, proj_o, fc1_o, head_o, patch_o, pos_o, bias_o, first_o, *sums_out = refs[given:given + made]
    lhs, rhs, out, turned, block, wide, logit, lsem, rsem, osem, bsem, wsem, hsem = refs[given + made:]
    width = rhs.shape[2]
    size, wide_size = lhs.shape[2], block.shape[2]
    tail = width % size
    patches = patch_l.shape[1] // size + 1
    ends = [fc2_l.shape[1] // size]
    ends.append(ends[0] + qkv_l.shape[1] // size)
    ends.append(ends[1] + width // size + 1)
    ends.append(ends[2] + patches)
    starts = [0] + ends[:3]
    steps = ends[3]
    wide_steps = fc1_r.shape[1] // wide_size

    def lines(at, unit):
        return pl.ds(pl.multiple_of(at * unit, LANES), unit)

    def left_copy(step, act):
        slot = flip(step)
        for product, source in enumerate((fc2_l, qkv_l, proj_l, patch_l)):
            full = source.shape[1] // size
            first = starts[product]

            @pl.when(jnp.logical_and(step >= first, step < first + full))
            def _():
                act(pltpu.make_async_copy(source.at[:, lines(step - first, size)], lhs.at[slot], lsem.at[slot]))

            if source.shape[1] % size:
                @pl.when(step == first + full)
                def _():
                    act(pltpu.make_async_copy(source.at[:, pl.ds(full * size, tail)], lhs.at[slot, :, pl.ds(0, tail)], lsem.at[slot]))

    def out_copy(step, act):
        slot = flip(step)
        for product, target in enumerate((fc2_o, qkv_o, proj_o)):
            full = target.shape[0] // size
            first = starts[product]

            @pl.when(jnp.logical_and(step >= first, step < first + full))
            def _():
                act(pltpu.make_async_copy(out.at[slot], target.at[lines(step - first, size)], osem.at[slot]))

            if target.shape[0] % size:
                @pl.when(step == first + full)
                def _():
                    act(pltpu.make_async_copy(out.at[slot, pl.ds(0, tail)], target.at[pl.ds(full * size, tail)], osem.at[slot]))

    def right_copy(product):
        source = (fc2_r, qkv_r, proj_r, patch_r, fc1_l)[product]
        return pltpu.make_async_copy(source, rhs.at[product % 2], rsem.at[product % 2])

    def block_copy(step):
        slot = flip(step)
        return pltpu.make_async_copy(fc1_r.at[:, lines(step, wide_size)], block.at[slot], bsem.at[slot])

    def wide_copy(step):
        slot = flip(step)
        return pltpu.make_async_copy(wide.at[slot], fc1_o.at[:, lines(step, wide_size)], wsem.at[slot])

    start = lambda copy: copy.start()
    wait = lambda copy: copy.wait()
    left_copy(0, start)
    right_copy(0).start()
    right_copy(1).start()
    for total, passed in zip(sums, sums_out):
        passed[:] = total[:]
    logit[:] = dot(logit_l[:], logit_r[:], 0, 0)
    head_copy = pltpu.make_async_copy(logit, head_o, hsem)
    head_copy.start()

    def embedding_sums(source):
        bias = jnp.zeros_like(bias_o)
        for at in range(0, rows, BLOCK):
            total = sum(source[image + at:image + at + BLOCK, :].astype(F32) for image in range(0, source.shape[0], rows))
            count = min(BLOCK, pos_o.shape[0] - at)
            pos_o[at:at + count, :] = total[:count]
            is_first = lax.broadcasted_iota(jnp.int32, total.shape, 0) + at < 1
            bias = bias + jnp.sum(jnp.where(is_first, 0.0, total), axis=0)
            if at == 0:
                first_o[:] = jnp.sum(jnp.where(is_first, total, 0.0), axis=0)
        bias_o[:] = bias

    def one_step(step, carry):
        slot = flip(step)

        @pl.when(step >= 1)
        def _():
            out_copy(step - 1, start)

        @pl.when(step >= 2)
        def _():
            out_copy(step - 2, wait)

        @pl.when(step + 1 < steps)
        def _():
            left_copy(step + 1, start)

        for product, first in enumerate(starts):
            @pl.when(step == first)
            def _(product=product):
                right_copy(product).wait()
                if product >= 1:
                    right_copy(product + 1).start()
                if product == 3:
                    embedding_sums(rhs.at[1])

        @pl.when(step == steps - 1)
        def _():
            block_copy(0).start()

        left_copy(step, wait)
        which = lax.rem(sum((step >= end).astype(jnp.int32) for end in ends[:3]), 2)
        out[slot] = dot(lhs[slot], rhs[which], 0, 0)
        for at in range(patches):
            count = min(size, patch_o.shape[0] - at * size)

            @pl.when(step == starts[3] + at)
            def _():
                patch_o[at * size:at * size + count, :] = out[slot, :count, :]

        return carry

    lax.fori_loop(0, steps, one_step, 0)
    right_copy(4).wait()
    turned[:] = rhs[0].T

    def wide_step(step, carry):
        slot = flip(step)

        @pl.when(step >= 1)
        def _():
            wide_copy(step - 1).start()

        @pl.when(step >= 2)
        def _():
            wide_copy(step - 2).wait()

        @pl.when(step + 1 < wide_steps)
        def _():
            block_copy(step + 1).start()

        block_copy(step).wait()
        wide[slot] = dot(turned[:], block[slot])
        return carry

    lax.fori_loop(0, wide_steps, wide_step, 0)
    wide_copy(wide_steps - 1).start()
    wide_copy(wide_steps - 2).wait()
    wide_copy(wide_steps - 1).wait()
    head_copy.wait()


def run_weights(lefts, rights, logit_parts, patch_size, tokens, images, sums):
    fc2_l, qkv_l, proj_l, patch_l, fc1_l = lefts
    fc2_r, qkv_r, proj_r, patch_r, fc1_r = rights
    rows, width = fc2_r.shape
    size, wide_size = 3 * LANES, 4 * LANES
    classes = logit_parts[0].shape[1]
    outs = [(left.shape[1], right.shape[1]) for left, right in zip(lefts, rights)]
    outs = outs[:3] + outs[4:]
    flops = sum(2 * rows * a * b for a, b in outs)
    stored = sum(4 * a * b for a, b in outs)
    outs += [(classes, width), (patch_size, width), (tokens, width), (width,), (width,)] + [total.shape for total in sums]
    inputs = (fc2_l, qkv_l, proj_l, patch_l, fc2_r, qkv_r, proj_r, patch_r, fc1_l, fc1_r, *logit_parts, *sums)
    return pl.pallas_call(
        functools.partial(weight_kernel, rows // images, len(inputs), len(outs)),
        out_shape=tuple(jax.ShapeDtypeStruct(shape, F32) for shape in outs),
        in_specs=[ANY] * 10 + [VMEM] * (2 + len(sums)),
        out_specs=(ANY,) * 5 + (VMEM,) * (len(outs) - 5),
        scratch_shapes=[
            pltpu.VMEM((2, rows, size), BF16), pltpu.VMEM((2, rows, width), BF16), pltpu.VMEM((2, size, width), F32),
            pltpu.VMEM((width, rows), BF16), pltpu.VMEM((2, rows, wide_size), BF16), pltpu.VMEM((2, width, wide_size), F32),
            pltpu.VMEM((classes, width), F32), PAIR, PAIR, PAIR, PAIR, PAIR, DMA(())],
        compiler_params=pltpu.CompilerParams(vmem_limit_bytes=LIMIT),
        cost_estimate=pl.CostEstimate(flops=flops, bytes_accessed=stored, transcendentals=0),
        name="weights",
    )(*inputs)


def matmul_rows(spec, left, right):
    return jnp.einsum(spec, left, right, preferred_element_type=F32)


def solution(mesh):
    stages = mesh.shape["pp"]
    in_specs = (P("dp"), P("dp"), P(), P(), P(), P()) + (P("pp"),) * 12 + (P(),) * 4
    out_specs = (P("dp"),) * 5 + (P(("dp", "pp")),) * 12 + (P("dp"),) * 4

    def body(patches, labels, w_patch, b_patch, cls_token, pos_embed, *rest):
        ln1_gain, ln1_bias, w_qkv, b_qkv, w_proj, b_proj, ln2_gain, ln2_bias, w_fc1, b_fc1, w_fc2, b_fc2 = (tensor[0] for tensor in rest[:12])
        lnf_gain, lnf_bias, w_head, b_head = rest[12:]
        tokens, width = pos_embed.shape
        heads, head = w_qkv.shape[2:]
        images = labels.size
        inv_count = 1.0 / images
        rows = -(-tokens // 16) * 16
        dims = (stages, images, tokens, heads, head)

        patch_size = patches.shape[-1]
        spare = -patch_size % LANES
        patch_rows = jnp.pad(patches.reshape((images,) + patches.shape[2:]), ((0, 0), (1, rows - tokens), (0, spare)))
        w_embed = jnp.pad(w_patch, ((0, spare), (0, 0)))
        is_patch = lax.broadcasted_iota(jnp.int32, (rows, 1), 0) > 0
        base = jnp.pad(pos_embed, ((0, rows - tokens), (0, 0))).astype(F32) + jnp.where(is_patch, b_patch.astype(F32), cls_token.astype(F32))
        embedded = (matmul_rows("inp,pd->ind", patch_rows, w_embed) + base).astype(BF16)

        line = lambda tensor: tensor.reshape(1, -1)
        wqkv_t = jnp.transpose(w_qkv, (1, 2, 3, 0)).reshape(3 * width, width)
        big = (wqkv_t, w_proj.reshape(width, width), w_fc1, w_fc2)
        vectors = tuple(map(line, (ln1_gain, ln1_bias, b_qkv, b_proj, ln2_gain, ln2_bias, b_fc1, b_fc2)))
        x_s, a_s, qkv_s, c_s, h_s, n_s, d_s, g_s, p_s, tops = run_forward(dims, embedded, *big, vectors)

        loss, gtop, g_lnf_gain, g_lnf_bias, *logit_parts, g_b_head = run_head(
            inv_count, tops, jnp.transpose(labels), lnf_gain, lnf_bias, jnp.transpose(w_head), b_head)

        gy_s, gpre_s, gmid_s, gqkv_s, gemb, *sums = run_backward(dims, gtop, *big, vectors[0], vectors[4], x_s, qkv_s, h_s, d_s, p_s)
        flat = lambda array: array.reshape(images * rows, -1)
        g_w_fc2, g_w_qkv, g_w_proj, g_w_fc1, g_w_head, g_w_patch, g_pos_embed, g_b_patch, g_cls_token, *sums = run_weights(
            tuple(map(flat, (g_s, gqkv_s, c_s, patch_rows, n_s))), tuple(map(flat, (gy_s, a_s, gmid_s, gemb, gpre_s))),
            logit_parts, patch_size, tokens, images, sums)
        g_ln1_gain, g_ln1_bias, g_ln2_gain, g_ln2_bias, g_b_proj, g_b_fc2, g_b_qkv, g_b_fc1 = sums
        g_w_qkv = jnp.transpose(g_w_qkv.reshape(3, heads, head, width), (3, 0, 1, 2))[None]
        layer_grads = (
            g_ln1_gain, g_ln1_bias, g_w_qkv, g_b_qkv.reshape(1, 3, heads, head), g_w_proj.reshape(1, heads, head, width), g_b_proj,
            g_ln2_gain, g_ln2_bias, g_w_fc1[None], g_b_fc1, g_w_fc2[None], g_b_fc2,
        )
        embed_grads = (g_w_patch, g_b_patch, g_cls_token, g_pos_embed)
        return (loss.reshape(1),) + embed_grads + layer_grads + (g_lnf_gain, g_lnf_bias, jnp.transpose(g_w_head), g_b_head)

    return jax.shard_map(body, mesh=mesh, in_specs=in_specs, out_specs=out_specs, check_vma=False)
```
